512 devices in a mesh: wide: 64 (over z, x), narrow: 8 (over y, core).
Axes of the slice: x: 4, y: 4, z: 16, core: 2. Of those that a mesh axis runs over, the one named last changes fastest.
Arguments:
- particle_position: float32 [3, 4096, 128], P(None, ('wide', 'narrow')), may hold values from -6 to 6
- particle_velocity: float32 [3, 4096, 128], P(None, ('wide', 'narrow')), may hold values from -6 to 6
- radius: float32 [4096, 128], P(('wide', 'narrow')), may hold values from 0.4 to 1
- block_live_count: int32 [4096], P(('wide', 'narrow')), may hold values from 64 to 128
- cell_index: int32 [4096, 128], P(('wide', 'narrow')), may hold values from 0 to 8191
- block_offset: int32 [4096], P(('wide', 'narrow')), may hold values from -2 to 2, as said below
- neighbours: int32 [4096, 6], P(('wide', 'narrow')), may hold values from 0 to 7, as said below
- gas_velocity: float32 [3, 512, 64, 128], P(None, 'wide', 'narrow'), may hold values from -6 to 6
- pressure_source: float32 [512, 64, 128], P('wide', 'narrow'), may hold values from -6 to 6
- void_before: float32 [512, 64, 128], P('wide', 'narrow'), may hold values from 0.6 to 1
Outputs:
- pressure: float32 [512, 64, 128], P('wide', 'narrow')
- gas_next: float32 [3, 512, 64, 128], P(None, 'wide', 'narrow')
- updated_particle_velocity: float32 [3, 4096, 128], P(None, ('wide', 'narrow'))
The draws below stay inside these ranges and needn't reach their ends.
Inputs may be any that keep to these rules, and one draw needn't show every extreme that they name: For a block held at index w along wide, w + block_offset lies in 0 to 63. At most 3 blocks of one device share one offset, and on every device some offset has exactly 3. `neighbours`: each block lists 6 different blocks of its own device, never itself.
All inputs are finite; a program needn't handle non-finite values.
Results may differ from the reference program's by a relative error of at most 0.0003.
Values sent between devices are 32-bit elements; how exact they have to be, the bound alone decides.
A program may use at most 128 MiB of HBM per device.

```python
import math
import jax
import jax.numpy as jnp
from jax import lax

NX = 128
CZ = 8
CY = 8
PARTICLE_SLOTS = 128
BLOCKS_PER_CHIPSET = 8
NEIGHBOUR_COUNT = 6
SPREAD = 2
LEVELS = 4
SWEEPS = 2
COARSE_SWEEPS = 4
CAP = 3
NZ = 512
NY = 64
BLOCKS = 4096
N_WIDE = 64
N_NARROW = 8


def draw_block_offset(key, part):
    block_groups = N_WIDE * N_NARROW
    choices_total = 2 * SPREAD + 1
    slot_total = choices_total * CAP
    first_key, second_key, third_key = jax.random.split(jax.random.fold_in(key, 11), 3)
    holder = (jnp.arange(block_groups, dtype=jnp.int32) // N_NARROW)[:, None]
    offsets = jnp.arange(choices_total, dtype=jnp.int32) - SPREAD
    allowed = jnp.logical_and(holder + offsets[None, :] >= 0, holder + offsets[None, :] < N_WIDE)
    pick_score = jax.random.randint(first_key, (block_groups, choices_total), 0, 1024) * choices_total + jnp.arange(choices_total, dtype=jnp.int32)[None, :]
    pick_score = jnp.where(allowed, pick_score, 1 << 28)
    filled = jnp.argmin(pick_score, axis=1).astype(jnp.int32)
    slot_group = jnp.arange(slot_total, dtype=jnp.int32) // CAP
    slot_allowed = allowed[:, slot_group]
    priority = jax.random.randint(second_key, (block_groups, slot_total), 0, 1024) * slot_total + jnp.arange(slot_total, dtype=jnp.int32)[None, :] + slot_total
    priority = jnp.where(slot_group[None, :] == filled[:, None], jnp.arange(slot_total, dtype=jnp.int32)[None, :], priority)
    priority = jnp.where(slot_allowed, priority, priority + (1 << 28))
    order = jnp.argsort(priority, axis=1)[:, :BLOCKS_PER_CHIPSET]
    chosen_offset = slot_group[order] - SPREAD
    shuffle_score = jax.random.randint(third_key, (block_groups, BLOCKS_PER_CHIPSET), 0, 1024) * BLOCKS_PER_CHIPSET + jnp.arange(BLOCKS_PER_CHIPSET, dtype=jnp.int32)[None, :]
    shuffle = jnp.argsort(shuffle_score, axis=1)
    return jnp.take_along_axis(chosen_offset, shuffle, axis=1).reshape(-1).astype(jnp.int32)


def draw_neighbours(key, part):
    others = BLOCKS_PER_CHIPSET - 1
    score = jax.random.randint(jax.random.fold_in(key, 23), (BLOCKS, others), 0, 4096) * others + jnp.arange(others, dtype=jnp.int32)[None, :]
    picked = jnp.argsort(score, axis=1)[:, :NEIGHBOUR_COUNT].astype(jnp.int32)
    local_index = (jnp.arange(BLOCKS, dtype=jnp.int32) % BLOCKS_PER_CHIPSET)[:, None]
    return ((local_index + 1 + picked) % BLOCKS_PER_CHIPSET).astype(jnp.int32)


def set_ends(drawn, stream_key, least, top_value):
    dims = drawn.shape
    index_at = [jax.random.randint(jax.random.fold_in(stream_key, axis), (), 0, dims[axis]) for axis in range(len(dims))]
    drawn = drawn.at[tuple(index_at)].set(least)
    longest = dims.index(max(dims))
    index_at[longest] = (index_at[longest] + 1) % dims[longest]
    return drawn.at[tuple(index_at)].set(top_value)


def level_of(stream_key, dims, pieces, low, top_value):
    def one(axis_at, blocks):
        draws = jax.random.uniform(jax.random.fold_in(jax.random.fold_in(stream_key, 6), axis_at), (blocks,), jnp.float32, low / len(pieces), top_value / len(pieces))
        return jnp.repeat(jnp.exp(draws), dims[axis_at] // blocks).reshape((-1,) + (1,) * (len(dims) - axis_at - 1))

    level = one(*pieces[0])
    for cut in pieces[1:]:
        level = level * one(*cut)
    return level


def normal_values(key, dims, spread, bound, cuts=(), kind=jnp.bfloat16):
    loudness = level_of(key, dims, cuts, -0.22, 0.18) if cuts else 1.0
    result = jax.random.normal(key, dims, jnp.float32) * spread * loudness
    return jnp.minimum(jnp.maximum(result, -bound), bound).astype(kind)


def setup_inputs(seed: int = 0) -> dict:
    key_list = jax.random.split(jax.random.key(seed), 11)
    return {
        "particle_position": normal_values(key_list[0], (3, BLOCKS, PARTICLE_SLOTS), 1.0, 6.0, ((1, 512),), jnp.float32),
        "particle_velocity": normal_values(key_list[1], (3, BLOCKS, PARTICLE_SLOTS), 1.0, 6.0, ((1, 512),), jnp.float32),
        "radius": jnp.clip(jnp.exp(math.log(1.0) - 0.9162907 * jax.random.uniform(key_list[2], (BLOCKS, PARTICLE_SLOTS), jnp.float32) ** level_of(key_list[2], (BLOCKS, PARTICLE_SLOTS), ((0, 512),), -0.2, 0.2)), 0.4, 1.0),
        "block_live_count": set_ends(jax.random.randint(key_list[3], (BLOCKS,), PARTICLE_SLOTS // 2, PARTICLE_SLOTS + 1), jax.random.fold_in(key_list[3], 1), PARTICLE_SLOTS // 2, PARTICLE_SLOTS).astype(jnp.int32),
        "cell_index": set_ends(jax.random.randint(key_list[4], (BLOCKS, PARTICLE_SLOTS), 0, CZ * CY * NX), jax.random.fold_in(key_list[4], 1), 0, (CZ * CY * NX) - 1).astype(jnp.int32),
        "block_offset": draw_block_offset(jax.random.fold_in(key_list[10], 71), 0),
        "neighbours": draw_neighbours(jax.random.fold_in(key_list[10], 71), 0),
        "gas_velocity": normal_values(key_list[7], (3, NZ, NY, NX), 1.0, 6.0, ((1, 64), (2, 8)), jnp.float32),
        "pressure_source": normal_values(key_list[8], (NZ, NY, NX), 1.0, 6.0, ((0, 64), (1, 8)), jnp.float32),
        "void_before": jnp.clip(0.6 + 0.39999998 * jax.random.uniform(key_list[9], (NZ, NY, NX), jnp.float32) ** level_of(key_list[9], (NZ, NY, NX), ((0, 64), (1, 8)), -0.2, 0.2), 0.6, 1.0),
    }


relax_weight = 0.8
solid_most = 0.6
void_power = 2.65
drag_base = 0.5
drag_slope = 0.5
stiffness = 16.0
softening = 0.1
particle_density = 2.0
gas_density = 1.0
step_duration = 0.25
gravity = -1.0

def restrict(grid_field):
    depth_cells, lane_cells, width_cells = grid_field.shape
    return grid_field.reshape(depth_cells // 2, 2, lane_cells // 2, 2, width_cells // 2, 2).mean(axis=(1, 3, 5))

def prolong(grid_field):
    return jnp.repeat(jnp.repeat(jnp.repeat(grid_field, 2, axis=0), 2, axis=1), 2, axis=2)

def coefs_from_padded(padded, weight):
    middle = padded[1:-1, 1:-1, 1:-1]
    couplings = (0.5 * weight * (middle + padded[:-2, 1:-1, 1:-1]), 0.5 * weight * (middle + padded[2:, 1:-1, 1:-1]), 0.5 * weight * (middle + padded[1:-1, :-2, 1:-1]), 0.5 * weight * (middle + padded[1:-1, 2:, 1:-1]), 0.5 * weight * (middle + padded[1:-1, 1:-1, :-2]), 0.5 * weight * (middle + padded[1:-1, 1:-1, 2:]))
    diagonal = couplings[0] + couplings[1] + couplings[2] + couplings[3] + couplings[4] + couplings[5]
    return (couplings, diagonal)

def apply_padded(padded, couplings, diagonal):
    middle = padded[1:-1, 1:-1, 1:-1]
    beside = couplings[0] * padded[:-2, 1:-1, 1:-1] + couplings[1] * padded[2:, 1:-1, 1:-1]
    beside = beside + couplings[2] * padded[1:-1, :-2, 1:-1] + couplings[3] * padded[1:-1, 2:, 1:-1]
    beside = beside + couplings[4] * padded[1:-1, 1:-1, :-2] + couplings[5] * padded[1:-1, 1:-1, 2:]
    return diagonal * middle - beside

def pad_plain(grid_field):
    return jnp.pad(grid_field, 1)

def unchanged(grid_field):
    return grid_field

def cycle(right_side, levels, level_index):
    couplings, diagonal, padder, enter_level, leave_level = levels[level_index]
    right_side = enter_level(right_side)
    coarsest = level_index == len(levels) - 1
    sweep_total = COARSE_SWEEPS if coarsest else SWEEPS
    iterate = relax_weight * right_side / diagonal
    for sweep_index in range(sweep_total - 1):
        iterate = iterate + relax_weight * (right_side - apply_padded(padder(iterate), couplings, diagonal)) / diagonal
    if not coarsest:
        residual = right_side - apply_padded(padder(iterate), couplings, diagonal)
        iterate = iterate + prolong(cycle(restrict(residual), levels, level_index + 1))
        for sweep_index in range(SWEEPS):
            iterate = iterate + relax_weight * (right_side - apply_padded(padder(iterate), couplings, diagonal)) / diagonal
    return leave_level(iterate)

def pressure_gradient(padded):
    return jnp.stack([0.5 * (padded[2:, 1:-1, 1:-1] - padded[:-2, 1:-1, 1:-1]), 0.5 * (padded[1:-1, 2:, 1:-1] - padded[1:-1, :-2, 1:-1]), 0.5 * (padded[1:-1, 1:-1, 2:] - padded[1:-1, 1:-1, :-2])])

def pairwise_force(local_positions, local_radii, local_live_mask, there_pos, there_rad, there_live):
    apart_z = local_positions[0][:, :, None] - there_pos[0][:, None, :]
    apart_y = local_positions[1][:, :, None] - there_pos[1][:, None, :]
    apart_x = local_positions[2][:, :, None] - there_pos[2][:, None, :]
    distance = jnp.sqrt(apart_z * apart_z + apart_y * apart_y + apart_x * apart_x + softening * softening)
    intersection = jnp.maximum(local_radii[:, :, None] + there_rad[:, None, :] - distance, 0.0)
    weight = intersection * there_live[:, None, :] / distance
    return local_live_mask[None] * jnp.stack([lax.optimization_barrier(jnp.sum(apart_z * weight, axis=2)), lax.optimization_barrier(jnp.sum(apart_y * weight, axis=2)), lax.optimization_barrier(jnp.sum(apart_x * weight, axis=2))])

def block_contact_forces(slot_positions, slot_radii, live_flags, adjacent_blocks):
    block_count = slot_radii.shape[0]
    batch_extent = math.gcd(block_count, 8)
    factor = stiffness / (slot_radii.shape[1] * (adjacent_blocks.shape[1] + 1))

    def one_batch(batch_index):
        leading_row = batch_index * batch_extent
        local_positions = lax.dynamic_slice_in_dim(slot_positions, leading_row, batch_extent, 1)
        local_radii = lax.dynamic_slice_in_dim(slot_radii, leading_row, batch_extent, 0)
        local_live_mask = lax.dynamic_slice_in_dim(live_flags, leading_row, batch_extent, 0)
        near_list = lax.dynamic_slice_in_dim(adjacent_blocks, leading_row, batch_extent, 0)
        total_force_sum = pairwise_force(local_positions, local_radii, local_live_mask, local_positions, local_radii, local_live_mask)
        for column in range(adjacent_blocks.shape[1]):
            selected_blocks = near_list[:, column]
            total_force_sum = total_force_sum + pairwise_force(local_positions, local_radii, local_live_mask, slot_positions[:, selected_blocks], slot_radii[selected_blocks], live_flags[selected_blocks])
        return total_force_sum * factor
    stacked = lax.map(one_batch, jnp.arange(block_count // batch_extent, dtype=jnp.int32))
    return stacked.transpose(1, 0, 2, 3).reshape(3, block_count, -1)

def reference(particle_position, particle_velocity, radius, block_live_count, cell_index, block_offset, neighbours, gas_velocity, pressure_source, void_before):
    slot_index_list = jnp.arange(PARTICLE_SLOTS, dtype=jnp.int32)
    live_flags = (slot_index_list[None, :] < block_live_count[:, None]).astype(jnp.float32)
    particle_volume = radius * radius * radius
    volume_live_mask = particle_volume * live_flags
    owner_index = jnp.arange(BLOCKS, dtype=jnp.int32) // BLOCKS_PER_CHIPSET
    home_slab = owner_index // N_NARROW + block_offset
    lateral = owner_index % N_NARROW
    height = home_slab[:, None] * CZ + cell_index // (CY * NX)
    across = lateral[:, None] * CY + cell_index // NX % CY
    flat_cell = ((height * NY + across) * NX + cell_index % NX).reshape(-1).astype(jnp.int32)
    total_cells = NZ * NY * NX
    vol_flat = volume_live_mask.reshape(-1)
    solid_sum = jnp.zeros((total_cells,), jnp.float32).at[flat_cell].add(vol_flat)
    voidage = 1.0 - solid_most * solid_sum / (1.0 + solid_sum)
    slip_vel = gas_velocity.reshape(3, -1)[:, flat_cell] - particle_velocity.reshape(3, -1)
    slip_speed = jnp.sqrt(lax.optimization_barrier(jnp.sum(slip_vel * slip_vel, axis=0)))
    drag_force = (vol_flat * (drag_base + drag_slope * slip_speed) * voidage[flat_cell] ** (-void_power))[None] * slip_vel
    reaction = jnp.zeros((3, total_cells), jnp.float32).at[:, flat_cell].add(-drag_force)
    voidage_grid = voidage.reshape(NZ, NY, NX)
    right_side = pressure_source + (void_before - voidage_grid) / step_duration
    levels = []
    coarse = voidage_grid
    for level_index in range(LEVELS):
        if level_index > 0:
            coarse = restrict(coarse)
        couplings, diagonal = coefs_from_padded(pad_plain(coarse), 0.25 ** level_index)
        levels.append((couplings, diagonal, pad_plain, unchanged, unchanged))
    pressure = cycle(right_side, levels, 0)
    gradient = pressure_gradient(pad_plain(pressure))
    gas_next = gas_velocity + step_duration * (reaction.reshape(3, NZ, NY, NX) / (gas_density * voidage_grid)[None] - gradient / gas_density)
    fluid_force = drag_force - vol_flat[None] * gradient.reshape(3, -1)[:, flat_cell]
    block_groups = N_WIDE * N_NARROW
    position_groups = particle_position.reshape(3, block_groups, BLOCKS_PER_CHIPSET, PARTICLE_SLOTS).transpose(1, 0, 2, 3)

    def single_group(inputs):
        return block_contact_forces(inputs[0], inputs[1], inputs[2], inputs[3])
    contact_force = lax.map(single_group, (position_groups, radius.reshape(block_groups, BLOCKS_PER_CHIPSET, PARTICLE_SLOTS), live_flags.reshape(block_groups, BLOCKS_PER_CHIPSET, PARTICLE_SLOTS), neighbours.reshape(block_groups, BLOCKS_PER_CHIPSET, NEIGHBOUR_COUNT)))
    contact_force = contact_force.transpose(1, 0, 2, 3).reshape(3, BLOCKS, PARTICLE_SLOTS)
    downward = jnp.array([gravity, 0.0, 0.0], jnp.float32)[:, None, None]
    particle_acceleration = (contact_force + fluid_force.reshape(3, BLOCKS, PARTICLE_SLOTS)) / (particle_density * particle_volume)[None] + downward
    updated_particle_velocity = live_flags[None] * (particle_velocity + step_duration * particle_acceleration)
    return (pressure, gas_next, updated_particle_velocity)
```

```python
import functools

import jax
import jax.numpy as jnp
from jax import lax
from jax.experimental import pallas as pl
from jax.experimental.pallas import tpu as pltpu
from jax.sharding import PartitionSpec as P

SPREAD = 2
CAP = 3
GROUPS = 2 * SPREAD + 1
SLOTS = GROUPS * CAP
REACH = 7
RHS_REACH = 6

relax_weight = 0.8
solid_most = 0.6
void_power = 2.65
drag_base = 0.5
drag_slope = 0.5
stiffness = 16.0
softening = 0.1
particle_density = 2.0
step_duration = 0.25
gravity = -1.0

F32 = jnp.float32
BF16 = jnp.bfloat16
MESH = pl.DeviceIdType.MESH
AROUND = [(a, b) for a in (-1, 0, 1) for b in (-1, 0, 1) if (a, b) != (0, 0)]


def iota(shape, dim):
    return lax.broadcasted_iota(jnp.int32, shape, dim)


def zloop(low, high, body, step=4):
    whole = (high - low) // step
    if whole > 1:

        def chunk(i, carry):
            for k in range(step):
                body(low + i * step + k)
            return carry

        lax.fori_loop(0, whole, chunk, 0)
    else:
        whole = 0
    for z in range(low + whole * step, high):
        body(z)


def turn(v, shift, axis):
    return pltpu.roll(v, shift % v.shape[axis], axis)


def lanes_before(v, s):
    return jnp.where(iota(v.shape, 1) >= s, turn(v, s, 1), 0.0)


def lanes_after(v, s):
    return jnp.where(iota(v.shape, 1) < v.shape[1] - s, turn(v, -s, 1), 0.0)


def rows_before(v, s):
    return jnp.where(iota(v.shape, 0) >= s, turn(v, s, 0), 0.0)


def rows_after(v, s):
    return jnp.where(iota(v.shape, 0) < v.shape[0] - s, turn(v, -s, 0), 0.0)


def pair_sum(v, s, axis):
    low = (iota(v.shape, axis) & s) == 0
    return v + jnp.where(low, turn(v, -s, axis), turn(v, s, axis))


def halves(v):
    high = v.astype(BF16)
    return high, (v - high.astype(F32)).astype(BF16)


def kernel(
    nw, nn,
    counts, offs, nbr, pos, vel, rad, cell, gas, source, before,
    p_out, g_out, u_out,
    stage, pin, back, drg, gath, grow, con, cols,
    ohx, slhs, rlhs, glhs,
    por0, c0, b0, va0, vb0, z0, ym0, yp0, xm0, xp0, dg0, di0,
    por1, b1, va1, vb1, z1, ym1, yp1, xm1, xp1, dg1, di1,
    l1out, l1in, c1p, c1b, l2p, l2b,
    p2, b2, va2, vb2, z2, ci2, co2, xm2, xp2, dg2, di2,
    p3, b3, va3, vb3, z3, y3, xm3, xp3, dg3, di3,
    vfin,
    s_a, r_a, s_c0, r_c0, s_b, r_b, s_l1, r_l1, s_1p, r_1p, s_1b, r_1b, s_2p, r_2p, s_2b, r_2b, s_d, r_d,
):
    w = lax.axis_index("wide")
    n = lax.axis_index("narrow")
    blocks, slots = rad.shape

    def w_ok(d):
        return jnp.logical_and(w + d >= 0, w + d < nw)

    def n_ok(d):
        return jnp.logical_and(n + d >= 0, n + d < nn)

    def there(a, b):
        if b == 0:
            return w_ok(a)
        if a == 0:
            return n_ok(b)
        return jnp.logical_and(w_ok(a), n_ok(b))

    def remote(src, dst, send, recv, to):
        return pltpu.make_async_remote_copy(
            src_ref=src, dst_ref=dst, send_sem=send, recv_sem=recv, device_id=to, device_id_type=MESH
        )

    pending = []

    def start(copies):
        for copy, sends, _ in copies:
            pl.when(sends)(copy.start)
        pending.extend(copies)

    def arrive(copies):
        for copy, _, gets in copies:
            pl.when(gets)(copy.wait_recv)

    for ref in (pin, back, l1in, c1p, c1b, l2p, l2b, vfin):
        ref[...] = jnp.zeros_like(ref)
    for z in range(24):
        por0[z] = jnp.zeros((24, 128), F32)
        c0[z] = jnp.zeros((24, 128), F32)
    for z in range(8):
        c0[8 + z, 8:16] = source[z] + before[z] * (1.0 / step_duration)

    barrier = pltpu.get_barrier_semaphore()
    peers = []
    for d in range(1, REACH + 1):
        peers += [(w_ok(d), (w + d, n)), (w_ok(-d), (w - d, n))]
    for k in range(nn):
        peers.append((n != k, (w, k)))
    for a, b in AROUND:
        if a and b:
            peers.append((there(a, b), (w + a, n + b)))
    for ok, to in peers:
        pl.when(ok)(
            functools.partial(pl.semaphore_signal, barrier, inc=1, device_id=to, device_id_type=MESH)
        )

    off = [offs[b] for b in range(blocks)]
    rank = []
    for b in range(blocks):
        r = jnp.int32(0)
        for a in range(b):
            r = r + jnp.where(off[a] == off[b], 1, 0)
        rank.append(r)
    row8 = iota((blocks, slots), 0)
    live_count = jnp.zeros((blocks, slots), jnp.int32)
    for b in range(blocks):
        live_count = jnp.where(row8 == b, counts[b], live_count)
    live = jnp.where(iota((blocks, slots), 1) < live_count, 1.0, 0.0)
    radius = rad[...]
    volume = radius * radius * radius
    parts = [volume * live, vel[0], vel[1], vel[2], cell[...].astype(F32)]
    row16 = iota((16, slots), 0)
    for c, part in enumerate(parts):
        rows = jnp.zeros((16, slots), F32)
        for b in range(blocks):
            key = (off[b] + SPREAD) * CAP + rank[b]
            rows = jnp.where(row16 == key, jnp.broadcast_to(part[b : b + 1], rows.shape), rows)
        for o in range(GROUPS):
            stage[o, c * CAP : (c + 1) * CAP] = rows[o * CAP : (o + 1) * CAP]
    pin[SPREAD] = stage[SPREAD]

    count = jnp.int32(0)
    for ok, _ in peers:
        count = count + jnp.where(ok, 1, 0)
    pl.semaphore_wait(barrier, count)

    copies_a = []
    for o in range(GROUPS):
        d = o - SPREAD
        if d:
            copies_a.append(
                (remote(stage.at[o], pin.at[o], s_a.at[o], r_a.at[o], (w + d, n)), w_ok(d), w_ok(-d))
            )
    start(copies_a)

    def block_copies(ref, send, recv):
        return [
            (
                remote(
                    ref.at[8:16, 8:16],
                    ref.at[8 * (1 - a) : 8 * (2 - a), 8 * (1 - b) : 8 * (2 - b)],
                    send.at[i], recv.at[i], (w + a, n + b),
                ),
                there(a, b),
                there(-a, -b),
            )
            for i, (a, b) in enumerate(AROUND)
        ]

    copies_c0 = block_copies(c0, s_c0, r_c0)
    start(copies_c0)

    bar = jnp.concatenate(
        [pos[0], pos[1], pos[2], jnp.where(live > 0.0, radius, -1000.0), jnp.zeros((128 - 4 * blocks, slots), F32)],
        axis=0,
    ).T
    for c in range(4):
        for b in range(blocks):
            k = c * blocks + b
            cols[c, b] = jnp.broadcast_to(bar[:, k : k + 1], (slots, slots))
    factor = stiffness / (slots * 7)

    def contact_of(g, carry):
        own = [jnp.broadcast_to(pos[c, pl.ds(g, 1)], (8, slots)) for c in range(3)]
        own_rad = jnp.broadcast_to(rad[pl.ds(g, 1)], (8, slots))
        total = [jnp.zeros((8, slots), F32) for _ in range(3)]
        for k in range(7):
            other = g if k == 6 else nbr[g, k]
            for j in range(0, slots, 8):
                apart = [own[c] - cols[c, other, j : j + 8] for c in range(3)]
                square = apart[0] * apart[0] + apart[1] * apart[1]
                square = square + (apart[2] * apart[2] + softening * softening)
                inverse = lax.rsqrt(square)
                weight = jnp.maximum((own_rad + cols[3, other, j : j + 8]) * inverse - 1.0, 0.0)
                total = [total[c] + apart[c] * weight for c in range(3)]
        for c in range(3):
            con[c, pl.ds(g, 1)] = jnp.sum(total[c], axis=0, keepdims=True) * factor
        return carry

    lax.fori_loop(0, blocks, contact_of, 0)

    arrive(copies_a)

    zy_iota = iota((64, slots), 0)
    x_iota = iota((128, slots), 0)

    def cells_of(o, r):
        where = pin[o, 4 * CAP + r : 4 * CAP + r + 1].astype(jnp.int32)
        return where >> 7, where & 127

    def spread_volume(o, carry):
        for r in range(CAP):
            at = pl.ds(pl.multiple_of((o * CAP + r) * slots, slots), slots)
            zy, x = cells_of(o, r)
            one = jnp.where(jnp.broadcast_to(x, x_iota.shape) == x_iota, 1.0, 0.0).astype(BF16)
            ohx[0:128, at] = one
            ohx[128:256, at] = one
            hit = jnp.broadcast_to(zy, zy_iota.shape) == zy_iota
            here = jnp.where(hit, jnp.broadcast_to(pin[o, r : r + 1], zy_iota.shape), 0.0)
            high, low = halves(here)
            slhs[0:64, at] = high
            slhs[64:128, at] = low
        return carry

    lax.fori_loop(0, GROUPS, spread_volume, 0)
    both = lax.dot_general(
        slhs[...], ohx[0:128], (((1,), (1,)), ((), ())), preferred_element_type=F32
    )
    solid = both[0:64] + both[64:128]
    voidage = 1.0 - solid_most * solid / (1.0 + solid)
    for z in range(8):
        por0[8 + z, 8:16] = voidage[8 * z : 8 * z + 8]

    lane = iota((8, 128), 1)
    lane4 = iota((1, 128), 1) & 3

    def coarser(pairs, s):
        return pair_sum(pair_sum(pairs[0] + pairs[1], s, 0), s, 1) * 0.125

    def packed(cells):
        rows = [cells[0][0:1], cells[0][4:5], cells[1][0:1], cells[1][4:5]]
        row = rows[3]
        for k in range(3):
            row = jnp.where(lane4 == k, rows[k], row)
        return row

    finer = [coarser((voidage[16 * i : 16 * i + 8], voidage[16 * i + 8 : 16 * i + 16]), 1) for i in range(4)]
    c1p[n] = packed([coarser((finer[0], finer[1]), 2), coarser((finer[2], finer[3]), 2)])

    copies_b = block_copies(por0, s_b, r_b)
    start(copies_b)

    def row_copies(ref, send, recv):
        return [
            (
                remote(ref.at[n], ref.at[n], send.at[d], recv.at[d], (w, lax.rem(n + d, nn))),
                jnp.bool_(True),
                jnp.bool_(True),
            )
            for d in range(1, nn)
        ]

    def start_rows(copies):
        for copy, _, _ in copies:
            copy.start()
        pending.extend(copies)

    def arrive_rows(copies):
        for copy, _, _ in copies:
            copy.wait_recv()

    def slab_copies(ref, reach, send, recv):
        made = []
        for d in [s * k for k in range(1, reach + 1) for s in (1, -1)]:
            i = d + REACH
            made.append(
                (
                    remote(ref.at[REACH], ref.at[REACH - d], send.at[i], recv.at[i], (w + d, n)),
                    w_ok(d),
                    w_ok(-d),
                )
            )
        return made

    def rows_to_slab(ref):
        row = iota((8, 128), 0)
        slab = jnp.zeros((8, 128), F32)
        for k in range(nn):
            slab = jnp.where(row == k, jnp.broadcast_to(ref[k], (8, 128)), slab)
        return slab

    copies_1p = row_copies(c1p, s_1p, r_1p)
    start_rows(copies_1p)

    def fill_gather(f, values):
        high, low = halves(values)
        glhs[f * 64 : f * 64 + 64, 0:128] = high
        glhs[f * 64 : f * 64 + 64, 128:256] = low

    def gather(fields):
        def one(o, carry):
            for r in range(CAP):
                at = pl.ds(pl.multiple_of((o * CAP + r) * slots, slots), slots)
                found = jnp.dot(glhs[0 : 64 * fields], ohx[:, at], preferred_element_type=F32)
                zy, _ = cells_of(o, r)
                hit = jnp.broadcast_to(zy, zy_iota.shape) == zy_iota
                for f in range(fields):
                    gath[o, f * CAP + r : f * CAP + r + 1] = jnp.sum(
                        jnp.where(hit, found[64 * f : 64 * f + 64], 0.0), axis=0, keepdims=True
                    )
            return carry

        lax.fori_loop(0, GROUPS, one, 0)

    for f in range(3):
        fill_gather(f, gas[f].reshape(64, 128))
    fill_gather(3, voidage)
    gather(4)
    for o in range(GROUPS):
        slip = [gath[o, c * CAP : (c + 1) * CAP] - pin[o, (1 + c) * CAP : (2 + c) * CAP] for c in range(3)]
        speed = jnp.sqrt(slip[0] * slip[0] + slip[1] * slip[1] + slip[2] * slip[2])
        held = gath[o, 3 * CAP : 4 * CAP]
        scale = pin[o, 0:CAP] * (drag_base + drag_slope * speed) * jnp.exp(-void_power * jnp.log(held))
        for c in range(3):
            drg[o, c * CAP : (c + 1) * CAP] = scale * slip[c]

    arrive_rows(copies_1p)
    l2p[REACH] = rows_to_slab(c1p)
    copies_2p = slab_copies(l2p, REACH, s_2p, r_2p)
    start(copies_2p)

    def spread_drag(o, carry):
        for r in range(CAP):
            at = pl.ds(pl.multiple_of((o * CAP + r) * slots, slots), slots)
            zy, _ = cells_of(o, r)
            hit = jnp.broadcast_to(zy, zy_iota.shape) == zy_iota
            for c in range(3):
                row = drg[o, c * CAP + r : c * CAP + r + 1]
                high, low = halves(jnp.where(hit, jnp.broadcast_to(row, zy_iota.shape), 0.0))
                rlhs[128 * c : 128 * c + 64, at] = high
                rlhs[128 * c + 64 : 128 * c + 128, at] = low
        return carry

    lax.fori_loop(0, GROUPS, spread_drag, 0)
    sums = lax.dot_general(
        rlhs[...], ohx[0:128], (((1,), (1,)), ((), ())), preferred_element_type=F32
    )
    for c in range(3):
        onto = sums[128 * c : 128 * c + 64] + sums[128 * c + 64 : 128 * c + 128]
        grow[c] = gas[c].reshape(64, 128) - step_duration * onto / voidage

    arrive(copies_c0)
    arrive(copies_b)

    row24 = iota((24, 128), 0)
    inside_y = jnp.logical_and(
        jnp.logical_or(row24 >= 8, n > 0), jnp.logical_or(row24 < 16, n < nn - 1)
    )
    inside_y = jnp.where(inside_y, 1, 0)

    def inside(block):
        ok = jnp.logical_and(w + block >= 0, w + block < nw)
        return inside_y * jnp.where(ok, 1, 0) > 0

    def coefs(por, z, s, half, layers, cz, cym, cyp, cxm, cxp, dg, di):
        here = por[z]
        zm = half * (here + por[z - 1])
        zp = half * (here + por[z + 1])
        ym = half * (here + turn(here, s, 0))
        yp = half * (here + turn(here, -s, 0))
        xm = half * (here + lanes_before(here, s))
        xp = half * (here + lanes_after(here, s))
        diagonal = zm + zp + ym + yp + xm + xp
        lanes = iota(here.shape, 1)
        cz[z] = zm
        cym[z] = ym
        cyp[z] = yp
        cxm[z] = jnp.where(lanes >= s, xm, 0.0)
        cxp[z] = jnp.where(lanes < 128 - s, xp, 0.0)
        dg[z] = diagonal
        scaled = jnp.where(inside(z // layers - 1), relax_weight / diagonal, 0.0)
        di[z] = scaled
        return scaled

    def residual_at(v, b, z, s, cz, cym, cyp, cxm, cxp, dg):
        here = v[z]
        beside = cz[z] * v[z - 1] + cz[z + 1] * v[z + 1]
        beside = beside + (cym[z] * turn(here, s, 0) + cyp[z] * turn(here, -s, 0))
        beside = beside + (cxm[z] * turn(here, s, 1) + cxp[z] * turn(here, -s, 1))
        return here, (b[z] - dg[z] * here) + beside

    def sweep(v, to, b, z, s, cz, cym, cyp, cxm, cxp, dg, di):
        here, residual = residual_at(v, b, z, s, cz, cym, cyp, cxm, cxp, dg)
        to[z] = here + di[z] * residual

    level0 = (z0, ym0, yp0, xm0, xp0, dg0)
    level1 = (z1, ym1, yp1, xm1, xp1, dg1)

    def first0(z):
        b = c0[z] - por0[z] * (1.0 / step_duration)
        b0[z] = b
        va0[z] = coefs(por0, z, 1, 0.5, 8, *level0, di0) * b

    zloop(2, 22, first0)
    zloop(3, 21, lambda z: sweep(va0, vb0, b0, z, 1, *level0, di0))

    def por1_of(i):
        por1[i] = coarser((por0[2 * i], por0[2 * i + 1]), 1)

    zloop(0, 12, por1_of)

    def down0(i):
        _, low = residual_at(vb0, b0, 2 * i, 1, *level0)
        _, high = residual_at(vb0, b0, 2 * i + 1, 1, *level0)
        b1[i] = coarser((low, high), 1)

    zloop(2, 10, down0, 2)
    zloop(1, 11, lambda i: coefs(por1, i, 2, 0.125, 4, *level1, di1), 5)
    z1[11] = 0.125 * (por1[11] + por1[10])

    def first1(i):
        va1[i] = di1[i] * b1[i]

    zloop(2, 10, first1, 8)
    zloop(3, 9, lambda i: sweep(va1, vb1, b1, i, 2, *level1, di1), 6)
    left = [residual_at(vb1, b1, i, 2, *level1)[1][8:16] for i in range(4, 8)]
    c1b[n] = packed([coarser((left[0], left[1]), 2), coarser((left[2], left[3]), 2)])
    copies_1b = row_copies(c1b, s_1b, r_1b)
    start_rows(copies_1b)

    even_lane = (lane & 1) == 0
    row = iota((8, 128), 0)
    even_row = (row & 1) == 0
    for k in range(2):
        i = 4 + 2 * k
        right = jnp.where(even_lane, b1[i, 8:16], b1[i + 1, 8:16])
        iterate = jnp.where(even_lane, vb1[i, 8:16], vb1[i + 1, 8:16])
        l1out[k] = jnp.where(even_row, right, iterate)
    copies_l1 = [
        (
            remote(l1out, l1in.at[1 - a, 1 - b], s_l1.at[i], r_l1.at[i], (w + a, n + b)),
            there(a, b),
            there(-a, -b),
        )
        for i, (a, b) in enumerate(AROUND)
    ]
    start(copies_l1)

    arrive(copies_2p)

    def unpack4(slab):
        cells = []
        for k in range(4):
            one = jnp.where((lane & 3) == k, slab, 0.0)
            cells.append(pair_sum(pair_sum(one, 1, 1), 2, 1))
        return cells

    def unpack_por(k):
        cells = unpack4(l2p[k])
        for q in range(4):
            p2[2 * k + q // 2, q % 2] = cells[q]
        p3[k] = pair_sum((cells[0] + cells[1]) + (cells[2] + cells[3]), 4, 1) * 0.125

    zloop(0, 2 * REACH + 1, unpack_por, 5)
    real_row = jnp.where(row < nn, 1, 0)

    def inside_coarse(block):
        ok = jnp.logical_and(w + block >= 0, w + block < nw)
        return real_row * jnp.where(ok, 1, 0) > 0

    def coefs2(j):
        half = 0.5 * 0.25**2
        even, odd = p2[j, 0], p2[j, 1]
        inner = half * (even + odd)
        ci2[j] = inner
        outer = half * (even + rows_before(odd, 1))
        co2[j] = outer
        outer_odd = half * (odd + rows_after(even, 1))
        ok = inside_coarse(j // 2 - REACH)
        for y, here in enumerate((even, odd)):
            zm = half * (here + p2[j - 1, y])
            zp = half * (here + p2[j + 1, y])
            xm = half * (here + lanes_before(here, 4))
            xp = half * (here + lanes_after(here, 4))
            diagonal = zm + zp + inner + (outer_odd if y else outer) + xm + xp
            z2[j, y] = zm
            xm2[j, y] = jnp.where(lane >= 4, xm, 0.0)
            xp2[j, y] = jnp.where(lane < 124, xp, 0.0)
            dg2[j, y] = diagonal
            di2[j, y] = jnp.where(ok, relax_weight / diagonal, 0.0)

    zloop(1, 4 * REACH + 1, coefs2)

    def coefs3(k):
        half = 0.5 * 0.25**3
        here = p3[k]
        zm = half * (here + p3[k - 1])
        zp = half * (here + p3[k + 1])
        ym = half * (here + rows_before(here, 1))
        yp = half * (here + rows_after(here, 1))
        xm = half * (here + lanes_before(here, 8))
        xp = half * (here + lanes_after(here, 8))
        diagonal = zm + zp + ym + yp + xm + xp
        z3[k] = zm
        y3[k] = ym
        xm3[k] = jnp.where(lane >= 8, xm, 0.0)
        xp3[k] = jnp.where(lane < 120, xp, 0.0)
        dg3[k] = diagonal
        di3[k] = jnp.where(inside_coarse(k - REACH), relax_weight / diagonal, 0.0)

    zloop(1, 2 * REACH, coefs3)

    arrive_rows(copies_1b)
    l2b[REACH] = rows_to_slab(c1b)
    copies_2b = slab_copies(l2b, RHS_REACH, s_2b, r_2b)
    start(copies_2b)

    arrive(copies_l1)
    for a, b in AROUND:
        for k in range(2):
            both_layers = l1in[1 + a, 1 + b, k]
            for q in range(2):
                if q == 0:
                    layer = jnp.where(even_lane, both_layers, turn(both_layers, 1, 1))
                else:
                    layer = jnp.where(even_lane, turn(both_layers, -1, 1), both_layers)
                i = 4 * (1 + a) + 2 * k + q
                at = slice(8 * (1 + b), 8 * (2 + b))
                b1[i, at] = jnp.where(even_row, layer, turn(layer, 1, 0))
                vb1[i, at] = jnp.where(even_row, turn(layer, -1, 0), layer)

    def residual2(v, j):
        even, odd = v[j, 0], v[j, 1]
        outer = co2[j]
        made = []
        for y, here in enumerate((even, odd)):
            beside = z2[j, y] * v[j - 1, y] + z2[j + 1, y] * v[j + 1, y]
            if y == 0:
                beside = beside + (ci2[j] * odd + outer * rows_before(odd, 1))
            else:
                beside = beside + (ci2[j] * even + rows_after(outer, 1) * rows_after(even, 1))
            beside = beside + (xm2[j, y] * turn(here, 4, 1) + xp2[j, y] * turn(here, -4, 1))
            made.append((here, (b2[j, y] - dg2[j, y] * here) + beside))
        return made

    def sweep2(v, to):
        def at(j):
            for y, (here, residual) in enumerate(residual2(v, j)):
                to[j, y] = here + di2[j, y] * residual

        return at

    def residual3(v, k):
        here = v[k]
        beside = z3[k] * v[k - 1] + z3[k + 1] * v[k + 1]
        beside = beside + (y3[k] * rows_before(here, 1) + rows_after(y3[k], 1) * rows_after(here, 1))
        beside = beside + (xm3[k] * turn(here, 8, 1) + xp3[k] * turn(here, -8, 1))
        return here, (b3[k] - dg3[k] * here) + beside

    def sweep3(v, to):
        def at(k):
            here, residual = residual3(v, k)
            to[k] = here + di3[k] * residual

        return at

    arrive(copies_2b)

    def first2(k):
        cells = unpack4(l2b[k])
        for q in range(4):
            j, y = 2 * k + q // 2, q % 2
            b2[j, y] = cells[q]
            va2[j, y] = di2[j, y] * cells[q]

    zloop(1, 2 * REACH, first2)
    zloop(3, 27, sweep2(va2, vb2))

    def down2(k):
        low = residual2(vb2, 2 * k)
        high = residual2(vb2, 2 * k + 1)
        b = pair_sum((low[0][1] + low[1][1]) + (high[0][1] + high[1][1]), 4, 1) * 0.125
        b3[k] = b
        va3[k] = di3[k] * b

    zloop(2, 13, down2, 3)
    zloop(3, 12, sweep3(va3, vb3), 9)
    zloop(4, 11, sweep3(vb3, va3), 7)
    zloop(5, 10, sweep3(va3, vb3), 5)

    def up2(k):
        for q in range(4):
            j, y = 2 * k + q // 2, q % 2
            va2[j, y] = vb2[j, y] + vb3[k]

    zloop(5, 10, up2, 5)
    zloop(11, 19, sweep2(va2, vb2))
    for j in range(12, 18):
        for y, (here, residual) in enumerate(residual2(vb2, j)):
            vfin[j - 12, y, 8:16] = here + di2[j, y] * residual

    low_row = row < 4
    for q in range(6):
        for b in range(3):
            cells = [
                jnp.broadcast_to(vfin[q, y, pl.ds(7 + n + b, 1)], (8, 128)) for y in range(2)
            ]
            step = jnp.where(low_row, cells[0], cells[1])
            at = slice(8 * b, 8 * b + 8)
            for i in (2 * q, 2 * q + 1):
                va1[i, at] = vb1[i, at] + step
    zloop(1, 11, lambda i: sweep(va1, vb1, b1, i, 2, *level1, di1), 5)
    zloop(2, 10, lambda i: sweep(vb1, va1, b1, i, 2, *level1, di1))

    def up0(i):
        step = va1[i]
        va0[2 * i] = vb0[2 * i] + step
        va0[2 * i + 1] = vb0[2 * i + 1] + step

    zloop(2, 10, up0)
    zloop(6, 18, lambda z: sweep(va0, vb0, b0, z, 1, *level0, di0))
    zloop(7, 17, lambda z: sweep(vb0, va0, b0, z, 1, *level0, di0), 5)

    for z in range(8):
        whole = va0[8 + z]
        here = whole[8:16]
        p_out[z] = here
        slopes = [
            0.5 * (va0[9 + z, 8:16] - va0[7 + z, 8:16]),
            0.5 * (turn(whole, -1, 0)[8:16] - turn(whole, 1, 0)[8:16]),
            0.5 * (lanes_after(here, 1) - lanes_before(here, 1)),
        ]
        for c in range(3):
            g_out[c, z] = grow[c, 8 * z : 8 * z + 8] - step_duration * slopes[c]
            high, low = halves(slopes[c])
            glhs[64 * c + 8 * z : 64 * c + 8 * z + 8, 0:128] = high
            glhs[64 * c + 8 * z : 64 * c + 8 * z + 8, 128:256] = low
    gather(3)
    for o in range(GROUPS):
        for c in range(3):
            at = slice(c * CAP, (c + 1) * CAP)
            drg[o, at] = drg[o, at] - pin[o, 0:CAP] * gath[o, at]
    copies_d = []
    for o in range(GROUPS):
        d = o - SPREAD
        if d:
            copies_d.append(
                (remote(drg.at[o], back.at[o], s_d.at[o], r_d.at[o], (w - d, n)), w_ok(-d), w_ok(d))
            )
    start(copies_d)
    back[SPREAD] = drg[SPREAD]
    arrive(copies_d)
    for c in range(3):
        fluid = jnp.zeros((blocks, slots), F32)
        for b in range(blocks):
            one = back[off[b] + SPREAD, pl.ds(c * CAP + rank[b], 1)]
            fluid = jnp.where(row8 == b, jnp.broadcast_to(one, fluid.shape), fluid)
        push = (con[c] * live + fluid) / (particle_density * volume)
        if c == 0:
            push = push + gravity
        u_out[c] = live * (vel[c] + step_duration * push)

    for copy, sends, _ in pending:
        pl.when(sends)(copy.wait_send)


def local(nw, nn, position, velocity, radius, count, cell, offset, neighbours, gas, source, before):
    vmem = pl.BlockSpec(memory_space=pltpu.VMEM)
    smem = pl.BlockSpec(memory_space=pltpu.SMEM)

    def ram(*shape, dtype=F32):
        return pltpu.VMEM(shape, dtype)

    dma = pltpu.SemaphoreType.DMA
    block = ram(24, 24, 128)
    block1 = ram(12, 24, 128)
    tall = 2 * REACH + 1
    coarse2 = ram(2 * tall, 2, 8, 128)
    coarse2y = ram(2 * tall, 8, 128)
    coarse3 = ram(tall, 8, 128)
    particles = SLOTS * radius.shape[1]
    scratch = [
        *[ram(GROUPS, 16, 128)] * 5,
        ram(3, 64, 128),
        ram(3, 8, 128),
        ram(4, 8, 128, 128),
        ram(256, particles, dtype=BF16),
        ram(128, particles, dtype=BF16),
        ram(384, particles, dtype=BF16),
        ram(256, 256, dtype=BF16),
        *[block] * 12,
        *[block1] * 11,
        ram(2, 8, 128),
        ram(3, 3, 2, 8, 128),
        ram(8, 1, 128),
        ram(8, 1, 128),
        coarse3,
        coarse3,
        *[coarse2] * 5,
        coarse2y,
        coarse2y,
        *[coarse2] * 4,
        *[coarse3] * 10,
        ram(6, 2, 24, 128),
        *[dma((GROUPS,))] * 2,
        *[dma((8,))] * 6,
        *[dma((8,))] * 4,
        *[dma((tall,))] * 4,
        *[dma((GROUPS,))] * 2,
    ]
    return pl.pallas_call(
        functools.partial(kernel, nw, nn),
        out_shape=(
            jax.ShapeDtypeStruct(source.shape, F32),
            jax.ShapeDtypeStruct(gas.shape, F32),
            jax.ShapeDtypeStruct(velocity.shape, F32),
        ),
        in_specs=[smem] * 3 + [vmem] * 7,
        out_specs=(vmem, vmem, vmem),
        scratch_shapes=scratch,
        compiler_params=pltpu.CompilerParams(collective_id=0, has_side_effects=True),
        name="bed_step",
    )(count, offset, neighbours, position, velocity, radius, cell, gas, source, before)


def solution(mesh):
    placed = (
        P(None, ("wide", "narrow"), None),
        P(None, ("wide", "narrow"), None),
        P(("wide", "narrow"), None),
        P(("wide", "narrow")),
        P(("wide", "narrow"), None),
        P(("wide", "narrow")),
        P(("wide", "narrow"), None),
        P(None, "wide", "narrow", None),
        P("wide", "narrow", None),
        P("wide", "narrow", None),
    )
    return jax.shard_map(
        functools.partial(local, mesh.shape["wide"], mesh.shape["narrow"]),
        mesh=mesh,
        in_specs=placed,
        out_specs=(
            P("wide", "narrow", None),
            P(None, "wide", "narrow", None),
            P(None, ("wide", "narrow"), None),
        ),
        check_vma=False,
    )
```

```python
import functools

import jax
import jax.numpy as jnp
from jax import lax
from jax.experimental import pallas as pl
from jax.experimental.pallas import tpu as pltpu
from jax.sharding import PartitionSpec as P

SPREAD = 2
CAP = 3
GROUPS = 2 * SPREAD + 1
SLOTS = GROUPS * CAP
REACH = 7
RHS_REACH = 6

relax_weight = 0.8
solid_most = 0.6
void_power = 2.65
drag_base = 0.5
drag_slope = 0.5
stiffness = 16.0
softening = 0.1
particle_density = 2.0
step_duration = 0.25
gravity = -1.0

F32 = jnp.float32
BF16 = jnp.bfloat16
MESH = pl.DeviceIdType.MESH
AROUND = [(a, b) for a in (-1, 0, 1) for b in (-1, 0, 1) if (a, b) != (0, 0)]


def iota(shape, dim):
    return lax.broadcasted_iota(jnp.int32, shape, dim)


def zloop(low, high, body, step=4):
    whole = (high - low) // step
    if whole > 1:

        def chunk(i, carry):
            for k in range(step):
                body(low + i * step + k)
            return carry

        lax.fori_loop(0, whole, chunk, 0)
    else:
        whole = 0
    for z in range(low + whole * step, high):
        body(z)


def turn(v, shift, axis):
    return pltpu.roll(v, shift % v.shape[axis], axis)


def lanes_before(v, s):
    return jnp.where(iota(v.shape, 1) >= s, turn(v, s, 1), 0.0)


def lanes_after(v, s):
    return jnp.where(iota(v.shape, 1) < v.shape[1] - s, turn(v, -s, 1), 0.0)


def rows_before(v, s):
    return jnp.where(iota(v.shape, 0) >= s, turn(v, s, 0), 0.0)


def rows_after(v, s):
    return jnp.where(iota(v.shape, 0) < v.shape[0] - s, turn(v, -s, 0), 0.0)


def pair_sum(v, s, axis):
    low = (iota(v.shape, axis) & s) == 0
    return v + jnp.where(low, turn(v, -s, axis), turn(v, s, axis))


def halves(v):
    high = v.astype(BF16)
    return high, (v - high.astype(F32)).astype(BF16)


def kernel(
    nw, nn,
    counts_in, offs_in, nbr_in, pos_in, vel_in, rad_in, cell_in, gas_in, source_in, before_in,
    p_out, g_out, u_out,
    counts, offs, nbr, pos, vel, rad, cell, gas, source, before, s_in,
    stage, pin, back, drg, gath, grow, con, cols,
    ohx, rlhs, glhs,
    por0, c0, b0, va0, vb0, z0, ym0, yp0, xm0, xp0, dg0, di0,
    por1, b1, va1, vb1, z1, ym1, yp1, xm1, xp1, dg1, di1,
    l1out, l1in, c1p, c1b, l2p, l2b,
    p2, b2, va2, vb2, z2, ci2, co2, xm2, xp2, dg2, di2,
    p3, b3, va3, vb3, z3, y3, xm3, xp3, dg3, di3,
    vfin,
    s_a, r_a, s_c0, r_c0, s_b, r_b, s_l1, r_l1, s_1p, r_1p, s_1b, r_1b, s_2p, r_2p, s_2b, r_2b, s_d, r_d,
):
    w = lax.axis_index("wide")
    n = lax.axis_index("narrow")
    blocks, slots = rad.shape

    def w_ok(d):
        return jnp.logical_and(w + d >= 0, w + d < nw)

    def n_ok(d):
        return jnp.logical_and(n + d >= 0, n + d < nn)

    def there(a, b):
        if b == 0:
            return w_ok(a)
        if a == 0:
            return n_ok(b)
        return jnp.logical_and(w_ok(a), n_ok(b))

    def remote(src, dst, send, recv, to):
        return pltpu.make_async_remote_copy(
            src_ref=src, dst_ref=dst, send_sem=send, recv_sem=recv, device_id=to, device_id_type=MESH
        )

    pending = []

    def start(copies):
        for copy, sends, _ in copies:
            pl.when(sends)(copy.start)
        pending.extend(copies)

    def arrive(copies):
        for copy, _, gets in copies:
            pl.when(gets)(copy.wait_recv)

    given = (counts_in, offs_in, nbr_in, pos_in, vel_in, rad_in, cell_in, gas_in, source_in, before_in)
    taken = (counts, offs, nbr, pos, vel, rad, cell, gas, source, before)
    loads = [pltpu.make_async_copy(a, b, s_in.at[i]) for i, (a, b) in enumerate(zip(given, taken))]
    for i in (0, 1, 5, 4, 6, 8, 9, 3, 2, 7):
        loads[i].start()

    for ref in (pin, back, l1in, c1p, c1b, l2p, l2b, vfin):
        ref[...] = jnp.zeros_like(ref)
    for z in range(24):
        por0[z] = jnp.zeros((24, 128), F32)
        c0[z] = jnp.zeros((24, 128), F32)
    barrier = pltpu.get_barrier_semaphore()
    peers = []
    for d in range(1, REACH + 1):
        peers += [(w_ok(d), (w + d, n)), (w_ok(-d), (w - d, n))]
    for k in range(nn):
        peers.append((n != k, (w, k)))
    for a, b in AROUND:
        if a and b:
            peers.append((there(a, b), (w + a, n + b)))
    for ok, to in peers:
        pl.when(ok)(
            functools.partial(pl.semaphore_signal, barrier, inc=1, device_id=to, device_id_type=MESH)
        )

    for i in (0, 1, 5, 4, 6):
        loads[i].wait()

    off = [offs[b] for b in range(blocks)]
    rank = []
    for b in range(blocks):
        r = jnp.int32(0)
        for a in range(b):
            r = r + jnp.where(off[a] == off[b], 1, 0)
        rank.append(r)
    row8 = iota((blocks, slots), 0)
    live_count = jnp.zeros((blocks, slots), jnp.int32)
    for b in range(blocks):
        live_count = jnp.where(row8 == b, counts[b], live_count)
    live = jnp.where(iota((blocks, slots), 1) < live_count, 1.0, 0.0)
    radius = rad[...]
    volume = radius * radius * radius
    parts = [volume * live, vel[0], vel[1], vel[2], cell[...].astype(F32)]
    row16 = iota((16, slots), 0)
    for c, part in enumerate(parts):
        rows = jnp.zeros((16, slots), F32)
        for b in range(blocks):
            key = (off[b] + SPREAD) * CAP + rank[b]
            rows = jnp.where(row16 == key, jnp.broadcast_to(part[b : b + 1], rows.shape), rows)
        for o in range(GROUPS):
            stage[o, c * CAP : (c + 1) * CAP] = rows[o * CAP : (o + 1) * CAP]
    pin[SPREAD] = stage[SPREAD]
    for i in (8, 9):
        loads[i].wait()
    for z in range(8):
        c0[8 + z, 8:16] = source[z] + before[z] * (1.0 / step_duration)

    count = jnp.int32(0)
    for ok, _ in peers:
        count = count + jnp.where(ok, 1, 0)
    pl.semaphore_wait(barrier, count)

    copies_a = []
    for o in range(GROUPS):
        d = o - SPREAD
        if d:
            copies_a.append(
                (remote(stage.at[o], pin.at[o], s_a.at[o], r_a.at[o], (w + d, n)), w_ok(d), w_ok(-d))
            )
    start(copies_a)

    def block_copies(ref, corner, send, recv):
        made = []
        for i, (a, b) in enumerate(AROUND):
            low, high = 8, 16
            if a == 1:
                low = 16 - corner[0 if b == 0 else 1]
            if a == -1:
                high = 8 + corner[0 if b == 0 else 1]
            made.append(
                (
                    remote(
                        ref.at[low:high, 8:16],
                        ref.at[low - 8 * a : high - 8 * a, 8 * (1 - b) : 8 * (2 - b)],
                        send.at[i], recv.at[i], (w + a, n + b),
                    ),
                    there(a, b),
                    there(-a, -b),
                )
            )
        return made

    copies_c0 = block_copies(c0, (6, 6), s_c0, r_c0)

    for i in (3, 2, 7):
        loads[i].wait()

    bar = jnp.concatenate(
        [pos[0], pos[1], pos[2], jnp.where(live > 0.0, radius, -1000.0), jnp.zeros((128 - 4 * blocks, slots), F32)],
        axis=0,
    ).T
    for c in range(4):
        for b in range(blocks):
            k = c * blocks + b
            cols[c, b] = jnp.broadcast_to(bar[:, k : k + 1], (slots, slots))
    factor = stiffness / (slots * 7)

    def contact_of(g, carry):
        own = [jnp.broadcast_to(pos[c, pl.ds(g, 1)], (8, slots)) for c in range(3)]
        own_rad = jnp.broadcast_to(rad[pl.ds(g, 1)], (8, slots))
        total = [jnp.zeros((8, slots), F32) for _ in range(3)]
        for k in range(7):
            other = g if k == 6 else nbr[g, k]
            for j in range(0, slots, 8):
                apart = [own[c] - cols[c, other, j : j + 8] for c in range(3)]
                square = apart[0] * apart[0] + apart[1] * apart[1]
                square = square + (apart[2] * apart[2] + softening * softening)
                inverse = lax.rsqrt(square)
                weight = jnp.maximum((own_rad + cols[3, other, j : j + 8]) * inverse - 1.0, 0.0)
                total = [total[c] + apart[c] * weight for c in range(3)]
        for c in range(3):
            con[c, pl.ds(g, 1)] = jnp.sum(total[c], axis=0, keepdims=True) * factor
        return carry

    lax.fori_loop(0, blocks // 2, contact_of, 0)
    start(copies_c0)
    lax.fori_loop(blocks // 2, blocks, contact_of, 0)

    arrive(copies_a)

    zy_iota = iota((64, slots), 0)
    x_iota = iota((128, slots), 0)

    def cells_of(o, r):
        where = pin[o, 4 * CAP + r : 4 * CAP + r + 1].astype(jnp.int32)
        return where >> 7, where & 127

    both = jnp.zeros((128, 128), F32)
    for o in range(GROUPS):
        ones, values = [], []
        for r in range(CAP):
            zy, x = cells_of(o, r)
            ones.append(jnp.where(jnp.broadcast_to(x, x_iota.shape) == x_iota, 1.0, 0.0).astype(BF16))
            hit = jnp.broadcast_to(zy, zy_iota.shape) == zy_iota
            here = jnp.where(hit, jnp.broadcast_to(pin[o, r : r + 1], zy_iota.shape), 0.0)
            values.append(jnp.concatenate(halves(here), axis=0))
        one = jnp.concatenate(ones, axis=1)
        at = slice(o * CAP * slots, (o + 1) * CAP * slots)
        ohx[0:128, at] = one
        ohx[128:256, at] = one
        both = both + lax.dot_general(
            jnp.concatenate(values, axis=1), one, (((1,), (1,)), ((), ())), preferred_element_type=F32
        )
    solid = both[0:64] + both[64:128]
    voidage = 1.0 - solid_most * solid / (1.0 + solid)
    for z in range(8):
        por0[8 + z, 8:16] = voidage[8 * z : 8 * z + 8]
    copies_b = block_copies(por0, (8, 6), s_b, r_b)
    start(copies_b)

    lane = iota((8, 128), 1)
    lane4 = iota((1, 128), 1) & 3

    def coarser(pairs, s):
        return pair_sum(pair_sum(pairs[0] + pairs[1], s, 0), s, 1) * 0.125

    def packed(cells):
        rows = [cells[0][0:1], cells[0][4:5], cells[1][0:1], cells[1][4:5]]
        row = rows[3]
        for k in range(3):
            row = jnp.where(lane4 == k, rows[k], row)
        return row

    finer = [coarser((voidage[16 * i : 16 * i + 8], voidage[16 * i + 8 : 16 * i + 16]), 1) for i in range(4)]
    c1p[n] = packed([coarser((finer[0], finer[1]), 2), coarser((finer[2], finer[3]), 2)])


    def row_copies(ref, send, recv):
        return [
            (
                remote(ref.at[n], ref.at[n], send.at[d], recv.at[d], (w, lax.rem(n + d, nn))),
                jnp.bool_(True),
                jnp.bool_(True),
            )
            for d in range(1, nn)
        ]

    def start_rows(copies):
        for copy, _, _ in copies:
            copy.start()
        pending.extend(copies)

    def arrive_rows(copies):
        for copy, _, _ in copies:
            copy.wait_recv()

    def slab_copies(ref, reach, send, recv):
        made = []
        for d in [s * k for k in range(1, reach + 1) for s in (1, -1)]:
            i = d + REACH
            made.append(
                (
                    remote(ref.at[REACH], ref.at[REACH - d], send.at[i], recv.at[i], (w + d, n)),
                    w_ok(d),
                    w_ok(-d),
                )
            )
        return made

    def rows_to_slab(ref):
        row = iota((8, 128), 0)
        slab = jnp.zeros((8, 128), F32)
        for k in range(nn):
            slab = jnp.where(row == k, jnp.broadcast_to(ref[k], (8, 128)), slab)
        return slab

    copies_1p = row_copies(c1p, s_1p, r_1p)
    start_rows(copies_1p)

    def fill_gather(f, values):
        high, low = halves(values)
        glhs[f * 64 : f * 64 + 64, 0:128] = high
        glhs[f * 64 : f * 64 + 64, 128:256] = low

    def gather(fields):
        def one(o, carry):
            width = CAP * slots
            at = pl.ds(pl.multiple_of(o * width, slots), width)
            found = jnp.dot(glhs[0 : 64 * fields], ohx[:, at], preferred_element_type=F32)
            for r in range(CAP):
                zy, _ = cells_of(o, r)
                hit = jnp.broadcast_to(zy, zy_iota.shape) == zy_iota
                for f in range(fields):
                    gath[o, f * CAP + r : f * CAP + r + 1] = jnp.sum(
                        jnp.where(hit, found[64 * f : 64 * f + 64, r * slots : (r + 1) * slots], 0.0),
                        axis=0, keepdims=True,
                    )
            return carry

        lax.fori_loop(0, GROUPS, one, 0)

    for f in range(3):
        fill_gather(f, gas[f].reshape(64, 128))
    fill_gather(3, voidage)
    gather(4)
    for o in range(GROUPS):
        slip = [gath[o, c * CAP : (c + 1) * CAP] - pin[o, (1 + c) * CAP : (2 + c) * CAP] for c in range(3)]
        speed = jnp.sqrt(slip[0] * slip[0] + slip[1] * slip[1] + slip[2] * slip[2])
        held = gath[o, 3 * CAP : 4 * CAP]
        scale = pin[o, 0:CAP] * (drag_base + drag_slope * speed) * jnp.exp(-void_power * jnp.log(held))
        for c in range(3):
            drg[o, c * CAP : (c + 1) * CAP] = scale * slip[c]

    arrive_rows(copies_1p)
    l2p[REACH] = rows_to_slab(c1p)
    copies_2p = slab_copies(l2p, REACH, s_2p, r_2p)
    start(copies_2p)

    def spread_drag(o, carry):
        for r in range(CAP):
            at = pl.ds(pl.multiple_of((o * CAP + r) * slots, slots), slots)
            zy, _ = cells_of(o, r)
            hit = jnp.broadcast_to(zy, zy_iota.shape) == zy_iota
            for c in range(3):
                row = drg[o, c * CAP + r : c * CAP + r + 1]
                high, low = halves(jnp.where(hit, jnp.broadcast_to(row, zy_iota.shape), 0.0))
                rlhs[128 * c : 128 * c + 64, at] = high
                rlhs[128 * c + 64 : 128 * c + 128, at] = low
        return carry

    lax.fori_loop(0, GROUPS, spread_drag, 0)
    sums = lax.dot_general(
        rlhs[...], ohx[0:128], (((1,), (1,)), ((), ())), preferred_element_type=F32
    )
    for c in range(3):
        onto = sums[128 * c : 128 * c + 64] + sums[128 * c + 64 : 128 * c + 128]
        grow[c] = gas[c].reshape(64, 128) - step_duration * onto / voidage

    arrive(copies_c0)
    arrive(copies_b)

    row24 = iota((24, 128), 0)
    inside_y = jnp.logical_and(
        jnp.logical_or(row24 >= 8, n > 0), jnp.logical_or(row24 < 16, n < nn - 1)
    )
    inside_y = jnp.where(inside_y, 1, 0)

    def inside(block):
        ok = jnp.logical_and(w + block >= 0, w + block < nw)
        return inside_y * jnp.where(ok, 1, 0) > 0

    def coefs(por, z, s, half, layers, cz, cym, cyp, cxm, cxp, dg, di):
        here = por[z]
        zm = half * (here + por[z - 1])
        zp = half * (here + por[z + 1])
        ym = half * (here + turn(here, s, 0))
        yp = half * (here + turn(here, -s, 0))
        xm = half * (here + lanes_before(here, s))
        xp = half * (here + lanes_after(here, s))
        diagonal = zm + zp + ym + yp + xm + xp
        lanes = iota(here.shape, 1)
        cz[z] = zm
        cym[z] = ym
        cyp[z] = yp
        cxm[z] = jnp.where(lanes >= s, xm, 0.0)
        cxp[z] = jnp.where(lanes < 128 - s, xp, 0.0)
        dg[z] = diagonal
        scaled = jnp.where(inside(z // layers - 1), relax_weight / diagonal, 0.0)
        di[z] = scaled
        return scaled

    def residual_at(v, b, z, s, cz, cym, cyp, cxm, cxp, dg):
        here = v[z]
        beside = cz[z] * v[z - 1] + cz[z + 1] * v[z + 1]
        beside = beside + (cym[z] * turn(here, s, 0) + cyp[z] * turn(here, -s, 0))
        beside = beside + (cxm[z] * turn(here, s, 1) + cxp[z] * turn(here, -s, 1))
        return here, (b[z] - dg[z] * here) + beside

    def sweep(v, to, b, z, s, cz, cym, cyp, cxm, cxp, dg, di):
        here, residual = residual_at(v, b, z, s, cz, cym, cyp, cxm, cxp, dg)
        to[z] = here + di[z] * residual

    level0 = (z0, ym0, yp0, xm0, xp0, dg0)
    level1 = (z1, ym1, yp1, xm1, xp1, dg1)

    def first0(z):
        b = c0[z] - por0[z] * (1.0 / step_duration)
        b0[z] = b
        va0[z] = coefs(por0, z, 1, 0.5, 8, *level0, di0) * b

    zloop(2, 22, first0)
    zloop(3, 21, lambda z: sweep(va0, vb0, b0, z, 1, *level0, di0))

    def por1_of(i):
        por1[i] = coarser((por0[2 * i], por0[2 * i + 1]), 1)

    zloop(0, 12, por1_of)

    def down0(i):
        _, low = residual_at(vb0, b0, 2 * i, 1, *level0)
        _, high = residual_at(vb0, b0, 2 * i + 1, 1, *level0)
        b1[i] = coarser((low, high), 1)

    zloop(2, 10, down0, 2)
    zloop(1, 11, lambda i: coefs(por1, i, 2, 0.125, 4, *level1, di1), 5)
    z1[11] = 0.125 * (por1[11] + por1[10])

    def first1(i):
        va1[i] = di1[i] * b1[i]

    zloop(2, 10, first1, 8)
    zloop(3, 9, lambda i: sweep(va1, vb1, b1, i, 2, *level1, di1), 6)
    left = [residual_at(vb1, b1, i, 2, *level1)[1][8:16] for i in range(4, 8)]
    c1b[n] = packed([coarser((left[0], left[1]), 2), coarser((left[2], left[3]), 2)])
    copies_1b = row_copies(c1b, s_1b, r_1b)
    start_rows(copies_1b)

    even_lane = (lane & 1) == 0
    row = iota((8, 128), 0)
    even_row = (row & 1) == 0
    for k in range(2):
        i = 4 + 2 * k
        right = jnp.where(even_lane, b1[i, 8:16], b1[i + 1, 8:16])
        iterate = jnp.where(even_lane, vb1[i, 8:16], vb1[i + 1, 8:16])
        l1out[k] = jnp.where(even_row, right, iterate)
    copies_l1 = [
        (
            remote(l1out, l1in.at[1 - a, 1 - b], s_l1.at[i], r_l1.at[i], (w + a, n + b)),
            there(a, b),
            there(-a, -b),
        )
        for i, (a, b) in enumerate(AROUND)
    ]
    start(copies_l1)

    arrive(copies_2p)

    def unpack4(slab):
        cells = []
        for k in range(4):
            one = jnp.where((lane & 3) == k, slab, 0.0)
            cells.append(pair_sum(pair_sum(one, 1, 1), 2, 1))
        return cells

    def unpack_por(k):
        cells = unpack4(l2p[k])
        for q in range(4):
            p2[2 * k + q // 2, q % 2] = cells[q]
        p3[k] = pair_sum((cells[0] + cells[1]) + (cells[2] + cells[3]), 4, 1) * 0.125

    zloop(0, 2 * REACH + 1, unpack_por, 5)
    real_row = jnp.where(row < nn, 1, 0)

    def inside_coarse(block):
        ok = jnp.logical_and(w + block >= 0, w + block < nw)
        return real_row * jnp.where(ok, 1, 0) > 0

    def coefs2(j):
        half = 0.5 * 0.25**2
        even, odd = p2[j, 0], p2[j, 1]
        inner = half * (even + odd)
        ci2[j] = inner
        outer = half * (even + rows_before(odd, 1))
        co2[j] = outer
        outer_odd = half * (odd + rows_after(even, 1))
        ok = inside_coarse(j // 2 - REACH)
        for y, here in enumerate((even, odd)):
            zm = half * (here + p2[j - 1, y])
            zp = half * (here + p2[j + 1, y])
            xm = half * (here + lanes_before(here, 4))
            xp = half * (here + lanes_after(here, 4))
            diagonal = zm + zp + inner + (outer_odd if y else outer) + xm + xp
            z2[j, y] = zm
            xm2[j, y] = jnp.where(lane >= 4, xm, 0.0)
            xp2[j, y] = jnp.where(lane < 124, xp, 0.0)
            dg2[j, y] = diagonal
            di2[j, y] = jnp.where(ok, relax_weight / diagonal, 0.0)

    zloop(1, 4 * REACH + 1, coefs2)

    def coefs3(k):
        half = 0.5 * 0.25**3
        here = p3[k]
        zm = half * (here + p3[k - 1])
        zp = half * (here + p3[k + 1])
        ym = half * (here + rows_before(here, 1))
        yp = half * (here + rows_after(here, 1))
        xm = half * (here + lanes_before(here, 8))
        xp = half * (here + lanes_after(here, 8))
        diagonal = zm + zp + ym + yp + xm + xp
        z3[k] = zm
        y3[k] = ym
        xm3[k] = jnp.where(lane >= 8, xm, 0.0)
        xp3[k] = jnp.where(lane < 120, xp, 0.0)
        dg3[k] = diagonal
        di3[k] = jnp.where(inside_coarse(k - REACH), relax_weight / diagonal, 0.0)

    zloop(1, 2 * REACH, coefs3)

    arrive_rows(copies_1b)
    l2b[REACH] = rows_to_slab(c1b)
    copies_2b = slab_copies(l2b, RHS_REACH, s_2b, r_2b)
    start(copies_2b)

    arrive(copies_l1)
    for a, b in AROUND:
        for k in range(2):
            both_layers = l1in[1 + a, 1 + b, k]
            for q in range(2):
                if q == 0:
                    layer = jnp.where(even_lane, both_layers, turn(both_layers, 1, 1))
                else:
                    layer = jnp.where(even_lane, turn(both_layers, -1, 1), both_layers)
                i = 4 * (1 + a) + 2 * k + q
                at = slice(8 * (1 + b), 8 * (2 + b))
                b1[i, at] = jnp.where(even_row, layer, turn(layer, 1, 0))
                vb1[i, at] = jnp.where(even_row, turn(layer, -1, 0), layer)

    def residual2(v, j):
        even, odd = v[j, 0], v[j, 1]
        outer = co2[j]
        made = []
        for y, here in enumerate((even, odd)):
            beside = z2[j, y] * v[j - 1, y] + z2[j + 1, y] * v[j + 1, y]
            if y == 0:
                beside = beside + (ci2[j] * odd + outer * rows_before(odd, 1))
            else:
                beside = beside + (ci2[j] * even + rows_after(outer, 1) * rows_after(even, 1))
            beside = beside + (xm2[j, y] * turn(here, 4, 1) + xp2[j, y] * turn(here, -4, 1))
            made.append((here, (b2[j, y] - dg2[j, y] * here) + beside))
        return made

    def sweep2(v, to):
        def at(j):
            for y, (here, residual) in enumerate(residual2(v, j)):
                to[j, y] = here + di2[j, y] * residual

        return at

    def residual3(v, k):
        here = v[k]
        beside = z3[k] * v[k - 1] + z3[k + 1] * v[k + 1]
        beside = beside + (y3[k] * rows_before(here, 1) + rows_after(y3[k], 1) * rows_after(here, 1))
        beside = beside + (xm3[k] * turn(here, 8, 1) + xp3[k] * turn(here, -8, 1))
        return here, (b3[k] - dg3[k] * here) + beside

    def sweep3(v, to):
        def at(k):
            here, residual = residual3(v, k)
            to[k] = here + di3[k] * residual

        return at

    arrive(copies_2b)

    def first2(k):
        cells = unpack4(l2b[k])
        for q in range(4):
            j, y = 2 * k + q // 2, q % 2
            b2[j, y] = cells[q]
            va2[j, y] = di2[j, y] * cells[q]

    zloop(1, 2 * REACH, first2)
    zloop(3, 27, sweep2(va2, vb2))

    def down2(k):
        low = residual2(vb2, 2 * k)
        high = residual2(vb2, 2 * k + 1)
        b = pair_sum((low[0][1] + low[1][1]) + (high[0][1] + high[1][1]), 4, 1) * 0.125
        b3[k] = b
        va3[k] = di3[k] * b

    zloop(2, 13, down2, 3)
    zloop(3, 12, sweep3(va3, vb3), 9)
    zloop(4, 11, sweep3(vb3, va3), 7)
    zloop(5, 10, sweep3(va3, vb3), 5)

    def up2(k):
        for q in range(4):
            j, y = 2 * k + q // 2, q % 2
            va2[j, y] = vb2[j, y] + vb3[k]

    zloop(5, 10, up2, 5)
    zloop(11, 19, sweep2(va2, vb2))
    for j in range(12, 18):
        for y, (here, residual) in enumerate(residual2(vb2, j)):
            vfin[j - 12, y, 8:16] = here + di2[j, y] * residual

    low_row = row < 4
    for q in range(6):
        for b in range(3):
            cells = [
                jnp.broadcast_to(vfin[q, y, pl.ds(7 + n + b, 1)], (8, 128)) for y in range(2)
            ]
            step = jnp.where(low_row, cells[0], cells[1])
            at = slice(8 * b, 8 * b + 8)
            for i in (2 * q, 2 * q + 1):
                va1[i, at] = vb1[i, at] + step
    zloop(1, 11, lambda i: sweep(va1, vb1, b1, i, 2, *level1, di1), 5)
    zloop(2, 10, lambda i: sweep(vb1, va1, b1, i, 2, *level1, di1))

    def up0(i):
        step = va1[i]
        va0[2 * i] = vb0[2 * i] + step
        va0[2 * i + 1] = vb0[2 * i + 1] + step

    zloop(2, 10, up0)
    zloop(6, 18, lambda z: sweep(va0, vb0, b0, z, 1, *level0, di0))
    zloop(7, 17, lambda z: sweep(vb0, va0, b0, z, 1, *level0, di0), 5)

    for z in range(8):
        whole = va0[8 + z]
        here = whole[8:16]
        slopes = [
            0.5 * (va0[9 + z, 8:16] - va0[7 + z, 8:16]),
            0.5 * (turn(whole, -1, 0)[8:16] - turn(whole, 1, 0)[8:16]),
            0.5 * (lanes_after(here, 1) - lanes_before(here, 1)),
        ]
        for c in range(3):
            g_out[c, z] = slopes[c]
            high, low = halves(slopes[c])
            glhs[64 * c + 8 * z : 64 * c + 8 * z + 8, 0:128] = high
            glhs[64 * c + 8 * z : 64 * c + 8 * z + 8, 128:256] = low
    gather(3)
    for o in range(GROUPS):
        for c in range(3):
            at = slice(c * CAP, (c + 1) * CAP)
            drg[o, at] = drg[o, at] - pin[o, 0:CAP] * gath[o, at]
    copies_d = []
    for o in range(GROUPS):
        d = o - SPREAD
        if d:
            copies_d.append(
                (remote(drg.at[o], back.at[o], s_d.at[o], r_d.at[o], (w - d, n)), w_ok(-d), w_ok(d))
            )
    start(copies_d)
    back[SPREAD] = drg[SPREAD]
    for z in range(8):
        p_out[z] = va0[8 + z, 8:16]
        for c in range(3):
            g_out[c, z] = grow[c, 8 * z : 8 * z + 8] - step_duration * g_out[c, z]
    for copy, sends, _ in pending[: -len(copies_d)]:
        pl.when(sends)(copy.wait_send)
    fluid_scale = live * step_duration / (particle_density * volume)
    moved = [
        live * (vel[c] + (step_duration * gravity if c == 0 else 0.0)) + fluid_scale * con[c] * live
        for c in range(3)
    ]
    arrive(copies_d)
    for c in range(3):
        fluid = jnp.zeros((blocks, slots), F32)
        for b in range(blocks):
            one = back[off[b] + SPREAD, pl.ds(c * CAP + rank[b], 1)]
            fluid = jnp.where(row8 == b, jnp.broadcast_to(one, fluid.shape), fluid)
        u_out[c] = moved[c] + fluid_scale * fluid

    for copy, sends, _ in copies_d:
        pl.when(sends)(copy.wait_send)


def put_out(p, g, u, p_out, g_out, u_out):
    p_out[...] = p[...]
    g_out[...] = g[...]
    u_out[...] = u[...]


def local(nw, nn, position, velocity, radius, count, cell, offset, neighbours, gas, source, before):
    vmem = pl.BlockSpec(memory_space=pltpu.VMEM)
    hbm = pl.BlockSpec(memory_space=pltpu.HBM)

    def ram(*shape, dtype=F32):
        return pltpu.VMEM(shape, dtype)

    dma = pltpu.SemaphoreType.DMA
    block = ram(24, 24, 128)
    block1 = ram(12, 24, 128)
    tall = 2 * REACH + 1
    coarse2 = ram(2 * tall, 2, 8, 128)
    coarse2y = ram(2 * tall, 8, 128)
    coarse3 = ram(tall, 8, 128)
    particles = SLOTS * radius.shape[1]
    given = (count, offset, neighbours, position, velocity, radius, cell, gas, source, before)
    scratch = [
        *[pltpu.SMEM(a.shape, a.dtype) for a in given[:3]],
        *[pltpu.VMEM(a.shape, a.dtype) for a in given[3:]],
        dma((len(given),)),
        *[ram(GROUPS, 16, 128)] * 5,
        ram(3, 64, 128),
        ram(3, 8, 128),
        ram(4, 8, 128, 128),
        ram(256, particles, dtype=BF16),
        ram(384, particles, dtype=BF16),
        ram(256, 256, dtype=BF16),
        *[block] * 12,
        *[block1] * 11,
        ram(2, 8, 128),
        ram(3, 3, 2, 8, 128),
        ram(8, 1, 128),
        ram(8, 1, 128),
        coarse3,
        coarse3,
        *[coarse2] * 5,
        coarse2y,
        coarse2y,
        *[coarse2] * 4,
        *[coarse3] * 10,
        ram(6, 2, 24, 128),
        *[dma((GROUPS,))] * 2,
        *[dma((8,))] * 6,
        *[dma((8,))] * 4,
        *[dma((tall,))] * 4,
        *[dma((GROUPS,))] * 2,
    ]
    results = (
        jax.ShapeDtypeStruct(source.shape, F32),
        jax.ShapeDtypeStruct(gas.shape, F32),
        jax.ShapeDtypeStruct(velocity.shape, F32),
    )
    made = pl.pallas_call(
        functools.partial(kernel, nw, nn),
        out_shape=results,
        in_specs=[hbm] * len(given),
        out_specs=(vmem, vmem, vmem),
        scratch_shapes=scratch,
        compiler_params=pltpu.CompilerParams(
            collective_id=0, has_side_effects=True, vmem_limit_bytes=24 << 20
        ),
        name="bed_step",
    )(*[pltpu.with_memory_space_constraint(a, pltpu.HBM) for a in given])
    return pl.pallas_call(
        put_out,
        out_shape=results,
        in_specs=[vmem] * 3,
        out_specs=(vmem, vmem, vmem),
        compiler_params=pltpu.CompilerParams(vmem_limit_bytes=8 << 20),
        name="put_out",
    )(*made)


def solution(mesh):
    placed = (
        P(None, ("wide", "narrow"), None),
        P(None, ("wide", "narrow"), None),
        P(("wide", "narrow"), None),
        P(("wide", "narrow")),
        P(("wide", "narrow"), None),
        P(("wide", "narrow")),
        P(("wide", "narrow"), None),
        P(None, "wide", "narrow", None),
        P("wide", "narrow", None),
        P("wide", "narrow", None),
    )
    return jax.shard_map(
        functools.partial(local, mesh.shape["wide"], mesh.shape["narrow"]),
        mesh=mesh,
        in_specs=placed,
        out_specs=(
            P("wide", "narrow", None),
            P(None, "wide", "narrow", None),
            P(None, ("wide", "narrow"), None),
        ),
        check_vma=False,
    )
```

```python
import functools

import jax
import jax.numpy as jnp
from jax import lax
from jax.experimental import pallas as pl
from jax.experimental.pallas import tpu as pltpu
from jax.sharding import PartitionSpec as P

SPREAD = 2
CAP = 3
GROUPS = 2 * SPREAD + 1
SLOTS = GROUPS * CAP
REACH = 7
RHS_REACH = 6

relax_weight = 0.8
solid_most = 0.6
void_power = 2.65
drag_base = 0.5
drag_slope = 0.5
stiffness = 16.0
softening = 0.1
particle_density = 2.0
step_duration = 0.25
gravity = -1.0

F32 = jnp.float32
BF16 = jnp.bfloat16
MESH = pl.DeviceIdType.MESH
AROUND = [(a, b) for a in (-1, 0, 1) for b in (-1, 0, 1) if (a, b) != (0, 0)]


def iota(shape, dim):
    return lax.broadcasted_iota(jnp.int32, shape, dim)


def zloop(low, high, body, step=4):
    whole = (high - low) // step
    if whole > 1:

        def chunk(i, carry):
            for k in range(step):
                body(low + i * step + k)
            return carry

        lax.fori_loop(0, whole, chunk, 0)
    else:
        whole = 0
    for z in range(low + whole * step, high):
        body(z)


def turn(v, shift, axis):
    return pltpu.roll(v, shift % v.shape[axis], axis)


def lanes_before(v, s):
    return jnp.where(iota(v.shape, 1) >= s, turn(v, s, 1), 0.0)


def lanes_after(v, s):
    return jnp.where(iota(v.shape, 1) < v.shape[1] - s, turn(v, -s, 1), 0.0)


def rows_before(v, s):
    return jnp.where(iota(v.shape, 0) >= s, turn(v, s, 0), 0.0)


def rows_after(v, s):
    return jnp.where(iota(v.shape, 0) < v.shape[0] - s, turn(v, -s, 0), 0.0)


def pair_sum(v, s, axis):
    low = (iota(v.shape, axis) & s) == 0
    return v + jnp.where(low, turn(v, -s, axis), turn(v, s, axis))


def halves(v):
    high = v.astype(BF16)
    return high, (v - high.astype(F32)).astype(BF16)


def kernel(
    nw, nn,
    counts_in, offs_in, nbr_in, pos_in, vel_in, rad_in, cell_in, gas_in, source_in, before_in,
    p_out, g_out, u_out,
    counts, offs, nbr, pos, vel, rad, cell, gas, source, before, s_in,
    stage, pin, back, drg, gath, grow, con, cols,
    ohx, rlhs, glhs,
    por0, c0, b0, va0, vb0, z0, ym0, yp0, xm0, xp0, dg0, di0,
    por1, b1, va1, vb1, z1, ym1, yp1, xm1, xp1, dg1, di1,
    l1out, l1in, c1p, c1b, l2p, l2b,
    p2, b2, va2, vb2, z2, ci2, co2, xm2, xp2, dg2, di2,
    p3, b3, va3, vb3, z3, y3, xm3, xp3, dg3, di3,
    vfin,
    s_a, r_a, s_c0, r_c0, s_b, r_b, s_l1, r_l1, s_1p, r_1p, s_1b, r_1b, s_2p, r_2p, s_2b, r_2b, s_d, r_d, hello,
):
    w = lax.axis_index("wide")
    n = lax.axis_index("narrow")
    blocks, slots = rad.shape

    def w_ok(d):
        return jnp.logical_and(w + d >= 0, w + d < nw)

    def n_ok(d):
        return jnp.logical_and(n + d >= 0, n + d < nn)

    def there(a, b):
        if b == 0:
            return w_ok(a)
        if a == 0:
            return n_ok(b)
        return jnp.logical_and(w_ok(a), n_ok(b))

    def remote(src, dst, send, recv, to):
        return pltpu.make_async_remote_copy(
            src_ref=src, dst_ref=dst, send_sem=send, recv_sem=recv, device_id=to, device_id_type=MESH
        )

    pending = []

    def start(copies):
        for copy, sends, _ in copies:
            pl.when(sends)(copy.start)
        pending.extend(copies)

    def arrive(copies):
        for copy, _, gets in copies:
            pl.when(gets)(copy.wait_recv)

    given = (counts_in, offs_in, nbr_in, pos_in, vel_in, rad_in, cell_in, gas_in, source_in, before_in)
    taken = (counts, offs, nbr, pos, vel, rad, cell, gas, source, before)
    loads = [pltpu.make_async_copy(a, b, s_in.at[i]) for i, (a, b) in enumerate(zip(given, taken))]
    for i in (0, 1, 5, 4, 6, 8, 9, 3, 2, 7):
        loads[i].start()

    for ref in (pin, back, l1in, c1p, c1b, l2p, l2b, vfin):
        ref[...] = jnp.zeros_like(ref)
    for z in range(24):
        por0[z] = jnp.zeros((24, 128), F32)
        c0[z] = jnp.zeros((24, 128), F32)
    barrier = pltpu.get_barrier_semaphore()
    peers = []
    for d in range(1, SPREAD + 1):
        peers += [(w_ok(d), (w + d, n)), (w_ok(-d), (w - d, n))]
    for k in range(nn):
        peers.append((n != k, (w, k)))
    for a, b in AROUND:
        if a and b:
            peers.append((there(a, b), (w + a, n + b)))
    for ok, to in peers:
        pl.when(ok)(
            functools.partial(pl.semaphore_signal, barrier, inc=1, device_id=to, device_id_type=MESH)
        )

    for i in (0, 1, 5, 4, 6):
        loads[i].wait()

    off = [offs[b] for b in range(blocks)]
    rank = []
    for b in range(blocks):
        r = jnp.int32(0)
        for a in range(b):
            r = r + jnp.where(off[a] == off[b], 1, 0)
        rank.append(r)
    row8 = iota((blocks, slots), 0)
    live_count = jnp.zeros((blocks, slots), jnp.int32)
    for b in range(blocks):
        live_count = jnp.where(row8 == b, counts[b], live_count)
    live = jnp.where(iota((blocks, slots), 1) < live_count, 1.0, 0.0)
    radius = rad[...]
    volume = radius * radius * radius
    parts = [volume * live, vel[0], vel[1], vel[2], cell[...].astype(F32)]
    row16 = iota((16, slots), 0)
    for c, part in enumerate(parts):
        rows = jnp.zeros((16, slots), F32)
        for b in range(blocks):
            key = (off[b] + SPREAD) * CAP + rank[b]
            rows = jnp.where(row16 == key, jnp.broadcast_to(part[b : b + 1], rows.shape), rows)
        for o in range(GROUPS):
            stage[o, c * CAP : (c + 1) * CAP] = rows[o * CAP : (o + 1) * CAP]
    pin[SPREAD] = stage[SPREAD]
    for i in (8, 9):
        loads[i].wait()
    for z in range(8):
        c0[8 + z, 8:16] = source[z] + before[z] * (1.0 / step_duration)

    count = jnp.int32(0)
    for ok, _ in peers:
        count = count + jnp.where(ok, 1, 0)
    pl.semaphore_wait(barrier, count)

    copies_a = []
    for o in range(GROUPS):
        d = o - SPREAD
        if d:
            copies_a.append(
                (remote(stage.at[o], pin.at[o], s_a.at[o], r_a.at[o], (w + d, n)), w_ok(d), w_ok(-d))
            )
    start(copies_a)

    def block_copies(ref, corner, send, recv):
        made = []
        for i, (a, b) in enumerate(AROUND):
            low, high = 8, 16
            if a == 1:
                low = 16 - corner[0 if b == 0 else 1]
            if a == -1:
                high = 8 + corner[0 if b == 0 else 1]
            made.append(
                (
                    remote(
                        ref.at[low:high, 8:16],
                        ref.at[low - 8 * a : high - 8 * a, 8 * (1 - b) : 8 * (2 - b)],
                        send.at[i], recv.at[i], (w + a, n + b),
                    ),
                    there(a, b),
                    there(-a, -b),
                )
            )
        return made

    copies_c0 = block_copies(c0, (6, 6), s_c0, r_c0)

    for i in (3, 2, 7):
        loads[i].wait()

    bar = jnp.concatenate(
        [pos[0], pos[1], pos[2], jnp.where(live > 0.0, radius, -1000.0), jnp.zeros((128 - 4 * blocks, slots), F32)],
        axis=0,
    ).T
    for c in range(4):
        for b in range(blocks):
            k = c * blocks + b
            cols[c, b] = jnp.broadcast_to(bar[:, k : k + 1], (slots, slots))
    factor = stiffness / (slots * 7)

    def contact_of(g, carry):
        own = [jnp.broadcast_to(pos[c, pl.ds(g, 1)], (8, slots)) for c in range(3)]
        own_rad = jnp.broadcast_to(rad[pl.ds(g, 1)], (8, slots))
        total = [jnp.zeros((8, slots), F32) for _ in range(3)]
        for k in range(7):
            other = g if k == 6 else nbr[g, k]
            for j in range(0, slots, 8):
                apart = [own[c] - cols[c, other, j : j + 8] for c in range(3)]
                square = apart[0] * apart[0] + apart[1] * apart[1]
                square = square + (apart[2] * apart[2] + softening * softening)
                inverse = lax.rsqrt(square)
                weight = jnp.maximum((own_rad + cols[3, other, j : j + 8]) * inverse - 1.0, 0.0)
                total = [total[c] + apart[c] * weight for c in range(3)]
        for c in range(3):
            con[c, pl.ds(g, 1)] = jnp.sum(total[c], axis=0, keepdims=True) * factor
        return carry

    lax.fori_loop(0, blocks // 2, contact_of, 0)
    start(copies_c0)
    lax.fori_loop(blocks // 2, blocks, contact_of, 0)

    arrive(copies_a)

    for i, d in enumerate((2 * SPREAD, -2 * SPREAD)):
        pl.when(w_ok(d))(
            functools.partial(
                pl.semaphore_signal, hello.at[i], inc=1, device_id=(w + d, n), device_id_type=MESH
            )
        )

    zy_iota = iota((64, slots), 0)
    x_iota = iota((128, slots), 0)

    def cells_of(o, r):
        where = pin[o, 4 * CAP + r : 4 * CAP + r + 1].astype(jnp.int32)
        return where >> 7, where & 127

    both = jnp.zeros((128, 128), F32)
    for o in range(GROUPS):
        ones, values = [], []
        for r in range(CAP):
            zy, x = cells_of(o, r)
            ones.append(jnp.where(jnp.broadcast_to(x, x_iota.shape) == x_iota, 1.0, 0.0).astype(BF16))
            hit = jnp.broadcast_to(zy, zy_iota.shape) == zy_iota
            here = jnp.where(hit, jnp.broadcast_to(pin[o, r : r + 1], zy_iota.shape), 0.0)
            values.append(jnp.concatenate(halves(here), axis=0))
        one = jnp.concatenate(ones, axis=1)
        at = slice(o * CAP * slots, (o + 1) * CAP * slots)
        ohx[0:128, at] = one
        ohx[128:256, at] = one
        both = both + lax.dot_general(
            jnp.concatenate(values, axis=1), one, (((1,), (1,)), ((), ())), preferred_element_type=F32
        )
    solid = both[0:64] + both[64:128]
    voidage = 1.0 - solid_most * solid / (1.0 + solid)
    for z in range(8):
        por0[8 + z, 8:16] = voidage[8 * z : 8 * z + 8]
    copies_b = block_copies(por0, (8, 6), s_b, r_b)
    start(copies_b)

    lane = iota((8, 128), 1)
    lane4 = iota((1, 128), 1) & 3

    def coarser(pairs, s):
        return pair_sum(pair_sum(pairs[0] + pairs[1], s, 0), s, 1) * 0.125

    def packed(cells):
        rows = [cells[0][0:1], cells[0][4:5], cells[1][0:1], cells[1][4:5]]
        row = rows[3]
        for k in range(3):
            row = jnp.where(lane4 == k, rows[k], row)
        return row

    finer = [coarser((voidage[16 * i : 16 * i + 8], voidage[16 * i + 8 : 16 * i + 16]), 1) for i in range(4)]
    c1p[n] = packed([coarser((finer[0], finer[1]), 2), coarser((finer[2], finer[3]), 2)])


    def row_copies(ref, send, recv):
        return [
            (
                remote(ref.at[n], ref.at[n], send.at[d], recv.at[d], (w, lax.rem(n + d, nn))),
                jnp.bool_(True),
                jnp.bool_(True),
            )
            for d in range(1, nn)
        ]

    def start_rows(copies):
        for copy, _, _ in copies:
            copy.start()
        pending.extend(copies)

    def arrive_rows(copies):
        for copy, _, _ in copies:
            copy.wait_recv()

    def slab_copies(ref, reach, send, recv):
        made = []
        for d in [s * k for k in range(1, reach + 1) for s in (1, -1)]:
            i = d + REACH
            made.append(
                (
                    remote(ref.at[REACH], ref.at[REACH - d], send.at[i], recv.at[i], (w + d, n)),
                    w_ok(d),
                    w_ok(-d),
                )
            )
        return made

    def rows_to_slab(ref):
        row = iota((8, 128), 0)
        slab = jnp.zeros((8, 128), F32)
        for k in range(nn):
            slab = jnp.where(row == k, jnp.broadcast_to(ref[k], (8, 128)), slab)
        return slab

    copies_1p = row_copies(c1p, s_1p, r_1p)
    start_rows(copies_1p)

    def fill_gather(f, values):
        high, low = halves(values)
        glhs[f * 64 : f * 64 + 64, 0:128] = high
        glhs[f * 64 : f * 64 + 64, 128:256] = low

    def gather(fields):
        def one(o, carry):
            width = CAP * slots
            at = pl.ds(pl.multiple_of(o * width, slots), width)
            found = jnp.dot(glhs[0 : 64 * fields], ohx[:, at], preferred_element_type=F32)
            for r in range(CAP):
                zy, _ = cells_of(o, r)
                hit = jnp.broadcast_to(zy, zy_iota.shape) == zy_iota
                for f in range(fields):
                    gath[o, f * CAP + r : f * CAP + r + 1] = jnp.sum(
                        jnp.where(hit, found[64 * f : 64 * f + 64, r * slots : (r + 1) * slots], 0.0),
                        axis=0, keepdims=True,
                    )
            return carry

        lax.fori_loop(0, GROUPS, one, 0)

    for f in range(3):
        fill_gather(f, gas[f].reshape(64, 128))
    fill_gather(3, voidage)
    gather(4)
    for o in range(GROUPS):
        slip = [gath[o, c * CAP : (c + 1) * CAP] - pin[o, (1 + c) * CAP : (2 + c) * CAP] for c in range(3)]
        speed = jnp.sqrt(slip[0] * slip[0] + slip[1] * slip[1] + slip[2] * slip[2])
        held = gath[o, 3 * CAP : 4 * CAP]
        scale = pin[o, 0:CAP] * (drag_base + drag_slope * speed) * jnp.exp(-void_power * jnp.log(held))
        for c in range(3):
            drg[o, c * CAP : (c + 1) * CAP] = scale * slip[c]

    arrive_rows(copies_1p)
    l2p[REACH] = rows_to_slab(c1p)
    for i, d in enumerate((2 * SPREAD, -2 * SPREAD)):
        pl.when(w_ok(-d))(functools.partial(pl.semaphore_wait, hello.at[i], 1))
    copies_2p = slab_copies(l2p, REACH, s_2p, r_2p)
    start(copies_2p)

    def spread_drag(o, carry):
        for r in range(CAP):
            at = pl.ds(pl.multiple_of((o * CAP + r) * slots, slots), slots)
            zy, _ = cells_of(o, r)
            hit = jnp.broadcast_to(zy, zy_iota.shape) == zy_iota
            for c in range(3):
                row = drg[o, c * CAP + r : c * CAP + r + 1]
                high, low = halves(jnp.where(hit, jnp.broadcast_to(row, zy_iota.shape), 0.0))
                rlhs[128 * c : 128 * c + 64, at] = high
                rlhs[128 * c + 64 : 128 * c + 128, at] = low
        return carry

    lax.fori_loop(0, GROUPS, spread_drag, 0)
    sums = lax.dot_general(
        rlhs[...], ohx[0:128], (((1,), (1,)), ((), ())), preferred_element_type=F32
    )
    for c in range(3):
        onto = sums[128 * c : 128 * c + 64] + sums[128 * c + 64 : 128 * c + 128]
        grow[c] = gas[c].reshape(64, 128) - step_duration * onto / voidage

    arrive(copies_c0)
    arrive(copies_b)

    row24 = iota((24, 128), 0)
    inside_y = jnp.logical_and(
        jnp.logical_or(row24 >= 8, n > 0), jnp.logical_or(row24 < 16, n < nn - 1)
    )
    inside_y = jnp.where(inside_y, 1, 0)

    def inside(block):
        ok = jnp.logical_and(w + block >= 0, w + block < nw)
        return inside_y * jnp.where(ok, 1, 0) > 0

    def coefs(por, z, s, half, layers, cz, cym, cyp, cxm, cxp, dg, di):
        here = por[z]
        zm = half * (here + por[z - 1])
        zp = half * (here + por[z + 1])
        ym = half * (here + turn(here, s, 0))
        yp = half * (here + turn(here, -s, 0))
        xm = half * (here + lanes_before(here, s))
        xp = half * (here + lanes_after(here, s))
        diagonal = zm + zp + ym + yp + xm + xp
        lanes = iota(here.shape, 1)
        cz[z] = zm
        cym[z] = ym
        cyp[z] = yp
        cxm[z] = jnp.where(lanes >= s, xm, 0.0)
        cxp[z] = jnp.where(lanes < 128 - s, xp, 0.0)
        dg[z] = diagonal
        scaled = jnp.where(inside(z // layers - 1), relax_weight / diagonal, 0.0)
        di[z] = scaled
        return scaled

    def residual_at(v, b, z, s, cz, cym, cyp, cxm, cxp, dg):
        here = v[z]
        beside = cz[z] * v[z - 1] + cz[z + 1] * v[z + 1]
        beside = beside + (cym[z] * turn(here, s, 0) + cyp[z] * turn(here, -s, 0))
        beside = beside + (cxm[z] * turn(here, s, 1) + cxp[z] * turn(here, -s, 1))
        return here, (b[z] - dg[z] * here) + beside

    def sweep(v, to, b, z, s, cz, cym, cyp, cxm, cxp, dg, di):
        here, residual = residual_at(v, b, z, s, cz, cym, cyp, cxm, cxp, dg)
        to[z] = here + di[z] * residual

    level0 = (z0, ym0, yp0, xm0, xp0, dg0)
    level1 = (z1, ym1, yp1, xm1, xp1, dg1)

    def first0(z):
        b = c0[z] - por0[z] * (1.0 / step_duration)
        b0[z] = b
        va0[z] = coefs(por0, z, 1, 0.5, 8, *level0, di0) * b

    zloop(2, 22, first0)
    zloop(3, 21, lambda z: sweep(va0, vb0, b0, z, 1, *level0, di0))

    def por1_of(i):
        por1[i] = coarser((por0[2 * i], por0[2 * i + 1]), 1)

    zloop(0, 12, por1_of)

    def down0(i):
        _, low = residual_at(vb0, b0, 2 * i, 1, *level0)
        _, high = residual_at(vb0, b0, 2 * i + 1, 1, *level0)
        b1[i] = coarser((low, high), 1)

    zloop(2, 10, down0, 2)
    zloop(1, 11, lambda i: coefs(por1, i, 2, 0.125, 4, *level1, di1), 5)
    z1[11] = 0.125 * (por1[11] + por1[10])

    def first1(i):
        va1[i] = di1[i] * b1[i]

    zloop(2, 10, first1, 8)
    zloop(3, 9, lambda i: sweep(va1, vb1, b1, i, 2, *level1, di1), 6)
    left = [residual_at(vb1, b1, i, 2, *level1)[1][8:16] for i in range(4, 8)]
    c1b[n] = packed([coarser((left[0], left[1]), 2), coarser((left[2], left[3]), 2)])
    copies_1b = row_copies(c1b, s_1b, r_1b)
    start_rows(copies_1b)

    even_lane = (lane & 1) == 0
    row = iota((8, 128), 0)
    even_row = (row & 1) == 0
    for k in range(2):
        i = 4 + 2 * k
        right = jnp.where(even_lane, b1[i, 8:16], b1[i + 1, 8:16])
        iterate = jnp.where(even_lane, vb1[i, 8:16], vb1[i + 1, 8:16])
        l1out[k] = jnp.where(even_row, right, iterate)
    copies_l1 = [
        (
            remote(l1out, l1in.at[1 - a, 1 - b], s_l1.at[i], r_l1.at[i], (w + a, n + b)),
            there(a, b),
            there(-a, -b),
        )
        for i, (a, b) in enumerate(AROUND)
    ]
    start(copies_l1)

    arrive(copies_2p)

    def unpack4(slab):
        cells = []
        for k in range(4):
            one = jnp.where((lane & 3) == k, slab, 0.0)
            cells.append(pair_sum(pair_sum(one, 1, 1), 2, 1))
        return cells

    def unpack_por(k):
        cells = unpack4(l2p[k])
        for q in range(4):
            p2[2 * k + q // 2, q % 2] = cells[q]
        p3[k] = pair_sum((cells[0] + cells[1]) + (cells[2] + cells[3]), 4, 1) * 0.125

    zloop(0, 2 * REACH + 1, unpack_por, 5)
    real_row = jnp.where(row < nn, 1, 0)

    def inside_coarse(block):
        ok = jnp.logical_and(w + block >= 0, w + block < nw)
        return real_row * jnp.where(ok, 1, 0) > 0

    def coefs2(j):
        half = 0.5 * 0.25**2
        even, odd = p2[j, 0], p2[j, 1]
        inner = half * (even + odd)
        ci2[j] = inner
        outer = half * (even + rows_before(odd, 1))
        co2[j] = outer
        outer_odd = half * (odd + rows_after(even, 1))
        ok = inside_coarse(j // 2 - REACH)
        for y, here in enumerate((even, odd)):
            zm = half * (here + p2[j - 1, y])
            zp = half * (here + p2[j + 1, y])
            xm = half * (here + lanes_before(here, 4))
            xp = half * (here + lanes_after(here, 4))
            diagonal = zm + zp + inner + (outer_odd if y else outer) + xm + xp
            z2[j, y] = zm
            xm2[j, y] = jnp.where(lane >= 4, xm, 0.0)
            xp2[j, y] = jnp.where(lane < 124, xp, 0.0)
            dg2[j, y] = diagonal
            di2[j, y] = jnp.where(ok, relax_weight / diagonal, 0.0)

    zloop(1, 4 * REACH + 1, coefs2)

    def coefs3(k):
        half = 0.5 * 0.25**3
        here = p3[k]
        zm = half * (here + p3[k - 1])
        zp = half * (here + p3[k + 1])
        ym = half * (here + rows_before(here, 1))
        yp = half * (here + rows_after(here, 1))
        xm = half * (here + lanes_before(here, 8))
        xp = half * (here + lanes_after(here, 8))
        diagonal = zm + zp + ym + yp + xm + xp
        z3[k] = zm
        y3[k] = ym
        xm3[k] = jnp.where(lane >= 8, xm, 0.0)
        xp3[k] = jnp.where(lane < 120, xp, 0.0)
        dg3[k] = diagonal
        di3[k] = jnp.where(inside_coarse(k - REACH), relax_weight / diagonal, 0.0)

    zloop(1, 2 * REACH, coefs3)

    arrive_rows(copies_1b)
    l2b[REACH] = rows_to_slab(c1b)
    copies_2b = slab_copies(l2b, RHS_REACH, s_2b, r_2b)
    start(copies_2b)

    arrive(copies_l1)
    for a, b in AROUND:
        for k in range(2):
            both_layers = l1in[1 + a, 1 + b, k]
            for q in range(2):
                if q == 0:
                    layer = jnp.where(even_lane, both_layers, turn(both_layers, 1, 1))
                else:
                    layer = jnp.where(even_lane, turn(both_layers, -1, 1), both_layers)
                i = 4 * (1 + a) + 2 * k + q
                at = slice(8 * (1 + b), 8 * (2 + b))
                b1[i, at] = jnp.where(even_row, layer, turn(layer, 1, 0))
                vb1[i, at] = jnp.where(even_row, turn(layer, -1, 0), layer)

    def residual2(v, j):
        even, odd = v[j, 0], v[j, 1]
        outer = co2[j]
        made = []
        for y, here in enumerate((even, odd)):
            beside = z2[j, y] * v[j - 1, y] + z2[j + 1, y] * v[j + 1, y]
            if y == 0:
                beside = beside + (ci2[j] * odd + outer * rows_before(odd, 1))
            else:
                beside = beside + (ci2[j] * even + rows_after(outer, 1) * rows_after(even, 1))
            beside = beside + (xm2[j, y] * turn(here, 4, 1) + xp2[j, y] * turn(here, -4, 1))
            made.append((here, (b2[j, y] - dg2[j, y] * here) + beside))
        return made

    def sweep2(v, to):
        def at(j):
            for y, (here, residual) in enumerate(residual2(v, j)):
                to[j, y] = here + di2[j, y] * residual

        return at

    def residual3(v, k):
        here = v[k]
        beside = z3[k] * v[k - 1] + z3[k + 1] * v[k + 1]
        beside = beside + (y3[k] * rows_before(here, 1) + rows_after(y3[k], 1) * rows_after(here, 1))
        beside = beside + (xm3[k] * turn(here, 8, 1) + xp3[k] * turn(here, -8, 1))
        return here, (b3[k] - dg3[k] * here) + beside

    def sweep3(v, to):
        def at(k):
            here, residual = residual3(v, k)
            to[k] = here + di3[k] * residual

        return at

    arrive(copies_2b)

    def first2(k):
        cells = unpack4(l2b[k])
        for q in range(4):
            j, y = 2 * k + q // 2, q % 2
            b2[j, y] = cells[q]
            va2[j, y] = di2[j, y] * cells[q]

    zloop(1, 2 * REACH, first2)
    zloop(3, 27, sweep2(va2, vb2))

    def down2(k):
        low = residual2(vb2, 2 * k)
        high = residual2(vb2, 2 * k + 1)
        b = pair_sum((low[0][1] + low[1][1]) + (high[0][1] + high[1][1]), 4, 1) * 0.125
        b3[k] = b
        va3[k] = di3[k] * b

    zloop(2, 13, down2, 3)
    zloop(3, 12, sweep3(va3, vb3), 9)
    zloop(4, 11, sweep3(vb3, va3), 7)
    zloop(5, 10, sweep3(va3, vb3), 5)

    def up2(k):
        for q in range(4):
            j, y = 2 * k + q // 2, q % 2
            va2[j, y] = vb2[j, y] + vb3[k]

    zloop(5, 10, up2, 5)
    zloop(11, 19, sweep2(va2, vb2))
    for j in range(12, 18):
        for y, (here, residual) in enumerate(residual2(vb2, j)):
            vfin[j - 12, y, 8:16] = here + di2[j, y] * residual

    low_row = row < 4
    for q in range(6):
        for b in range(3):
            cells = [
                jnp.broadcast_to(vfin[q, y, pl.ds(7 + n + b, 1)], (8, 128)) for y in range(2)
            ]
            step = jnp.where(low_row, cells[0], cells[1])
            at = slice(8 * b, 8 * b + 8)
            for i in (2 * q, 2 * q + 1):
                va1[i, at] = vb1[i, at] + step
    zloop(1, 11, lambda i: sweep(va1, vb1, b1, i, 2, *level1, di1), 5)
    zloop(2, 10, lambda i: sweep(vb1, va1, b1, i, 2, *level1, di1))

    def up0(i):
        step = va1[i]
        va0[2 * i] = vb0[2 * i] + step
        va0[2 * i + 1] = vb0[2 * i + 1] + step

    zloop(2, 10, up0)
    zloop(6, 18, lambda z: sweep(va0, vb0, b0, z, 1, *level0, di0))
    zloop(7, 17, lambda z: sweep(vb0, va0, b0, z, 1, *level0, di0), 5)

    for z in range(8):
        whole = va0[8 + z]
        here = whole[8:16]
        slopes = [
            0.5 * (va0[9 + z, 8:16] - va0[7 + z, 8:16]),
            0.5 * (turn(whole, -1, 0)[8:16] - turn(whole, 1, 0)[8:16]),
            0.5 * (lanes_after(here, 1) - lanes_before(here, 1)),
        ]
        for c in range(3):
            g_out[c, z] = slopes[c]
            high, low = halves(slopes[c])
            glhs[64 * c + 8 * z : 64 * c + 8 * z + 8, 0:128] = high
            glhs[64 * c + 8 * z : 64 * c + 8 * z + 8, 128:256] = low
    gather(3)
    for o in range(GROUPS):
        for c in range(3):
            at = slice(c * CAP, (c + 1) * CAP)
            drg[o, at] = drg[o, at] - pin[o, 0:CAP] * gath[o, at]
    copies_d = []
    for o in range(GROUPS):
        d = o - SPREAD
        if d:
            copies_d.append(
                (remote(drg.at[o], back.at[o], s_d.at[o], r_d.at[o], (w - d, n)), w_ok(-d), w_ok(d))
            )
    start(copies_d)
    back[SPREAD] = drg[SPREAD]
    for z in range(8):
        p_out[z] = va0[8 + z, 8:16]
        for c in range(3):
            g_out[c, z] = grow[c, 8 * z : 8 * z + 8] - step_duration * g_out[c, z]
    for copy, sends, _ in pending[: -len(copies_d)]:
        pl.when(sends)(copy.wait_send)
    fluid_scale = live * step_duration / (particle_density * volume)
    moved = [
        live * (vel[c] + (step_duration * gravity if c == 0 else 0.0)) + fluid_scale * con[c] * live
        for c in range(3)
    ]
    arrive(copies_d)
    for c in range(3):
        fluid = jnp.zeros((blocks, slots), F32)
        for b in range(blocks):
            one = back[off[b] + SPREAD, pl.ds(c * CAP + rank[b], 1)]
            fluid = jnp.where(row8 == b, jnp.broadcast_to(one, fluid.shape), fluid)
        u_out[c] = moved[c] + fluid_scale * fluid

    for copy, sends, _ in copies_d:
        pl.when(sends)(copy.wait_send)


def put_out(p, g, u, p_out, g_out, u_out):
    p_out[...] = p[...]
    g_out[...] = g[...]
    u_out[...] = u[...]


def local(nw, nn, position, velocity, radius, count, cell, offset, neighbours, gas, source, before):
    vmem = pl.BlockSpec(memory_space=pltpu.VMEM)
    hbm = pl.BlockSpec(memory_space=pltpu.HBM)

    def ram(*shape, dtype=F32):
        return pltpu.VMEM(shape, dtype)

    dma = pltpu.SemaphoreType.DMA
    block = ram(24, 24, 128)
    block1 = ram(12, 24, 128)
    tall = 2 * REACH + 1
    coarse2 = ram(2 * tall, 2, 8, 128)
    coarse2y = ram(2 * tall, 8, 128)
    coarse3 = ram(tall, 8, 128)
    particles = SLOTS * radius.shape[1]
    given = (count, offset, neighbours, position, velocity, radius, cell, gas, source, before)
    scratch = [
        *[pltpu.SMEM(a.shape, a.dtype) for a in given[:3]],
        *[pltpu.VMEM(a.shape, a.dtype) for a in given[3:]],
        dma((len(given),)),
        *[ram(GROUPS, 16, 128)] * 5,
        ram(3, 64, 128),
        ram(3, 8, 128),
        ram(4, 8, 128, 128),
        ram(256, particles, dtype=BF16),
        ram(384, particles, dtype=BF16),
        ram(256, 256, dtype=BF16),
        *[block] * 12,
        *[block1] * 11,
        ram(2, 8, 128),
        ram(3, 3, 2, 8, 128),
        ram(8, 1, 128),
        ram(8, 1, 128),
        coarse3,
        coarse3,
        *[coarse2] * 5,
        coarse2y,
        coarse2y,
        *[coarse2] * 4,
        *[coarse3] * 10,
        ram(6, 2, 24, 128),
        *[dma((GROUPS,))] * 2,
        *[dma((8,))] * 6,
        *[dma((8,))] * 4,
        *[dma((tall,))] * 4,
        *[dma((GROUPS,))] * 2,
        pltpu.SemaphoreType.REGULAR((2,)),
    ]
    results = (
        jax.ShapeDtypeStruct(source.shape, F32),
        jax.ShapeDtypeStruct(gas.shape, F32),
        jax.ShapeDtypeStruct(velocity.shape, F32),
    )
    made = pl.pallas_call(
        functools.partial(kernel, nw, nn),
        out_shape=results,
        in_specs=[hbm] * len(given),
        out_specs=(vmem, vmem, vmem),
        scratch_shapes=scratch,
        compiler_params=pltpu.CompilerParams(
            collective_id=0, has_side_effects=True, vmem_limit_bytes=24 << 20
        ),
        name="bed_step",
    )(*[pltpu.with_memory_space_constraint(a, pltpu.HBM) for a in given])
    return pl.pallas_call(
        put_out,
        out_shape=results,
        in_specs=[vmem] * 3,
        out_specs=(vmem, vmem, vmem),
        compiler_params=pltpu.CompilerParams(vmem_limit_bytes=8 << 20),
        name="put_out",
    )(*made)


def solution(mesh):
    placed = (
        P(None, ("wide", "narrow"), None),
        P(None, ("wide", "narrow"), None),
        P(("wide", "narrow"), None),
        P(("wide", "narrow")),
        P(("wide", "narrow"), None),
        P(("wide", "narrow")),
        P(("wide", "narrow"), None),
        P(None, "wide", "narrow", None),
        P("wide", "narrow", None),
        P("wide", "narrow", None),
    )
    return jax.shard_map(
        functools.partial(local, mesh.shape["wide"], mesh.shape["narrow"]),
        mesh=mesh,
        in_specs=placed,
        out_specs=(
            P("wide", "narrow", None),
            P(None, "wide", "narrow", None),
            P(None, ("wide", "narrow"), None),
        ),
        check_vma=False,
    )
```

```python
import functools

import jax
import jax.numpy as jnp
from jax import lax
from jax.experimental import pallas as pl
from jax.experimental.pallas import tpu as pltpu
from jax.sharding import PartitionSpec as P

SPREAD = 2
CAP = 3
GROUPS = 2 * SPREAD + 1
SLOTS = GROUPS * CAP
REACH = 7
RHS_REACH = 6

relax_weight = 0.8
solid_most = 0.6
void_power = 2.65
drag_base = 0.5
drag_slope = 0.5
stiffness = 16.0
softening = 0.1
particle_density = 2.0
step_duration = 0.25
gravity = -1.0

F32 = jnp.float32
BF16 = jnp.bfloat16
MESH = pl.DeviceIdType.MESH
EDGES = [(a, b) for a in (-1, 1) for b in (-1, 1)]
AROUND = [(a, b) for a in (-1, 0, 1) for b in (-1, 0, 1) if (a, b) != (0, 0)]


def iota(shape, dim):
    return lax.broadcasted_iota(jnp.int32, shape, dim)


def zloop(low, high, body, step=4):
    whole = (high - low) // step
    if whole > 1:

        def chunk(i, carry):
            for k in range(step):
                body(low + i * step + k)
            return carry

        lax.fori_loop(0, whole, chunk, 0)
    else:
        whole = 0
    for z in range(low + whole * step, high):
        body(z)


def turn(v, shift, axis):
    return pltpu.roll(v, shift % v.shape[axis], axis)


def lanes_before(v, s):
    return jnp.where(iota(v.shape, 1) >= s, turn(v, s, 1), 0.0)


def lanes_after(v, s):
    return jnp.where(iota(v.shape, 1) < v.shape[1] - s, turn(v, -s, 1), 0.0)


def rows_before(v, s):
    return jnp.where(iota(v.shape, 0) >= s, turn(v, s, 0), 0.0)


def rows_after(v, s):
    return jnp.where(iota(v.shape, 0) < v.shape[0] - s, turn(v, -s, 0), 0.0)


def pair_sum(v, s, axis):
    low = (iota(v.shape, axis) & s) == 0
    return v + jnp.where(low, turn(v, -s, axis), turn(v, s, axis))


def halves(v):
    high = v.astype(BF16)
    return high, (v - high.astype(F32)).astype(BF16)


def kernel(
    nw, nn,
    counts_in, offs_in, nbr_in, pos_in, vel_in, rad_in, cell_in, gas_in, source_in, before_in,
    p_out, g_out, u_out,
    counts, offs, nbr, pos, vel, rad, cell, gas, source, before, s_in,
    stage, pin, back, drg, gath, grow, con, cols,
    ohx, rlhs, glhs,
    por0, c0, b0, va0, vb0, z0, ym0, yp0, xm0, xp0, dg0, di0,
    por1, b1, va1, vb1, z1, ym1, yp1, xm1, xp1, dg1, di1,
    edge_out, edge_in, l1out, l1in, c1p, c1b, l2p, l2b,
    p2, b2, va2, vb2, z2, ci2, co2, xm2, xp2, dg2, di2,
    p3, b3, va3, vb3, z3, y3, xm3, xp3, dg3, di3,
    vfin,
    s_a, r_a, s_c0, r_c0, s_b, r_b, s_l1, r_l1, s_1p, r_1p, s_1b, r_1b, s_2p, r_2p, s_2b, r_2b, s_d, r_d, hello,
):
    w = lax.axis_index("wide")
    n = lax.axis_index("narrow")
    blocks, slots = rad.shape

    def w_ok(d):
        return jnp.logical_and(w + d >= 0, w + d < nw)

    def n_ok(d):
        return jnp.logical_and(n + d >= 0, n + d < nn)

    def there(a, b):
        if b == 0:
            return w_ok(a)
        if a == 0:
            return n_ok(b)
        return jnp.logical_and(w_ok(a), n_ok(b))

    def remote(src, dst, send, recv, to):
        return pltpu.make_async_remote_copy(
            src_ref=src, dst_ref=dst, send_sem=send, recv_sem=recv, device_id=to, device_id_type=MESH
        )

    pending = []

    def start(copies):
        for copy, sends, _ in copies:
            pl.when(sends)(copy.start)
        pending.extend(copies)

    def arrive(copies):
        for copy, _, gets in copies:
            pl.when(gets)(copy.wait_recv)

    given = (counts_in, offs_in, nbr_in, pos_in, vel_in, rad_in, cell_in, gas_in, source_in, before_in)
    taken = (counts, offs, nbr, pos, vel, rad, cell, gas, source, before)
    loads = [pltpu.make_async_copy(a, b, s_in.at[i]) for i, (a, b) in enumerate(zip(given, taken))]
    for i in (0, 1, 5, 4, 6, 8, 9, 3, 2, 7):
        loads[i].start()

    for ref in (pin, back, edge_in, l1in, c1p, c1b, l2p, l2b, vfin):
        ref[...] = jnp.zeros_like(ref)
    for z in range(24):
        por0[z] = jnp.zeros((24, 128), F32)
        c0[z] = jnp.zeros((24, 128), F32)
    barrier = pltpu.get_barrier_semaphore()
    peers = []
    for d in range(1, SPREAD + 1):
        peers += [(w_ok(d), (w + d, n)), (w_ok(-d), (w - d, n))]
    for k in range(nn):
        peers.append((n != k, (w, k)))
    for a, b in AROUND:
        if a and b:
            peers.append((there(a, b), (w + a, n + b)))
    for ok, to in peers:
        pl.when(ok)(
            functools.partial(pl.semaphore_signal, barrier, inc=1, device_id=to, device_id_type=MESH)
        )

    for i in (0, 1, 5, 4, 6):
        loads[i].wait()

    off = [offs[b] for b in range(blocks)]
    rank = []
    for b in range(blocks):
        r = jnp.int32(0)
        for a in range(b):
            r = r + jnp.where(off[a] == off[b], 1, 0)
        rank.append(r)
    row8 = iota((blocks, slots), 0)
    live_count = jnp.zeros((blocks, slots), jnp.int32)
    for b in range(blocks):
        live_count = jnp.where(row8 == b, counts[b], live_count)
    live = jnp.where(iota((blocks, slots), 1) < live_count, 1.0, 0.0)
    radius = rad[...]
    volume = radius * radius * radius
    parts = [volume * live, vel[0], vel[1], vel[2], cell[...].astype(F32)]
    row16 = iota((16, slots), 0)
    for c, part in enumerate(parts):
        rows = jnp.zeros((16, slots), F32)
        for b in range(blocks):
            key = (off[b] + SPREAD) * CAP + rank[b]
            rows = jnp.where(row16 == key, jnp.broadcast_to(part[b : b + 1], rows.shape), rows)
        for o in range(GROUPS):
            stage[o, c * CAP : (c + 1) * CAP] = rows[o * CAP : (o + 1) * CAP]
    pin[SPREAD] = stage[SPREAD]
    for i in (8, 9):
        loads[i].wait()
    for z in range(8):
        c0[8 + z, 8:16] = source[z] + before[z] * (1.0 / step_duration)

    count = jnp.int32(0)
    for ok, _ in peers:
        count = count + jnp.where(ok, 1, 0)
    pl.semaphore_wait(barrier, count)

    copies_a = []
    for o in range(GROUPS):
        d = o - SPREAD
        if d:
            copies_a.append(
                (remote(stage.at[o], pin.at[o], s_a.at[o], r_a.at[o], (w + d, n)), w_ok(d), w_ok(-d))
            )
    start(copies_a)

    def block_copies(ref, layers, send, recv, corners=True):
        made = []
        for i, (a, b) in enumerate(AROUND):
            if a and b and not corners:
                continue
            low, high = 8, 16
            if a == 1:
                low = 16 - layers
            if a == -1:
                high = 8 + layers
            made.append(
                (
                    remote(
                        ref.at[low:high, 8:16],
                        ref.at[low - 8 * a : high - 8 * a, 8 * (1 - b) : 8 * (2 - b)],
                        send.at[i], recv.at[i], (w + a, n + b),
                    ),
                    there(a, b),
                    there(-a, -b),
                )
            )
        return made

    copies_c0 = block_copies(c0, 6, s_c0, r_c0)

    for i in (3, 2, 7):
        loads[i].wait()

    bar = jnp.concatenate(
        [pos[0], pos[1], pos[2], jnp.where(live > 0.0, radius, -1000.0), jnp.zeros((128 - 4 * blocks, slots), F32)],
        axis=0,
    ).T
    for c in range(4):
        for b in range(blocks):
            k = c * blocks + b
            cols[c, b] = jnp.broadcast_to(bar[:, k : k + 1], (slots, slots))
    factor = stiffness / (slots * 7)

    def contact_of(g, carry):
        own = [jnp.broadcast_to(pos[c, pl.ds(g, 1)], (8, slots)) for c in range(3)]
        own_rad = jnp.broadcast_to(rad[pl.ds(g, 1)], (8, slots))
        total = [jnp.zeros((8, slots), F32) for _ in range(3)]
        for k in range(7):
            other = g if k == 6 else nbr[g, k]
            for j in range(0, slots, 8):
                apart = [own[c] - cols[c, other, j : j + 8] for c in range(3)]
                square = apart[0] * apart[0] + apart[1] * apart[1]
                square = square + (apart[2] * apart[2] + softening * softening)
                inverse = lax.rsqrt(square)
                weight = jnp.maximum((own_rad + cols[3, other, j : j + 8]) * inverse - 1.0, 0.0)
                total = [total[c] + apart[c] * weight for c in range(3)]
        for c in range(3):
            con[c, pl.ds(g, 1)] = jnp.sum(total[c], axis=0, keepdims=True) * factor
        return carry

    lax.fori_loop(0, blocks // 2, contact_of, 0)
    start(copies_c0)
    lax.fori_loop(blocks // 2, blocks, contact_of, 0)

    arrive(copies_a)

    for i, d in enumerate((2 * SPREAD, -2 * SPREAD)):
        pl.when(w_ok(d))(
            functools.partial(
                pl.semaphore_signal, hello.at[i], inc=1, device_id=(w + d, n), device_id_type=MESH
            )
        )

    zy_iota = iota((64, slots), 0)
    x_iota = iota((128, slots), 0)

    def cells_of(o, r):
        where = pin[o, 4 * CAP + r : 4 * CAP + r + 1].astype(jnp.int32)
        return where >> 7, where & 127

    both = jnp.zeros((128, 128), F32)
    for o in range(GROUPS):
        ones, values = [], []
        for r in range(CAP):
            zy, x = cells_of(o, r)
            ones.append(jnp.where(jnp.broadcast_to(x, x_iota.shape) == x_iota, 1.0, 0.0).astype(BF16))
            hit = jnp.broadcast_to(zy, zy_iota.shape) == zy_iota
            here = jnp.where(hit, jnp.broadcast_to(pin[o, r : r + 1], zy_iota.shape), 0.0)
            values.append(jnp.concatenate(halves(here), axis=0))
        one = jnp.concatenate(ones, axis=1)
        at = slice(o * CAP * slots, (o + 1) * CAP * slots)
        ohx[0:128, at] = one
        ohx[128:256, at] = one
        both = both + lax.dot_general(
            jnp.concatenate(values, axis=1), one, (((1,), (1,)), ((), ())), preferred_element_type=F32
        )
    solid = both[0:64] + both[64:128]
    voidage = 1.0 - solid_most * solid / (1.0 + solid)
    for z in range(8):
        por0[8 + z, 8:16] = voidage[8 * z : 8 * z + 8]
    copies_b = block_copies(por0, 8, s_b, r_b, corners=False)
    start(copies_b)

    row = iota((8, 128), 0)
    tiles = ((1, 6, 6), (2, 5, 6), (3, 4, 4))

    def kept(b, rows):
        return row >= 8 - rows if b == 1 else row < rows

    copies_e = []
    for e, (a, b) in enumerate(EDGES):
        for k, (one, two, rows) in enumerate(tiles):
            near, far = [por0[16 - d if a == 1 else 7 + d, 8:16] for d in (one, two)]
            shift = 8 - rows if b == 1 else rows
            edge_out[e, k] = jnp.where(kept(b, rows), near, turn(far, shift, 0))
        i = AROUND.index((a, b))
        copies_e.append(
            (
                remote(edge_out.at[e], edge_in.at[e], s_b.at[i], r_b.at[i], (w + a, n + b)),
                there(a, b),
                there(-a, -b),
            )
        )
    start(copies_e)

    lane = iota((8, 128), 1)
    lane4 = iota((1, 128), 1) & 3

    def coarser(pairs, s):
        return pair_sum(pair_sum(pairs[0] + pairs[1], s, 0), s, 1) * 0.125

    def packed(cells):
        rows = [cells[0][0:1], cells[0][4:5], cells[1][0:1], cells[1][4:5]]
        row = rows[3]
        for k in range(3):
            row = jnp.where(lane4 == k, rows[k], row)
        return row

    finer = [coarser((voidage[16 * i : 16 * i + 8], voidage[16 * i + 8 : 16 * i + 16]), 1) for i in range(4)]
    c1p[n] = packed([coarser((finer[0], finer[1]), 2), coarser((finer[2], finer[3]), 2)])


    def row_copies(ref, send, recv):
        return [
            (
                remote(ref.at[n], ref.at[n], send.at[d], recv.at[d], (w, lax.rem(n + d, nn))),
                jnp.bool_(True),
                jnp.bool_(True),
            )
            for d in range(1, nn)
        ]

    def start_rows(copies):
        for copy, _, _ in copies:
            copy.start()
        pending.extend(copies)

    def arrive_rows(copies):
        for copy, _, _ in copies:
            copy.wait_recv()

    def slab_copies(ref, reach, send, recv):
        made = []
        for d in [s * k for k in range(1, reach + 1) for s in (1, -1)]:
            i = d + REACH
            made.append(
                (
                    remote(ref.at[REACH], ref.at[REACH - d], send.at[i], recv.at[i], (w + d, n)),
                    w_ok(d),
                    w_ok(-d),
                )
            )
        return made

    def rows_to_slab(ref):
        row = iota((8, 128), 0)
        slab = jnp.zeros((8, 128), F32)
        for k in range(nn):
            slab = jnp.where(row == k, jnp.broadcast_to(ref[k], (8, 128)), slab)
        return slab

    copies_1p = row_copies(c1p, s_1p, r_1p)
    start_rows(copies_1p)

    def fill_gather(f, values):
        high, low = halves(values)
        glhs[f * 64 : f * 64 + 64, 0:128] = high
        glhs[f * 64 : f * 64 + 64, 128:256] = low

    def gather(fields):
        def one(o, carry):
            width = CAP * slots
            at = pl.ds(pl.multiple_of(o * width, slots), width)
            found = jnp.dot(glhs[0 : 64 * fields], ohx[:, at], preferred_element_type=F32)
            for r in range(CAP):
                zy, _ = cells_of(o, r)
                hit = jnp.broadcast_to(zy, zy_iota.shape) == zy_iota
                for f in range(fields):
                    gath[o, f * CAP + r : f * CAP + r + 1] = jnp.sum(
                        jnp.where(hit, found[64 * f : 64 * f + 64, r * slots : (r + 1) * slots], 0.0),
                        axis=0, keepdims=True,
                    )
            return carry

        lax.fori_loop(0, GROUPS, one, 0)

    for f in range(3):
        fill_gather(f, gas[f].reshape(64, 128))
    fill_gather(3, voidage)
    gather(4)
    for o in range(GROUPS):
        slip = [gath[o, c * CAP : (c + 1) * CAP] - pin[o, (1 + c) * CAP : (2 + c) * CAP] for c in range(3)]
        speed = jnp.sqrt(slip[0] * slip[0] + slip[1] * slip[1] + slip[2] * slip[2])
        held = gath[o, 3 * CAP : 4 * CAP]
        scale = pin[o, 0:CAP] * (drag_base + drag_slope * speed) * jnp.exp(-void_power * jnp.log(held))
        for c in range(3):
            drg[o, c * CAP : (c + 1) * CAP] = scale * slip[c]

    arrive_rows(copies_1p)
    l2p[REACH] = rows_to_slab(c1p)
    for i, d in enumerate((2 * SPREAD, -2 * SPREAD)):
        pl.when(w_ok(-d))(functools.partial(pl.semaphore_wait, hello.at[i], 1))
    copies_2p = slab_copies(l2p, REACH, s_2p, r_2p)
    start(copies_2p)

    def spread_drag(o, carry):
        for r in range(CAP):
            at = pl.ds(pl.multiple_of((o * CAP + r) * slots, slots), slots)
            zy, _ = cells_of(o, r)
            hit = jnp.broadcast_to(zy, zy_iota.shape) == zy_iota
            for c in range(3):
                row = drg[o, c * CAP + r : c * CAP + r + 1]
                high, low = halves(jnp.where(hit, jnp.broadcast_to(row, zy_iota.shape), 0.0))
                rlhs[128 * c : 128 * c + 64, at] = high
                rlhs[128 * c + 64 : 128 * c + 128, at] = low
        return carry

    lax.fori_loop(0, GROUPS, spread_drag, 0)
    sums = lax.dot_general(
        rlhs[...], ohx[0:128], (((1,), (1,)), ((), ())), preferred_element_type=F32
    )
    for c in range(3):
        onto = sums[128 * c : 128 * c + 64] + sums[128 * c + 64 : 128 * c + 128]
        grow[c] = gas[c].reshape(64, 128) - step_duration * onto / voidage

    arrive(copies_c0)
    arrive(copies_b)
    arrive(copies_e)
    for e, (a, b) in enumerate(EDGES):
        for k, (one, two, rows) in enumerate(tiles):
            tile = edge_in[e, k]
            shift = 8 - rows if b == 1 else rows
            at = slice(0, 8) if b == 1 else slice(16, 24)
            for d, layer in ((one, tile), (two, turn(tile, -shift, 0))):
                por0[8 - d if a == 1 else 15 + d, at] = layer

    row24 = iota((24, 128), 0)
    inside_y = jnp.logical_and(
        jnp.logical_or(row24 >= 8, n > 0), jnp.logical_or(row24 < 16, n < nn - 1)
    )
    inside_y = jnp.where(inside_y, 1, 0)

    def inside(block):
        ok = jnp.logical_and(w + block >= 0, w + block < nw)
        return inside_y * jnp.where(ok, 1, 0) > 0

    def coefs(por, z, s, half, layers, cz, cym, cyp, cxm, cxp, dg, di):
        here = por[z]
        zm = half * (here + por[z - 1])
        zp = half * (here + por[z + 1])
        ym = half * (here + turn(here, s, 0))
        yp = half * (here + turn(here, -s, 0))
        xm = half * (here + lanes_before(here, s))
        xp = half * (here + lanes_after(here, s))
        diagonal = zm + zp + ym + yp + xm + xp
        lanes = iota(here.shape, 1)
        cz[z] = zm
        cym[z] = ym
        cyp[z] = yp
        cxm[z] = jnp.where(lanes >= s, xm, 0.0)
        cxp[z] = jnp.where(lanes < 128 - s, xp, 0.0)
        dg[z] = diagonal
        scaled = jnp.where(inside(z // layers - 1), relax_weight / diagonal, 0.0)
        di[z] = scaled
        return scaled

    def residual_at(v, b, z, s, cz, cym, cyp, cxm, cxp, dg):
        here = v[z]
        beside = cz[z] * v[z - 1] + cz[z + 1] * v[z + 1]
        beside = beside + (cym[z] * turn(here, s, 0) + cyp[z] * turn(here, -s, 0))
        beside = beside + (cxm[z] * turn(here, s, 1) + cxp[z] * turn(here, -s, 1))
        return here, (b[z] - dg[z] * here) + beside

    def sweep(v, to, b, z, s, cz, cym, cyp, cxm, cxp, dg, di):
        here, residual = residual_at(v, b, z, s, cz, cym, cyp, cxm, cxp, dg)
        to[z] = here + di[z] * residual

    level0 = (z0, ym0, yp0, xm0, xp0, dg0)
    level1 = (z1, ym1, yp1, xm1, xp1, dg1)

    def first0(z):
        b = c0[z] - por0[z] * (1.0 / step_duration)
        b0[z] = b
        va0[z] = coefs(por0, z, 1, 0.5, 8, *level0, di0) * b

    zloop(2, 22, first0)
    zloop(3, 21, lambda z: sweep(va0, vb0, b0, z, 1, *level0, di0))

    def por1_of(i):
        por1[i] = coarser((por0[2 * i], por0[2 * i + 1]), 1)

    zloop(0, 12, por1_of)

    def down0(i):
        _, low = residual_at(vb0, b0, 2 * i, 1, *level0)
        _, high = residual_at(vb0, b0, 2 * i + 1, 1, *level0)
        b1[i] = coarser((low, high), 1)

    zloop(2, 10, down0, 2)
    zloop(1, 11, lambda i: coefs(por1, i, 2, 0.125, 4, *level1, di1), 5)
    z1[11] = 0.125 * (por1[11] + por1[10])

    def first1(i):
        va1[i] = di1[i] * b1[i]

    zloop(2, 10, first1, 8)
    zloop(3, 9, lambda i: sweep(va1, vb1, b1, i, 2, *level1, di1), 6)
    left = [residual_at(vb1, b1, i, 2, *level1)[1][8:16] for i in range(4, 8)]
    c1b[n] = packed([coarser((left[0], left[1]), 2), coarser((left[2], left[3]), 2)])
    copies_1b = row_copies(c1b, s_1b, r_1b)
    start_rows(copies_1b)

    even_lane = (lane & 1) == 0
    row = iota((8, 128), 0)
    even_row = (row & 1) == 0
    for k in range(2):
        i = 4 + 2 * k
        right = jnp.where(even_lane, b1[i, 8:16], b1[i + 1, 8:16])
        iterate = jnp.where(even_lane, vb1[i, 8:16], vb1[i + 1, 8:16])
        l1out[k] = jnp.where(even_row, right, iterate)
    copies_l1 = [
        (
            remote(l1out, l1in.at[1 - a, 1 - b], s_l1.at[i], r_l1.at[i], (w + a, n + b)),
            there(a, b),
            there(-a, -b),
        )
        for i, (a, b) in enumerate(AROUND)
    ]
    start(copies_l1)

    arrive(copies_2p)

    def unpack4(slab):
        def split(v, s):
            low = (lane & s) == 0
            return jnp.where(low, v, turn(v, s, 1)), jnp.where(low, turn(v, -s, 1), v)

        first, second = split(slab, 1)
        (zero, two), (one, three) = split(first, 2), split(second, 2)
        return zero, one, two, three

    def unpack_por(k):
        cells = unpack4(l2p[k])
        for q in range(4):
            p2[2 * k + q // 2, q % 2] = cells[q]
        p3[k] = pair_sum((cells[0] + cells[1]) + (cells[2] + cells[3]), 4, 1) * 0.125

    zloop(0, 2 * REACH + 1, unpack_por, 5)
    real_row = jnp.where(row < nn, 1, 0)

    def inside_coarse(block):
        ok = jnp.logical_and(w + block >= 0, w + block < nw)
        return real_row * jnp.where(ok, 1, 0) > 0

    def coefs2(j):
        half = 0.5 * 0.25**2
        even, odd = p2[j, 0], p2[j, 1]
        inner = half * (even + odd)
        ci2[j] = inner
        outer = half * (even + rows_before(odd, 1))
        co2[j] = outer
        outer_odd = half * (odd + rows_after(even, 1))
        ok = inside_coarse(j // 2 - REACH)
        for y, here in enumerate((even, odd)):
            zm = half * (here + p2[j - 1, y])
            zp = half * (here + p2[j + 1, y])
            xm = half * (here + lanes_before(here, 4))
            xp = half * (here + lanes_after(here, 4))
            diagonal = zm + zp + inner + (outer_odd if y else outer) + xm + xp
            z2[j, y] = zm
            xm2[j, y] = jnp.where(lane >= 4, xm, 0.0)
            xp2[j, y] = jnp.where(lane < 124, xp, 0.0)
            dg2[j, y] = diagonal
            di2[j, y] = jnp.where(ok, relax_weight / diagonal, 0.0)

    zloop(1, 4 * REACH + 1, coefs2)

    def coefs3(k):
        half = 0.5 * 0.25**3
        here = p3[k]
        zm = half * (here + p3[k - 1])
        zp = half * (here + p3[k + 1])
        ym = half * (here + rows_before(here, 1))
        yp = half * (here + rows_after(here, 1))
        xm = half * (here + lanes_before(here, 8))
        xp = half * (here + lanes_after(here, 8))
        diagonal = zm + zp + ym + yp + xm + xp
        z3[k] = zm
        y3[k] = ym
        xm3[k] = jnp.where(lane >= 8, xm, 0.0)
        xp3[k] = jnp.where(lane < 120, xp, 0.0)
        dg3[k] = diagonal
        di3[k] = jnp.where(inside_coarse(k - REACH), relax_weight / diagonal, 0.0)

    zloop(1, 2 * REACH, coefs3)

    arrive_rows(copies_1b)
    l2b[REACH] = rows_to_slab(c1b)
    copies_2b = slab_copies(l2b, RHS_REACH, s_2b, r_2b)
    start(copies_2b)

    arrive(copies_l1)
    for a, b in AROUND:
        for k in range(2):
            both_layers = l1in[1 + a, 1 + b, k]
            for q in range(2):
                if q == 0:
                    layer = jnp.where(even_lane, both_layers, turn(both_layers, 1, 1))
                else:
                    layer = jnp.where(even_lane, turn(both_layers, -1, 1), both_layers)
                i = 4 * (1 + a) + 2 * k + q
                at = slice(8 * (1 + b), 8 * (2 + b))
                b1[i, at] = jnp.where(even_row, layer, turn(layer, 1, 0))
                vb1[i, at] = jnp.where(even_row, turn(layer, -1, 0), layer)

    def residual2(v, j):
        even, odd = v[j, 0], v[j, 1]
        outer = co2[j]
        made = []
        for y, here in enumerate((even, odd)):
            beside = z2[j, y] * v[j - 1, y] + z2[j + 1, y] * v[j + 1, y]
            if y == 0:
                beside = beside + (ci2[j] * odd + outer * rows_before(odd, 1))
            else:
                beside = beside + (ci2[j] * even + rows_after(outer, 1) * rows_after(even, 1))
            beside = beside + (xm2[j, y] * turn(here, 4, 1) + xp2[j, y] * turn(here, -4, 1))
            made.append((here, (b2[j, y] - dg2[j, y] * here) + beside))
        return made

    def sweep2(v, to):
        def at(j):
            for y, (here, residual) in enumerate(residual2(v, j)):
                to[j, y] = here + di2[j, y] * residual

        return at

    def residual3(v, k):
        here = v[k]
        beside = z3[k] * v[k - 1] + z3[k + 1] * v[k + 1]
        beside = beside + (y3[k] * rows_before(here, 1) + rows_after(y3[k], 1) * rows_after(here, 1))
        beside = beside + (xm3[k] * turn(here, 8, 1) + xp3[k] * turn(here, -8, 1))
        return here, (b3[k] - dg3[k] * here) + beside

    def sweep3(v, to):
        def at(k):
            here, residual = residual3(v, k)
            to[k] = here + di3[k] * residual

        return at

    arrive(copies_2b)

    def first2(k):
        cells = unpack4(l2b[k])
        for q in range(4):
            j, y = 2 * k + q // 2, q % 2
            b2[j, y] = cells[q]
            va2[j, y] = di2[j, y] * cells[q]

    zloop(1, 2 * REACH, first2)
    zloop(3, 27, sweep2(va2, vb2))

    def down2(k):
        low = residual2(vb2, 2 * k)
        high = residual2(vb2, 2 * k + 1)
        b = pair_sum((low[0][1] + low[1][1]) + (high[0][1] + high[1][1]), 4, 1) * 0.125
        b3[k] = b
        va3[k] = di3[k] * b

    zloop(2, 13, down2, 3)
    zloop(3, 12, sweep3(va3, vb3), 9)
    zloop(4, 11, sweep3(vb3, va3), 7)
    zloop(5, 10, sweep3(va3, vb3), 5)

    def up2(k):
        for q in range(4):
            j, y = 2 * k + q // 2, q % 2
            va2[j, y] = vb2[j, y] + vb3[k]

    zloop(5, 10, up2, 5)
    zloop(11, 19, sweep2(va2, vb2))
    for j in range(12, 18):
        for y, (here, residual) in enumerate(residual2(vb2, j)):
            vfin[j - 12, y, 8:16] = here + di2[j, y] * residual

    low_row = row < 4
    for q in range(6):
        for b in range(3):
            cells = [
                jnp.broadcast_to(vfin[q, y, pl.ds(7 + n + b, 1)], (8, 128)) for y in range(2)
            ]
            step = jnp.where(low_row, cells[0], cells[1])
            at = slice(8 * b, 8 * b + 8)
            for i in (2 * q, 2 * q + 1):
                va1[i, at] = vb1[i, at] + step
    zloop(1, 11, lambda i: sweep(va1, vb1, b1, i, 2, *level1, di1), 5)
    zloop(2, 10, lambda i: sweep(vb1, va1, b1, i, 2, *level1, di1))

    def up0(i):
        step = va1[i]
        va0[2 * i] = vb0[2 * i] + step
        va0[2 * i + 1] = vb0[2 * i + 1] + step

    zloop(2, 10, up0)
    zloop(6, 18, lambda z: sweep(va0, vb0, b0, z, 1, *level0, di0))
    zloop(7, 17, lambda z: sweep(vb0, va0, b0, z, 1, *level0, di0), 5)

    for z in range(8):
        whole = va0[8 + z]
        here = whole[8:16]
        slopes = [
            0.5 * (va0[9 + z, 8:16] - va0[7 + z, 8:16]),
            0.5 * (turn(whole, -1, 0)[8:16] - turn(whole, 1, 0)[8:16]),
            0.5 * (lanes_after(here, 1) - lanes_before(here, 1)),
        ]
        for c in range(3):
            g_out[c, z] = slopes[c]
            high, low = halves(slopes[c])
            glhs[64 * c + 8 * z : 64 * c + 8 * z + 8, 0:128] = high
            glhs[64 * c + 8 * z : 64 * c + 8 * z + 8, 128:256] = low
    gather(3)
    for o in range(GROUPS):
        for c in range(3):
            at = slice(c * CAP, (c + 1) * CAP)
            drg[o, at] = drg[o, at] - pin[o, 0:CAP] * gath[o, at]
    copies_d = []
    for o in range(GROUPS):
        d = o - SPREAD
        if d:
            copies_d.append(
                (remote(drg.at[o], back.at[o], s_d.at[o], r_d.at[o], (w - d, n)), w_ok(-d), w_ok(d))
            )
    start(copies_d)
    back[SPREAD] = drg[SPREAD]
    for z in range(8):
        p_out[z] = va0[8 + z, 8:16]
        for c in range(3):
            g_out[c, z] = grow[c, 8 * z : 8 * z + 8] - step_duration * g_out[c, z]
    for copy, sends, _ in pending[: -len(copies_d)]:
        pl.when(sends)(copy.wait_send)
    fluid_scale = live * step_duration / (particle_density * volume)
    moved = [
        live * (vel[c] + (step_duration * gravity if c == 0 else 0.0)) + fluid_scale * con[c] * live
        for c in range(3)
    ]
    arrive(copies_d)
    for c in range(3):
        fluid = jnp.zeros((blocks, slots), F32)
        for b in range(blocks):
            one = back[off[b] + SPREAD, pl.ds(c * CAP + rank[b], 1)]
            fluid = jnp.where(row8 == b, jnp.broadcast_to(one, fluid.shape), fluid)
        u_out[c] = moved[c] + fluid_scale * fluid

    for copy, sends, _ in copies_d:
        pl.when(sends)(copy.wait_send)


def put_out(p, g, u, p_out, g_out, u_out):
    p_out[...] = p[...]
    g_out[...] = g[...]
    u_out[...] = u[...]


def local(nw, nn, position, velocity, radius, count, cell, offset, neighbours, gas, source, before):
    vmem = pl.BlockSpec(memory_space=pltpu.VMEM)
    hbm = pl.BlockSpec(memory_space=pltpu.HBM)

    def ram(*shape, dtype=F32):
        return pltpu.VMEM(shape, dtype)

    dma = pltpu.SemaphoreType.DMA
    block = ram(24, 24, 128)
    block1 = ram(12, 24, 128)
    tall = 2 * REACH + 1
    coarse2 = ram(2 * tall, 2, 8, 128)
    coarse2y = ram(2 * tall, 8, 128)
    coarse3 = ram(tall, 8, 128)
    particles = SLOTS * radius.shape[1]
    given = (count, offset, neighbours, position, velocity, radius, cell, gas, source, before)
    scratch = [
        *[pltpu.SMEM(a.shape, a.dtype) for a in given[:3]],
        *[pltpu.VMEM(a.shape, a.dtype) for a in given[3:]],
        dma((len(given),)),
        *[ram(GROUPS, 16, 128)] * 5,
        ram(3, 64, 128),
        ram(3, 8, 128),
        ram(4, 8, 128, 128),
        ram(256, particles, dtype=BF16),
        ram(384, particles, dtype=BF16),
        ram(256, 256, dtype=BF16),
        *[block] * 12,
        *[block1] * 11,
        ram(4, 3, 8, 128),
        ram(4, 3, 8, 128),
        ram(2, 8, 128),
        ram(3, 3, 2, 8, 128),
        ram(8, 1, 128),
        ram(8, 1, 128),
        coarse3,
        coarse3,
        *[coarse2] * 5,
        coarse2y,
        coarse2y,
        *[coarse2] * 4,
        *[coarse3] * 10,
        ram(6, 2, 24, 128),
        *[dma((GROUPS,))] * 2,
        *[dma((8,))] * 6,
        *[dma((8,))] * 4,
        *[dma((tall,))] * 4,
        *[dma((GROUPS,))] * 2,
        pltpu.SemaphoreType.REGULAR((2,)),
    ]
    results = (
        jax.ShapeDtypeStruct(source.shape, F32),
        jax.ShapeDtypeStruct(gas.shape, F32),
        jax.ShapeDtypeStruct(velocity.shape, F32),
    )
    made = pl.pallas_call(
        functools.partial(kernel, nw, nn),
        out_shape=results,
        in_specs=[hbm] * len(given),
        out_specs=(vmem, vmem, vmem),
        scratch_shapes=scratch,
        compiler_params=pltpu.CompilerParams(
            collective_id=0, has_side_effects=True, vmem_limit_bytes=24 << 20
        ),
        name="bed_step",
    )(*[pltpu.with_memory_space_constraint(a, pltpu.HBM) for a in given])
    return pl.pallas_call(
        put_out,
        out_shape=results,
        in_specs=[vmem] * 3,
        out_specs=(vmem, vmem, vmem),
        compiler_params=pltpu.CompilerParams(vmem_limit_bytes=8 << 20),
        name="put_out",
    )(*made)


def solution(mesh):
    placed = (
        P(None, ("wide", "narrow"), None),
        P(None, ("wide", "narrow"), None),
        P(("wide", "narrow"), None),
        P(("wide", "narrow")),
        P(("wide", "narrow"), None),
        P(("wide", "narrow")),
        P(("wide", "narrow"), None),
        P(None, "wide", "narrow", None),
        P("wide", "narrow", None),
        P("wide", "narrow", None),
    )
    return jax.shard_map(
        functools.partial(local, mesh.shape["wide"], mesh.shape["narrow"]),
        mesh=mesh,
        in_specs=placed,
        out_specs=(
            P("wide", "narrow", None),
            P(None, "wide", "narrow", None),
            P(None, ("wide", "narrow"), None),
        ),
        check_vma=False,
    )
```

```python
import functools

import jax
import jax.numpy as jnp
from jax import lax
from jax.experimental import pallas as pl
from jax.experimental.pallas import tpu as pltpu
from jax.sharding import PartitionSpec as P

SPREAD = 2
CAP = 3
GROUPS = 2 * SPREAD + 1
SLOTS = GROUPS * CAP
REACH = 7
RHS_REACH = 6

relax_weight = 0.8
solid_most = 0.6
void_power = 2.65
drag_base = 0.5
drag_slope = 0.5
stiffness = 16.0
softening = 0.1
particle_density = 2.0
step_duration = 0.25
gravity = -1.0

F32 = jnp.float32
BF16 = jnp.bfloat16
MESH = pl.DeviceIdType.MESH
EDGES = [(a, b) for a in (-1, 1) for b in (-1, 1)]
AROUND = [(a, b) for a in (-1, 0, 1) for b in (-1, 0, 1) if (a, b) != (0, 0)]


def iota(shape, dim):
    return lax.broadcasted_iota(jnp.int32, shape, dim)


def zloop(low, high, body, step=4):
    whole = (high - low) // step
    if whole > 1:

        def chunk(i, carry):
            for k in range(step):
                body(low + i * step + k)
            return carry

        lax.fori_loop(0, whole, chunk, 0)
    else:
        whole = 0
    for z in range(low + whole * step, high):
        body(z)


def turn(v, shift, axis):
    return pltpu.roll(v, shift % v.shape[axis], axis)


def lanes_before(v, s):
    return jnp.where(iota(v.shape, 1) >= s, turn(v, s, 1), 0.0)


def lanes_after(v, s):
    return jnp.where(iota(v.shape, 1) < v.shape[1] - s, turn(v, -s, 1), 0.0)


def rows_before(v, s):
    return jnp.where(iota(v.shape, 0) >= s, turn(v, s, 0), 0.0)


def rows_after(v, s):
    return jnp.where(iota(v.shape, 0) < v.shape[0] - s, turn(v, -s, 0), 0.0)


def pair_sum(v, s, axis):
    low = (iota(v.shape, axis) & s) == 0
    return v + jnp.where(low, turn(v, -s, axis), turn(v, s, axis))


def halves(v):
    high = v.astype(BF16)
    return high, (v - high.astype(F32)).astype(BF16)


def kernel(
    nw, nn,
    counts_in, offs_in, nbr_in, pos_in, vel_in, rad_in, cell_in, gas_in, source_in, before_in,
    p_out, g_out, u_out,
    counts, offs, nbr, pos, vel, rad, cell, gas, source, before,
    stage, pin, back, drg, gath, grow, con, cols,
    ohx, rlhs, glhs,
    por0, c0, b0, va0, vb0, z0, ym0, yp0, xm0, xp0, dg0, di0,
    por1, b1, va1, vb1, z1, ym1, yp1, xm1, xp1, dg1, di1,
    edge_out, edge_in, l1out, l1in, c1p, c1b, l2p, l2b,
    p2, b2, va2, vb2, z2, ci2, co2, xm2, xp2, dg2, di2,
    p3, b3, va3, vb3, z3, y3, xm3, xp3, dg3, di3,
    vfin,
    sent, sent_b, sent_all, r_a, r_c0, r_b, r_l1, r_all, hello,
):
    w = lax.axis_index("wide")
    n = lax.axis_index("narrow")
    blocks, slots = rad.shape

    def w_ok(d):
        return jnp.logical_and(w + d >= 0, w + d < nw)

    def n_ok(d):
        return jnp.logical_and(n + d >= 0, n + d < nn)

    def there(a, b):
        if b == 0:
            return w_ok(a)
        if a == 0:
            return n_ok(b)
        return jnp.logical_and(w_ok(a), n_ok(b))

    def remote(src, dst, send, recv, to):
        return pltpu.make_async_remote_copy(
            src_ref=src, dst_ref=dst, send_sem=send, recv_sem=recv, device_id=to, device_id_type=MESH
        )

    def start(copies):
        for copy, sends, _ in copies:
            pl.when(sends)(copy.start)

    def leave(copies):
        for copy, sends, _ in copies:
            pl.when(sends)(copy.wait_send)

    def arrive(copies):
        for copy, _, gets in copies:
            pl.when(gets)(copy.wait_recv)

    given = (counts_in, offs_in, nbr_in, pos_in, vel_in, rad_in, cell_in, gas_in, source_in, before_in)
    taken = (counts, offs, nbr, pos, vel, rad, cell, gas, source, before)
    loads = [pltpu.make_async_copy(a, b, sent.at[i]) for i, (a, b) in enumerate(zip(given, taken))]
    for i in (0, 1, 5, 4, 6, 8, 9, 3, 2, 7):
        loads[i].start()

    for ref in (pin, back, edge_in, l1in, c1p, c1b, l2p, l2b, vfin):
        ref[...] = jnp.zeros_like(ref)
    for z in range(24):
        por0[z] = jnp.zeros((24, 128), F32)
        c0[z] = jnp.zeros((24, 128), F32)
    barrier = pltpu.get_barrier_semaphore()
    peers = []
    for d in range(1, SPREAD + 1):
        peers += [(w_ok(d), (w + d, n)), (w_ok(-d), (w - d, n))]
    for k in range(nn):
        peers.append((n != k, (w, k)))
    for a, b in AROUND:
        if a and b:
            peers.append((there(a, b), (w + a, n + b)))
    for ok, to in peers:
        pl.when(ok)(
            functools.partial(pl.semaphore_signal, barrier, inc=1, device_id=to, device_id_type=MESH)
        )

    for i in (0, 1, 5, 4, 6):
        loads[i].wait()

    off = [offs[b] for b in range(blocks)]
    rank = []
    for b in range(blocks):
        r = jnp.int32(0)
        for a in range(b):
            r = r + jnp.where(off[a] == off[b], 1, 0)
        rank.append(r)
    row8 = iota((blocks, slots), 0)
    live_count = jnp.zeros((blocks, slots), jnp.int32)
    for b in range(blocks):
        live_count = jnp.where(row8 == b, counts[b], live_count)
    live = jnp.where(iota((blocks, slots), 1) < live_count, 1.0, 0.0)
    radius = rad[...]
    volume = radius * radius * radius
    parts = [volume * live, vel[0], vel[1], vel[2], cell[...].astype(F32)]
    row16 = iota((16, slots), 0)
    for c, part in enumerate(parts):
        rows = jnp.zeros((16, slots), F32)
        for b in range(blocks):
            key = (off[b] + SPREAD) * CAP + rank[b]
            rows = jnp.where(row16 == key, jnp.broadcast_to(part[b : b + 1], rows.shape), rows)
        for o in range(GROUPS):
            stage[o, c * CAP : (c + 1) * CAP] = rows[o * CAP : (o + 1) * CAP]
    pin[SPREAD] = stage[SPREAD]
    for i in (8, 9):
        loads[i].wait()
    for z in range(8):
        c0[8 + z, 8:16] = source[z] + before[z] * (1.0 / step_duration)

    count = jnp.int32(0)
    for ok, _ in peers:
        count = count + jnp.where(ok, 1, 0)
    pl.semaphore_wait(barrier, count)

    copies_a = []
    for o in range(GROUPS):
        d = o - SPREAD
        if d:
            i = len(copies_a)
            copy = remote(stage.at[o], pin.at[o], sent.at[(0, 1, 4, 5)[i]], r_a.at[i], (w + d, n))
            copies_a.append((copy, w_ok(d), w_ok(-d)))
    start(copies_a)

    def block_copies(ref, layers, send, recv, corners=True):
        made = []
        for i, (a, b) in enumerate(AROUND):
            if a and b and not corners:
                continue
            low, high = 8, 16
            if a == 1:
                low = 16 - layers
            if a == -1:
                high = 8 + layers
            made.append(
                (
                    remote(
                        ref.at[low:high, 8:16],
                        ref.at[low - 8 * a : high - 8 * a, 8 * (1 - b) : 8 * (2 - b)],
                        send[i], recv.at[i], (w + a, n + b),
                    ),
                    there(a, b),
                    there(-a, -b),
                )
            )
        return made

    copies_c0 = block_copies(c0, 6, [sent.at[i] for i in (2, 3, 6, 7, 8, 9, 10, 11)], r_c0)

    for i in (3, 2, 7):
        loads[i].wait()

    bar = jnp.concatenate(
        [pos[0], pos[1], pos[2], jnp.where(live > 0.0, radius, -1000.0), jnp.zeros((128 - 4 * blocks, slots), F32)],
        axis=0,
    ).T
    for c in range(4):
        for b in range(blocks):
            k = c * blocks + b
            cols[c, b] = jnp.broadcast_to(bar[:, k : k + 1], (slots, slots))
    factor = stiffness / (slots * 7)

    def contact_of(g, carry):
        own = [jnp.broadcast_to(pos[c, pl.ds(g, 1)], (8, slots)) for c in range(3)]
        own_rad = jnp.broadcast_to(rad[pl.ds(g, 1)], (8, slots))
        total = [jnp.zeros((8, slots), F32) for _ in range(3)]
        for k in range(7):
            other = g if k == 6 else nbr[g, k]
            for j in range(0, slots, 8):
                apart = [own[c] - cols[c, other, j : j + 8] for c in range(3)]
                square = apart[0] * apart[0] + apart[1] * apart[1]
                square = square + (apart[2] * apart[2] + softening * softening)
                inverse = lax.rsqrt(square)
                weight = jnp.maximum((own_rad + cols[3, other, j : j + 8]) * inverse - 1.0, 0.0)
                total = [total[c] + apart[c] * weight for c in range(3)]
        for c in range(3):
            con[c, pl.ds(g, 1)] = jnp.sum(total[c], axis=0, keepdims=True) * factor
        return carry

    lax.fori_loop(0, blocks // 2, contact_of, 0)
    start(copies_c0)
    lax.fori_loop(blocks // 2, blocks, contact_of, 0)

    arrive(copies_a)

    for i, d in enumerate((2 * SPREAD, -2 * SPREAD)):
        pl.when(w_ok(d))(
            functools.partial(
                pl.semaphore_signal, hello.at[i], inc=1, device_id=(w + d, n), device_id_type=MESH
            )
        )

    zy_iota = iota((64, slots), 0)
    x_iota = iota((128, slots), 0)

    def cells_of(o, r):
        where = pin[o, 4 * CAP + r : 4 * CAP + r + 1].astype(jnp.int32)
        return where >> 7, where & 127

    both = jnp.zeros((128, 128), F32)
    for o in range(GROUPS):
        ones, values = [], []
        for r in range(CAP):
            zy, x = cells_of(o, r)
            ones.append(jnp.where(jnp.broadcast_to(x, x_iota.shape) == x_iota, 1.0, 0.0).astype(BF16))
            hit = jnp.broadcast_to(zy, zy_iota.shape) == zy_iota
            here = jnp.where(hit, jnp.broadcast_to(pin[o, r : r + 1], zy_iota.shape), 0.0)
            values.append(jnp.concatenate(halves(here), axis=0))
        one = jnp.concatenate(ones, axis=1)
        at = slice(o * CAP * slots, (o + 1) * CAP * slots)
        ohx[0:128, at] = one
        both = both + lax.dot_general(
            jnp.concatenate(values, axis=1), one, (((1,), (1,)), ((), ())), preferred_element_type=F32
        )
    solid = both[0:64] + both[64:128]
    voidage = 1.0 - solid_most * solid / (1.0 + solid)
    for z in range(8):
        por0[8 + z, 8:16] = voidage[8 * z : 8 * z + 8]
    copies_b = block_copies(por0, 8, [sent_b.at[i] for i in range(8)], r_b, corners=False)
    start(copies_b)

    row = iota((8, 128), 0)
    tiles = ((1, 6, 6), (2, 5, 6), (3, 4, 4))

    def kept(b, rows):
        return row >= 8 - rows if b == 1 else row < rows

    copies_e = []
    for e, (a, b) in enumerate(EDGES):
        for k, (one, two, rows) in enumerate(tiles):
            near, far = [por0[16 - d if a == 1 else 7 + d, 8:16] for d in (one, two)]
            shift = 8 - rows if b == 1 else rows
            edge_out[e, k] = jnp.where(kept(b, rows), near, turn(far, shift, 0))
        i = AROUND.index((a, b))
        copies_e.append(
            (
                remote(edge_out.at[e], edge_in.at[e], sent_b.at[i], r_b.at[i], (w + a, n + b)),
                there(a, b),
                there(-a, -b),
            )
        )
    start(copies_e)

    lane = iota((8, 128), 1)
    lane4 = iota((1, 128), 1) & 3

    def coarser(pairs, s):
        return pair_sum(pair_sum(pairs[0] + pairs[1], s, 0), s, 1) * 0.125

    def packed(cells):
        rows = [cells[0][0:1], cells[0][4:5], cells[1][0:1], cells[1][4:5]]
        row = rows[3]
        for k in range(3):
            row = jnp.where(lane4 == k, rows[k], row)
        return row

    finer = [coarser((voidage[16 * i : 16 * i + 8], voidage[16 * i + 8 : 16 * i + 16]), 1) for i in range(4)]
    c1p[n] = packed([coarser((finer[0], finer[1]), 2), coarser((finer[2], finer[3]), 2)])


    def send_rows(ref, k):
        for d in range(1, nn):
            to = (w, lax.rem(n + d, nn))
            remote(ref.at[n], ref.at[n], sent_all.at[k], r_all.at[k], to).start()

    def all_rows(ref, k):
        part = ref.at[0 : nn - 1]
        return remote(part, part, sent_all.at[k], r_all.at[k], (w, lax.rem(n + 1, nn)))

    def send_slab(ref, reach, k):
        for d in [s * k for k in range(1, reach + 1) for s in (1, -1)]:
            copy = remote(ref.at[REACH], ref.at[REACH - d], sent_all.at[k], r_all.at[k], (w + d, n))
            pl.when(w_ok(d))(copy.start)

    def all_slabs(ref, reach, k):
        partners = jnp.int32(0)
        for d in range(1, reach + 1):
            partners = partners + jnp.where(w_ok(d), 1, 0) + jnp.where(w_ok(-d), 1, 0)
        waits = []
        for c in range(1, 2 * reach + 1):
            part = ref.at[0:c]
            waits.append((partners == c, remote(part, part, sent_all.at[k], r_all.at[k], (w, lax.rem(n + 1, nn)))))
        return waits

    def rows_to_slab(ref):
        row = iota((8, 128), 0)
        slab = jnp.zeros((8, 128), F32)
        for k in range(nn):
            slab = jnp.where(row == k, jnp.broadcast_to(ref[k], (8, 128)), slab)
        return slab

    send_rows(c1p, 0)
    for k in (slice(0, 64), slice(64, 128)):
        ohx[128 + k.start : 128 + k.stop] = ohx[k]

    def fill_gather(f, values):
        high, low = halves(values)
        glhs[f * 64 : f * 64 + 64, 0:128] = high
        glhs[f * 64 : f * 64 + 64, 128:256] = low

    def gather(fields):
        def one(o, carry):
            width = CAP * slots
            at = pl.ds(pl.multiple_of(o * width, slots), width)
            found = jnp.dot(glhs[0 : 64 * fields], ohx[:, at], preferred_element_type=F32)
            for r in range(CAP):
                zy, _ = cells_of(o, r)
                hit = jnp.broadcast_to(zy, zy_iota.shape) == zy_iota
                for f in range(fields):
                    gath[o, f * CAP + r : f * CAP + r + 1] = jnp.sum(
                        jnp.where(hit, found[64 * f : 64 * f + 64, r * slots : (r + 1) * slots], 0.0),
                        axis=0, keepdims=True,
                    )
            return carry

        lax.fori_loop(0, GROUPS, one, 0)

    for f in range(3):
        fill_gather(f, gas[f].reshape(64, 128))
    fill_gather(3, voidage)
    gather(4)
    for o in range(GROUPS):
        slip = [gath[o, c * CAP : (c + 1) * CAP] - pin[o, (1 + c) * CAP : (2 + c) * CAP] for c in range(3)]
        speed = jnp.sqrt(slip[0] * slip[0] + slip[1] * slip[1] + slip[2] * slip[2])
        held = gath[o, 3 * CAP : 4 * CAP]
        scale = pin[o, 0:CAP] * (drag_base + drag_slope * speed) * jnp.exp(-void_power * jnp.log(held))
        for c in range(3):
            drg[o, c * CAP : (c + 1) * CAP] = scale * slip[c]

    all_rows(c1p, 0).wait_recv()
    l2p[REACH] = rows_to_slab(c1p)
    for i, d in enumerate((2 * SPREAD, -2 * SPREAD)):
        pl.when(w_ok(-d))(functools.partial(pl.semaphore_wait, hello.at[i], 1))
    send_slab(l2p, REACH, 1)

    def spread_drag(o, carry):
        for r in range(CAP):
            at = pl.ds(pl.multiple_of((o * CAP + r) * slots, slots), slots)
            zy, _ = cells_of(o, r)
            hit = jnp.broadcast_to(zy, zy_iota.shape) == zy_iota
            for c in range(3):
                row = drg[o, c * CAP + r : c * CAP + r + 1]
                high, low = halves(jnp.where(hit, jnp.broadcast_to(row, zy_iota.shape), 0.0))
                rlhs[128 * c : 128 * c + 64, at] = high
                rlhs[128 * c + 64 : 128 * c + 128, at] = low
        return carry

    lax.fori_loop(0, GROUPS, spread_drag, 0)
    sums = lax.dot_general(
        rlhs[...], ohx[0:128], (((1,), (1,)), ((), ())), preferred_element_type=F32
    )
    for c in range(3):
        onto = sums[128 * c : 128 * c + 64] + sums[128 * c + 64 : 128 * c + 128]
        grow[c] = gas[c].reshape(64, 128) - step_duration * onto / voidage

    arrive(copies_c0)
    arrive(copies_b)
    arrive(copies_e)
    for e, (a, b) in enumerate(EDGES):
        for k, (one, two, rows) in enumerate(tiles):
            tile = edge_in[e, k]
            shift = 8 - rows if b == 1 else rows
            at = slice(0, 8) if b == 1 else slice(16, 24)
            for d, layer in ((one, tile), (two, turn(tile, -shift, 0))):
                por0[8 - d if a == 1 else 15 + d, at] = layer

    row24 = iota((24, 128), 0)
    inside_y = jnp.logical_and(
        jnp.logical_or(row24 >= 8, n > 0), jnp.logical_or(row24 < 16, n < nn - 1)
    )
    inside_y = jnp.where(inside_y, 1, 0)

    def inside(block):
        ok = jnp.logical_and(w + block >= 0, w + block < nw)
        return inside_y * jnp.where(ok, 1, 0) > 0

    def coefs(por, z, s, half, layers, cz, cym, cyp, cxm, cxp, dg, di):
        here = por[z]
        zm = half * (here + por[z - 1])
        zp = half * (here + por[z + 1])
        ym = half * (here + turn(here, s, 0))
        yp = half * (here + turn(here, -s, 0))
        xm = half * (here + lanes_before(here, s))
        xp = half * (here + lanes_after(here, s))
        diagonal = zm + zp + ym + yp + xm + xp
        lanes = iota(here.shape, 1)
        cz[z] = zm
        cym[z] = ym
        cyp[z] = yp
        cxm[z] = jnp.where(lanes >= s, xm, 0.0)
        cxp[z] = jnp.where(lanes < 128 - s, xp, 0.0)
        dg[z] = diagonal
        scaled = jnp.where(inside(z // layers - 1), relax_weight / diagonal, 0.0)
        di[z] = scaled
        return scaled

    def residual_at(v, b, z, s, cz, cym, cyp, cxm, cxp, dg):
        here = v[z]
        beside = cz[z] * v[z - 1] + cz[z + 1] * v[z + 1]
        beside = beside + (cym[z] * turn(here, s, 0) + cyp[z] * turn(here, -s, 0))
        beside = beside + (cxm[z] * turn(here, s, 1) + cxp[z] * turn(here, -s, 1))
        return here, (b[z] - dg[z] * here) + beside

    def sweep(v, to, b, z, s, cz, cym, cyp, cxm, cxp, dg, di):
        here, residual = residual_at(v, b, z, s, cz, cym, cyp, cxm, cxp, dg)
        to[z] = here + di[z] * residual

    level0 = (z0, ym0, yp0, xm0, xp0, dg0)
    level1 = (z1, ym1, yp1, xm1, xp1, dg1)

    def first0(z):
        b = c0[z] - por0[z] * (1.0 / step_duration)
        b0[z] = b
        va0[z] = coefs(por0, z, 1, 0.5, 8, *level0, di0) * b

    zloop(2, 22, first0)
    zloop(3, 21, lambda z: sweep(va0, vb0, b0, z, 1, *level0, di0))

    def por1_of(i):
        por1[i] = coarser((por0[2 * i], por0[2 * i + 1]), 1)

    zloop(0, 12, por1_of)

    def down0(i):
        _, low = residual_at(vb0, b0, 2 * i, 1, *level0)
        _, high = residual_at(vb0, b0, 2 * i + 1, 1, *level0)
        b1[i] = coarser((low, high), 1)

    zloop(2, 10, down0, 2)
    zloop(1, 11, lambda i: coefs(por1, i, 2, 0.125, 4, *level1, di1), 5)
    z1[11] = 0.125 * (por1[11] + por1[10])

    def first1(i):
        va1[i] = di1[i] * b1[i]

    zloop(2, 10, first1, 8)
    zloop(3, 9, lambda i: sweep(va1, vb1, b1, i, 2, *level1, di1), 6)
    left = [residual_at(vb1, b1, i, 2, *level1)[1][8:16] for i in range(4, 8)]
    c1b[n] = packed([coarser((left[0], left[1]), 2), coarser((left[2], left[3]), 2)])
    send_rows(c1b, 2)
    leave(copies_a + copies_c0)

    even_lane = (lane & 1) == 0
    row = iota((8, 128), 0)
    even_row = (row & 1) == 0
    for k in range(2):
        i = 4 + 2 * k
        right = jnp.where(even_lane, b1[i, 8:16], b1[i + 1, 8:16])
        iterate = jnp.where(even_lane, vb1[i, 8:16], vb1[i + 1, 8:16])
        l1out[k] = jnp.where(even_row, right, iterate)
    copies_l1 = [
        (
            remote(l1out, l1in.at[1 - a, 1 - b], sent.at[i], r_l1.at[i], (w + a, n + b)),
            there(a, b),
            there(-a, -b),
        )
        for i, (a, b) in enumerate(AROUND)
    ]
    start(copies_l1)

    for ok, wait in all_slabs(l2p, REACH, 1):
        pl.when(ok)(wait.wait_recv)

    def unpack4(slab):
        def split(v, s):
            low = (lane & s) == 0
            return jnp.where(low, v, turn(v, s, 1)), jnp.where(low, turn(v, -s, 1), v)

        first, second = split(slab, 1)
        (zero, two), (one, three) = split(first, 2), split(second, 2)
        return zero, one, two, three

    def unpack_por(k):
        cells = unpack4(l2p[k])
        for q in range(4):
            p2[2 * k + q // 2, q % 2] = cells[q]
        p3[k] = pair_sum((cells[0] + cells[1]) + (cells[2] + cells[3]), 4, 1) * 0.125

    zloop(0, 2 * REACH + 1, unpack_por, 5)
    real_row = jnp.where(row < nn, 1, 0)

    def inside_coarse(block):
        ok = jnp.logical_and(w + block >= 0, w + block < nw)
        return real_row * jnp.where(ok, 1, 0) > 0

    def coefs2(j):
        half = 0.5 * 0.25**2
        even, odd = p2[j, 0], p2[j, 1]
        inner = half * (even + odd)
        ci2[j] = inner
        outer = half * (even + rows_before(odd, 1))
        co2[j] = outer
        outer_odd = half * (odd + rows_after(even, 1))
        ok = inside_coarse(j // 2 - REACH)
        for y, here in enumerate((even, odd)):
            zm = half * (here + p2[j - 1, y])
            zp = half * (here + p2[j + 1, y])
            xm = half * (here + lanes_before(here, 4))
            xp = half * (here + lanes_after(here, 4))
            diagonal = zm + zp + inner + (outer_odd if y else outer) + xm + xp
            z2[j, y] = zm
            xm2[j, y] = jnp.where(lane >= 4, xm, 0.0)
            xp2[j, y] = jnp.where(lane < 124, xp, 0.0)
            dg2[j, y] = diagonal
            di2[j, y] = jnp.where(ok, relax_weight / diagonal, 0.0)

    zloop(1, 4 * REACH + 1, coefs2)

    def coefs3(k):
        half = 0.5 * 0.25**3
        here = p3[k]
        zm = half * (here + p3[k - 1])
        zp = half * (here + p3[k + 1])
        ym = half * (here + rows_before(here, 1))
        yp = half * (here + rows_after(here, 1))
        xm = half * (here + lanes_before(here, 8))
        xp = half * (here + lanes_after(here, 8))
        diagonal = zm + zp + ym + yp + xm + xp
        z3[k] = zm
        y3[k] = ym
        xm3[k] = jnp.where(lane >= 8, xm, 0.0)
        xp3[k] = jnp.where(lane < 120, xp, 0.0)
        dg3[k] = diagonal
        di3[k] = jnp.where(inside_coarse(k - REACH), relax_weight / diagonal, 0.0)

    zloop(1, 2 * REACH, coefs3)

    all_rows(c1b, 2).wait_recv()
    l2b[REACH] = rows_to_slab(c1b)
    send_slab(l2b, RHS_REACH, 3)
    leave(copies_b + copies_e)

    arrive(copies_l1)
    for a, b in AROUND:
        for k in range(2):
            both_layers = l1in[1 + a, 1 + b, k]
            for q in range(2):
                if q == 0:
                    layer = jnp.where(even_lane, both_layers, turn(both_layers, 1, 1))
                else:
                    layer = jnp.where(even_lane, turn(both_layers, -1, 1), both_layers)
                i = 4 * (1 + a) + 2 * k + q
                at = slice(8 * (1 + b), 8 * (2 + b))
                b1[i, at] = jnp.where(even_row, layer, turn(layer, 1, 0))
                vb1[i, at] = jnp.where(even_row, turn(layer, -1, 0), layer)

    def residual2(v, j):
        even, odd = v[j, 0], v[j, 1]
        outer = co2[j]
        made = []
        for y, here in enumerate((even, odd)):
            beside = z2[j, y] * v[j - 1, y] + z2[j + 1, y] * v[j + 1, y]
            if y == 0:
                beside = beside + (ci2[j] * odd + outer * rows_before(odd, 1))
            else:
                beside = beside + (ci2[j] * even + rows_after(outer, 1) * rows_after(even, 1))
            beside = beside + (xm2[j, y] * turn(here, 4, 1) + xp2[j, y] * turn(here, -4, 1))
            made.append((here, (b2[j, y] - dg2[j, y] * here) + beside))
        return made

    def sweep2(v, to):
        def at(j):
            for y, (here, residual) in enumerate(residual2(v, j)):
                to[j, y] = here + di2[j, y] * residual

        return at

    def residual3(v, k):
        here = v[k]
        beside = z3[k] * v[k - 1] + z3[k + 1] * v[k + 1]
        beside = beside + (y3[k] * rows_before(here, 1) + rows_after(y3[k], 1) * rows_after(here, 1))
        beside = beside + (xm3[k] * turn(here, 8, 1) + xp3[k] * turn(here, -8, 1))
        return here, (b3[k] - dg3[k] * here) + beside

    def sweep3(v, to):
        def at(k):
            here, residual = residual3(v, k)
            to[k] = here + di3[k] * residual

        return at

    for ok, wait in all_slabs(l2b, RHS_REACH, 3):
        pl.when(ok)(wait.wait_recv)

    def first2(k):
        cells = unpack4(l2b[k])
        for q in range(4):
            j, y = 2 * k + q // 2, q % 2
            b2[j, y] = cells[q]
            va2[j, y] = di2[j, y] * cells[q]

    zloop(1, 2 * REACH, first2)
    zloop(3, 27, sweep2(va2, vb2))

    def down2(k):
        low = residual2(vb2, 2 * k)
        high = residual2(vb2, 2 * k + 1)
        b = pair_sum((low[0][1] + low[1][1]) + (high[0][1] + high[1][1]), 4, 1) * 0.125
        b3[k] = b
        va3[k] = di3[k] * b

    zloop(2, 13, down2, 3)
    zloop(3, 12, sweep3(va3, vb3), 9)
    zloop(4, 11, sweep3(vb3, va3), 7)
    zloop(5, 10, sweep3(va3, vb3), 5)

    def up2(k):
        for q in range(4):
            j, y = 2 * k + q // 2, q % 2
            va2[j, y] = vb2[j, y] + vb3[k]

    zloop(5, 10, up2, 5)
    zloop(11, 19, sweep2(va2, vb2))
    for j in range(12, 18):
        for y, (here, residual) in enumerate(residual2(vb2, j)):
            vfin[j - 12, y, 8:16] = here + di2[j, y] * residual

    low_row = row < 4
    for q in range(6):
        for b in range(3):
            cells = [
                jnp.broadcast_to(vfin[q, y, pl.ds(7 + n + b, 1)], (8, 128)) for y in range(2)
            ]
            step = jnp.where(low_row, cells[0], cells[1])
            at = slice(8 * b, 8 * b + 8)
            for i in (2 * q, 2 * q + 1):
                va1[i, at] = vb1[i, at] + step
    zloop(1, 11, lambda i: sweep(va1, vb1, b1, i, 2, *level1, di1), 5)
    zloop(2, 10, lambda i: sweep(vb1, va1, b1, i, 2, *level1, di1))

    def up0(i):
        step = va1[i]
        va0[2 * i] = vb0[2 * i] + step
        va0[2 * i + 1] = vb0[2 * i + 1] + step

    zloop(2, 10, up0)
    zloop(6, 18, lambda z: sweep(va0, vb0, b0, z, 1, *level0, di0))
    zloop(7, 17, lambda z: sweep(vb0, va0, b0, z, 1, *level0, di0), 5)

    for z in range(8):
        whole = va0[8 + z]
        here = whole[8:16]
        slopes = [
            0.5 * (va0[9 + z, 8:16] - va0[7 + z, 8:16]),
            0.5 * (turn(whole, -1, 0)[8:16] - turn(whole, 1, 0)[8:16]),
            0.5 * (lanes_after(here, 1) - lanes_before(here, 1)),
        ]
        for c in range(3):
            g_out[c, z] = slopes[c]
            high, low = halves(slopes[c])
            glhs[64 * c + 8 * z : 64 * c + 8 * z + 8, 0:128] = high
            glhs[64 * c + 8 * z : 64 * c + 8 * z + 8, 128:256] = low
    gather(3)
    for o in range(GROUPS):
        for c in range(3):
            at = slice(c * CAP, (c + 1) * CAP)
            drg[o, at] = drg[o, at] - pin[o, 0:CAP] * gath[o, at]
    copies_d = []
    for o in range(GROUPS):
        d = o - SPREAD
        if d:
            i = len(copies_d)
            copies_d.append(
                (remote(drg.at[o], back.at[o], sent_b.at[i], r_b.at[i], (w - d, n)), w_ok(-d), w_ok(d))
            )
    start(copies_d)
    back[SPREAD] = drg[SPREAD]
    for z in range(8):
        p_out[z] = va0[8 + z, 8:16]
        for c in range(3):
            g_out[c, z] = grow[c, 8 * z : 8 * z + 8] - step_duration * g_out[c, z]
    leave(copies_l1)
    all_rows(c1p, 0).wait_send()
    all_rows(c1b, 2).wait_send()
    for ok, wait in all_slabs(l2p, REACH, 1) + all_slabs(l2b, RHS_REACH, 3):
        pl.when(ok)(wait.wait_send)
    fluid_scale = live * step_duration / (particle_density * volume)
    moved = [
        live * (vel[c] + (step_duration * gravity if c == 0 else 0.0)) + fluid_scale * con[c] * live
        for c in range(3)
    ]
    arrive(copies_d)
    for c in range(3):
        fluid = jnp.zeros((blocks, slots), F32)
        for b in range(blocks):
            one = back[off[b] + SPREAD, pl.ds(c * CAP + rank[b], 1)]
            fluid = jnp.where(row8 == b, jnp.broadcast_to(one, fluid.shape), fluid)
        u_out[c] = moved[c] + fluid_scale * fluid

    leave(copies_d)


def put_out(p, g, u, p_out, g_out, u_out):
    p_out[...] = p[...]
    g_out[...] = g[...]
    u_out[...] = u[...]


def local(nw, nn, position, velocity, radius, count, cell, offset, neighbours, gas, source, before):
    vmem = pl.BlockSpec(memory_space=pltpu.VMEM)
    hbm = pl.BlockSpec(memory_space=pltpu.HBM)

    def ram(*shape, dtype=F32):
        return pltpu.VMEM(shape, dtype)

    dma = pltpu.SemaphoreType.DMA
    block = ram(24, 24, 128)
    block1 = ram(12, 24, 128)
    tall = 2 * REACH + 1
    coarse2 = ram(2 * tall, 2, 8, 128)
    coarse2y = ram(2 * tall, 8, 128)
    coarse3 = ram(tall, 8, 128)
    particles = SLOTS * radius.shape[1]
    given = (count, offset, neighbours, position, velocity, radius, cell, gas, source, before)
    scratch = [
        *[pltpu.SMEM(a.shape, a.dtype) for a in given[:3]],
        *[pltpu.VMEM(a.shape, a.dtype) for a in given[3:]],
        *[ram(GROUPS, 16, 128)] * 5,
        ram(3, 64, 128),
        ram(3, 8, 128),
        ram(4, 8, 128, 128),
        ram(256, particles, dtype=BF16),
        ram(384, particles, dtype=BF16),
        ram(256, 256, dtype=BF16),
        *[block] * 12,
        *[block1] * 11,
        ram(4, 3, 8, 128),
        ram(4, 3, 8, 128),
        ram(2, 8, 128),
        ram(3, 3, 2, 8, 128),
        ram(8, 1, 128),
        ram(8, 1, 128),
        coarse3,
        coarse3,
        *[coarse2] * 5,
        coarse2y,
        coarse2y,
        *[coarse2] * 4,
        *[coarse3] * 10,
        ram(6, 2, 24, 128),
        dma((12,)),
        dma((8,)),
        dma((4,)),
        dma((4,)),
        *[dma((8,))] * 3,
        dma((4,)),
        pltpu.SemaphoreType.REGULAR((2,)),
    ]
    results = (
        jax.ShapeDtypeStruct(source.shape, F32),
        jax.ShapeDtypeStruct(gas.shape, F32),
        jax.ShapeDtypeStruct(velocity.shape, F32),
    )
    made = pl.pallas_call(
        functools.partial(kernel, nw, nn),
        out_shape=results,
        in_specs=[hbm] * len(given),
        out_specs=(vmem, vmem, vmem),
        scratch_shapes=scratch,
        compiler_params=pltpu.CompilerParams(
            collective_id=0, has_side_effects=True, vmem_limit_bytes=24 << 20
        ),
        name="bed_step",
    )(*[pltpu.with_memory_space_constraint(a, pltpu.HBM) for a in given])
    return pl.pallas_call(
        put_out,
        out_shape=results,
        in_specs=[vmem] * 3,
        out_specs=(vmem, vmem, vmem),
        compiler_params=pltpu.CompilerParams(vmem_limit_bytes=8 << 20),
        name="put_out",
    )(*made)


def solution(mesh):
    placed = (
        P(None, ("wide", "narrow"), None),
        P(None, ("wide", "narrow"), None),
        P(("wide", "narrow"), None),
        P(("wide", "narrow")),
        P(("wide", "narrow"), None),
        P(("wide", "narrow")),
        P(("wide", "narrow"), None),
        P(None, "wide", "narrow", None),
        P("wide", "narrow", None),
        P("wide", "narrow", None),
    )
    return jax.shard_map(
        functools.partial(local, mesh.shape["wide"], mesh.shape["narrow"]),
        mesh=mesh,
        in_specs=placed,
        out_specs=(
            P("wide", "narrow", None),
            P(None, "wide", "narrow", None),
            P(None, ("wide", "narrow"), None),
        ),
        check_vma=False,
    )
```

```python
import functools

import jax
import jax.numpy as jnp
from jax import lax
from jax.experimental import pallas as pl
from jax.experimental.pallas import tpu as pltpu
from jax.sharding import PartitionSpec as P

SPREAD = 2
CAP = 3
GROUPS = 2 * SPREAD + 1
SLOTS = GROUPS * CAP
REACH = 7
RHS_REACH = 6

relax_weight = 0.8
solid_most = 0.6
void_power = 2.65
drag_base = 0.5
drag_slope = 0.5
stiffness = 16.0
softening = 0.1
particle_density = 2.0
step_duration = 0.25
gravity = -1.0

F32 = jnp.float32
BF16 = jnp.bfloat16
MESH = pl.DeviceIdType.MESH
EDGES = [(a, b) for a in (-1, 1) for b in (-1, 1)]
AROUND = [(a, b) for a in (-1, 0, 1) for b in (-1, 0, 1) if (a, b) != (0, 0)]


def iota(shape, dim):
    return lax.broadcasted_iota(jnp.int32, shape, dim)


def zloop(low, high, body, step=4):
    whole = (high - low) // step
    if whole > 1:

        def chunk(i, carry):
            for k in range(step):
                body(low + i * step + k)
            return carry

        lax.fori_loop(0, whole, chunk, 0)
    else:
        whole = 0
    for z in range(low + whole * step, high):
        body(z)


def turn(v, shift, axis):
    return pltpu.roll(v, shift % v.shape[axis], axis)


def lanes_before(v, s):
    return jnp.where(iota(v.shape, 1) >= s, turn(v, s, 1), 0.0)


def lanes_after(v, s):
    return jnp.where(iota(v.shape, 1) < v.shape[1] - s, turn(v, -s, 1), 0.0)


def rows_before(v, s):
    return jnp.where(iota(v.shape, 0) >= s, turn(v, s, 0), 0.0)


def rows_after(v, s):
    return jnp.where(iota(v.shape, 0) < v.shape[0] - s, turn(v, -s, 0), 0.0)


def pair_sum(v, s, axis):
    low = (iota(v.shape, axis) & s) == 0
    return v + jnp.where(low, turn(v, -s, axis), turn(v, s, axis))


def halves(v):
    high = v.astype(BF16)
    return high, (v - high.astype(F32)).astype(BF16)


def kernel(
    nw, nn,
    counts_in, offs_in, nbr_in, pos_in, vel_in, rad_in, cell_in, gas_in, source_in, before_in,
    p_out, g_out, u_out,
    counts, offs, nbr, pos, vel, rad, cell, gas, source, before,
    stage, pin, back, drg, gath, grow, con, cols,
    ohx, rlhs, glhs,
    por0, c0, b0, va0, vb0, z0, ym0, yp0, xm0, xp0, dg0, di0,
    por1, b1, va1, vb1, z1, ym1, yp1, xm1, xp1, dg1, di1,
    edge_out, edge_in, l1out, l1in, c1p, c1b, l2p, l2b,
    p2, b2, va2, vb2, z2, ci2, co2, xm2, xp2, dg2, di2,
    p3, b3, va3, vb3, z3, y3, xm3, xp3, dg3, di3,
    vfin,
    sent, sent_b, sent_all, r_a, r_c0, r_b, r_l1, r_all, hello,
):
    w = lax.axis_index("wide")
    n = lax.axis_index("narrow")
    blocks, slots = rad.shape

    def w_ok(d):
        return jnp.logical_and(w + d >= 0, w + d < nw)

    def n_ok(d):
        return jnp.logical_and(n + d >= 0, n + d < nn)

    def there(a, b):
        if b == 0:
            return w_ok(a)
        if a == 0:
            return n_ok(b)
        return jnp.logical_and(w_ok(a), n_ok(b))

    def remote(src, dst, send, recv, to):
        return pltpu.make_async_remote_copy(
            src_ref=src, dst_ref=dst, send_sem=send, recv_sem=recv, device_id=to, device_id_type=MESH
        )

    def start(copies):
        for copy, sends, _ in copies:
            pl.when(sends)(copy.start)

    def leave(copies):
        for copy, sends, _ in copies:
            pl.when(sends)(copy.wait_send)

    def arrive(copies):
        for copy, _, gets in copies:
            pl.when(gets)(copy.wait_recv)

    given = (counts_in, offs_in, nbr_in, pos_in, vel_in, rad_in, cell_in, gas_in, source_in, before_in)
    taken = (counts, offs, nbr, pos, vel, rad, cell, gas, source, before)
    loads = [pltpu.make_async_copy(a, b, sent.at[i]) for i, (a, b) in enumerate(zip(given, taken))]
    for i in (0, 1, 5, 4, 6, 8, 9, 3, 2, 7):
        loads[i].start()

    for ref in (pin, back, edge_in, l1in, c1p, c1b, l2p, l2b, vfin):
        ref[...] = jnp.zeros_like(ref)
    for z in range(24):
        por0[z] = jnp.zeros((24, 128), F32)
        c0[z] = jnp.zeros((24, 128), F32)
    barrier = pltpu.get_barrier_semaphore()
    peers = []
    for d in range(1, SPREAD + 1):
        peers += [(w_ok(d), (w + d, n)), (w_ok(-d), (w - d, n))]
    for k in range(nn):
        peers.append((n != k, (w, k)))
    for a, b in AROUND:
        if a and b:
            peers.append((there(a, b), (w + a, n + b)))
    for ok, to in peers:
        pl.when(ok)(
            functools.partial(pl.semaphore_signal, barrier, inc=1, device_id=to, device_id_type=MESH)
        )

    for i in (0, 1, 5, 4, 6):
        loads[i].wait()

    off = [offs[b] for b in range(blocks)]
    rank = []
    for b in range(blocks):
        r = jnp.int32(0)
        for a in range(b):
            r = r + jnp.where(off[a] == off[b], 1, 0)
        rank.append(r)
    row8 = iota((blocks, slots), 0)
    live_count = jnp.zeros((blocks, slots), jnp.int32)
    for b in range(blocks):
        live_count = jnp.where(row8 == b, counts[b], live_count)
    live = jnp.where(iota((blocks, slots), 1) < live_count, 1.0, 0.0)
    radius = rad[...]
    volume = radius * radius * radius
    parts = [volume * live, vel[0], vel[1], vel[2], cell[...].astype(F32)]
    row16 = iota((16, slots), 0)
    for c, part in enumerate(parts):
        rows = jnp.zeros((16, slots), F32)
        for b in range(blocks):
            key = (off[b] + SPREAD) * CAP + rank[b]
            rows = jnp.where(row16 == key, jnp.broadcast_to(part[b : b + 1], rows.shape), rows)
        for o in range(GROUPS):
            stage[o, c * CAP : (c + 1) * CAP] = rows[o * CAP : (o + 1) * CAP]
    pin[SPREAD] = stage[SPREAD]
    for i in (8, 9):
        loads[i].wait()
    for z in range(8):
        c0[8 + z, 8:16] = source[z] + before[z] * (1.0 / step_duration)

    count = jnp.int32(0)
    for ok, _ in peers:
        count = count + jnp.where(ok, 1, 0)
    pl.semaphore_wait(barrier, count)

    copies_a = []
    for o in range(GROUPS):
        d = o - SPREAD
        if d:
            i = len(copies_a)
            copy = remote(stage.at[o], pin.at[o], sent.at[(0, 1, 4, 5)[i]], r_a.at[i], (w + d, n))
            copies_a.append((copy, w_ok(d), w_ok(-d)))
    start(copies_a)

    def block_copies(ref, layers, send, recv, corners=True):
        made = []
        for i, (a, b) in enumerate(AROUND):
            if a and b and not corners:
                continue
            low, high = 8, 16
            if a == 1:
                low = 16 - layers
            if a == -1:
                high = 8 + layers
            made.append(
                (
                    remote(
                        ref.at[low:high, 8:16],
                        ref.at[low - 8 * a : high - 8 * a, 8 * (1 - b) : 8 * (2 - b)],
                        send[i], recv.at[i], (w + a, n + b),
                    ),
                    there(a, b),
                    there(-a, -b),
                )
            )
        return made

    copies_c0 = block_copies(c0, 6, [sent.at[i] for i in (2, 3, 6, 7, 8, 9, 10, 11)], r_c0)

    for i in (3, 2, 7):
        loads[i].wait()

    bar = jnp.concatenate(
        [pos[0], pos[1], pos[2], jnp.where(live > 0.0, radius, -1000.0), jnp.zeros((128 - 4 * blocks, slots), F32)],
        axis=0,
    ).T
    for c in range(4):
        for b in range(blocks):
            k = c * blocks + b
            cols[c, b] = jnp.broadcast_to(bar[:, k : k + 1], (slots, slots))
    factor = stiffness / (slots * 7)

    def contact_of(g, carry):
        own = [jnp.broadcast_to(pos[c, pl.ds(g, 1)], (8, slots)) for c in range(3)]
        own_rad = jnp.broadcast_to(rad[pl.ds(g, 1)], (8, slots))
        total = [jnp.zeros((8, slots), F32) for _ in range(3)]
        for k in range(7):
            other = g if k == 6 else nbr[g, k]
            for j in range(0, slots, 8):
                apart = [own[c] - cols[c, other, j : j + 8] for c in range(3)]
                square = apart[0] * apart[0] + apart[1] * apart[1]
                square = square + (apart[2] * apart[2] + softening * softening)
                inverse = lax.rsqrt(square)
                weight = jnp.maximum((own_rad + cols[3, other, j : j + 8]) * inverse - 1.0, 0.0)
                total = [total[c] + apart[c] * weight for c in range(3)]
        for c in range(3):
            con[c, pl.ds(g, 1)] = jnp.sum(total[c], axis=0, keepdims=True) * factor
        return carry

    lax.fori_loop(0, blocks // 2, contact_of, 0)
    start(copies_c0)
    lax.fori_loop(blocks // 2, blocks, contact_of, 0)

    arrive(copies_a)

    for i, d in enumerate((2 * SPREAD, -2 * SPREAD)):
        pl.when(w_ok(d))(
            functools.partial(
                pl.semaphore_signal, hello.at[i], inc=1, device_id=(w + d, n), device_id_type=MESH
            )
        )

    zy_iota = iota((64, slots), 0)
    x_iota = iota((128, slots), 0)

    def cells_of(o, r):
        where = pin[o, 4 * CAP + r : 4 * CAP + r + 1].astype(jnp.int32)
        return where >> 7, where & 127

    both = jnp.zeros((128, 128), F32)
    for o in range(GROUPS):
        ones, values = [], []
        for r in range(CAP):
            zy, x = cells_of(o, r)
            ones.append(jnp.where(jnp.broadcast_to(x, x_iota.shape) == x_iota, 1.0, 0.0).astype(BF16))
            hit = jnp.broadcast_to(zy, zy_iota.shape) == zy_iota
            here = jnp.where(hit, jnp.broadcast_to(pin[o, r : r + 1], zy_iota.shape), 0.0)
            values.append(jnp.concatenate(halves(here), axis=0))
        one = jnp.concatenate(ones, axis=1)
        at = slice(o * CAP * slots, (o + 1) * CAP * slots)
        ohx[0:128, at] = one
        both = both + lax.dot_general(
            jnp.concatenate(values, axis=1), one, (((1,), (1,)), ((), ())), preferred_element_type=F32
        )
    solid = both[0:64] + both[64:128]
    voidage = 1.0 - solid_most * solid / (1.0 + solid)
    for z in range(8):
        por0[8 + z, 8:16] = voidage[8 * z : 8 * z + 8]
    copies_b = block_copies(por0, 8, [sent_b.at[i] for i in range(8)], r_b, corners=False)
    start(copies_b)

    row = iota((8, 128), 0)
    tiles = ((1, 6, 6), (2, 5, 6), (3, 4, 4))

    def kept(b, rows):
        return row >= 8 - rows if b == 1 else row < rows

    copies_e = []
    for e, (a, b) in enumerate(EDGES):
        for k, (one, two, rows) in enumerate(tiles):
            near, far = [por0[16 - d if a == 1 else 7 + d, 8:16] for d in (one, two)]
            shift = 8 - rows if b == 1 else rows
            edge_out[e, k] = jnp.where(kept(b, rows), near, turn(far, shift, 0))
        i = AROUND.index((a, b))
        copies_e.append(
            (
                remote(edge_out.at[e], edge_in.at[e], sent_b.at[i], r_b.at[i], (w + a, n + b)),
                there(a, b),
                there(-a, -b),
            )
        )
    start(copies_e)

    lane = iota((8, 128), 1)
    lane4 = iota((1, 128), 1) & 3

    def coarser(pairs, s):
        return pair_sum(pair_sum(pairs[0] + pairs[1], s, 0), s, 1) * 0.125

    def packed(cells):
        rows = [cells[0][0:1], cells[0][4:5], cells[1][0:1], cells[1][4:5]]
        row = rows[3]
        for k in range(3):
            row = jnp.where(lane4 == k, rows[k], row)
        return row

    finer = [coarser((voidage[16 * i : 16 * i + 8], voidage[16 * i + 8 : 16 * i + 16]), 1) for i in range(4)]
    c1p[n] = packed([coarser((finer[0], finer[1]), 2), coarser((finer[2], finer[3]), 2)])


    def send_rows(ref, k):
        for d in range(1, nn):
            to = (w, lax.rem(n + d, nn))
            remote(ref.at[n], ref.at[n], sent_all.at[k], r_all.at[k], to).start()

    def all_rows(ref, k):
        part = ref.at[0 : nn - 1]
        return remote(part, part, sent_all.at[k], r_all.at[k], (w, lax.rem(n + 1, nn)))

    def send_slab(ref, reach, k):
        for d in [s * k for k in range(1, reach + 1) for s in (1, -1)]:
            copy = remote(ref.at[REACH], ref.at[REACH - d], sent_all.at[k], r_all.at[k], (w + d, n))
            pl.when(w_ok(d))(copy.start)

    def all_slabs(ref, reach, k):
        partners = jnp.int32(0)
        for d in range(1, reach + 1):
            partners = partners + jnp.where(w_ok(d), 1, 0) + jnp.where(w_ok(-d), 1, 0)
        waits = []
        for c in range(1, 2 * reach + 1):
            part = ref.at[0:c]
            waits.append((partners == c, remote(part, part, sent_all.at[k], r_all.at[k], (w, lax.rem(n + 1, nn)))))
        return waits

    def rows_to_slab(ref):
        row = iota((8, 128), 0)
        slab = jnp.zeros((8, 128), F32)
        for k in range(nn):
            slab = jnp.where(row == k, jnp.broadcast_to(ref[k], (8, 128)), slab)
        return slab

    send_rows(c1p, 0)
    for k in (slice(0, 64), slice(64, 128)):
        ohx[128 + k.start : 128 + k.stop] = ohx[k]

    def fill_gather(f, values):
        high, low = halves(values)
        glhs[f * 64 : f * 64 + 64, 0:128] = high
        glhs[f * 64 : f * 64 + 64, 128:256] = low

    def gather(fields):
        def one(o, carry):
            width = CAP * slots
            at = pl.ds(pl.multiple_of(o * width, slots), width)
            found = jnp.dot(glhs[0 : 64 * fields], ohx[:, at], preferred_element_type=F32)
            for r in range(CAP):
                zy, _ = cells_of(o, r)
                hit = jnp.broadcast_to(zy, zy_iota.shape) == zy_iota
                for f in range(fields):
                    gath[o, f * CAP + r : f * CAP + r + 1] = jnp.sum(
                        jnp.where(hit, found[64 * f : 64 * f + 64, r * slots : (r + 1) * slots], 0.0),
                        axis=0, keepdims=True,
                    )
            return carry

        lax.fori_loop(0, GROUPS, one, 0)

    for f in range(3):
        fill_gather(f, gas[f].reshape(64, 128))
    fill_gather(3, voidage)
    gather(4)
    for o in range(GROUPS):
        slip = [gath[o, c * CAP : (c + 1) * CAP] - pin[o, (1 + c) * CAP : (2 + c) * CAP] for c in range(3)]
        speed = jnp.sqrt(slip[0] * slip[0] + slip[1] * slip[1] + slip[2] * slip[2])
        held = gath[o, 3 * CAP : 4 * CAP]
        scale = pin[o, 0:CAP] * (drag_base + drag_slope * speed) * jnp.exp(-void_power * jnp.log(held))
        for c in range(3):
            drg[o, c * CAP : (c + 1) * CAP] = scale * slip[c]

    all_rows(c1p, 0).wait_recv()
    l2p[REACH] = rows_to_slab(c1p)
    for i, d in enumerate((2 * SPREAD, -2 * SPREAD)):
        pl.when(w_ok(-d))(functools.partial(pl.semaphore_wait, hello.at[i], 1))
    send_slab(l2p, REACH, 1)

    def spread_drag(o, carry):
        for r in range(CAP):
            at = pl.ds(pl.multiple_of((o * CAP + r) * slots, slots), slots)
            zy, _ = cells_of(o, r)
            hit = jnp.broadcast_to(zy, zy_iota.shape) == zy_iota
            for c in range(3):
                row = drg[o, c * CAP + r : c * CAP + r + 1]
                high, low = halves(jnp.where(hit, jnp.broadcast_to(row, zy_iota.shape), 0.0))
                rlhs[128 * c : 128 * c + 64, at] = high
                rlhs[128 * c + 64 : 128 * c + 128, at] = low
        return carry

    lax.fori_loop(0, GROUPS, spread_drag, 0)
    sums = lax.dot_general(
        rlhs[...], ohx[0:128], (((1,), (1,)), ((), ())), preferred_element_type=F32
    )
    for c in range(3):
        onto = sums[128 * c : 128 * c + 64] + sums[128 * c + 64 : 128 * c + 128]
        grow[c] = gas[c].reshape(64, 128) - step_duration * onto / voidage

    arrive(copies_c0)
    arrive(copies_b)
    arrive(copies_e)
    for e, (a, b) in enumerate(EDGES):
        for k, (one, two, rows) in enumerate(tiles):
            tile = edge_in[e, k]
            shift = 8 - rows if b == 1 else rows
            at = slice(0, 8) if b == 1 else slice(16, 24)
            for d, layer in ((one, tile), (two, turn(tile, -shift, 0))):
                por0[8 - d if a == 1 else 15 + d, at] = layer

    row24 = iota((24, 128), 0)
    inside_y = jnp.logical_and(
        jnp.logical_or(row24 >= 8, n > 0), jnp.logical_or(row24 < 16, n < nn - 1)
    )
    inside_y = jnp.where(inside_y, 1, 0)

    def inside(block):
        ok = jnp.logical_and(w + block >= 0, w + block < nw)
        return inside_y * jnp.where(ok, 1, 0) > 0

    def coefs(por, z, s, half, layers, cz, cym, cyp, cxm, cxp, dg, di):
        here = por[z]
        zm = half * (here + por[z - 1])
        zp = half * (here + por[z + 1])
        ym = half * (here + turn(here, s, 0))
        yp = half * (here + turn(here, -s, 0))
        xm = half * (here + lanes_before(here, s))
        xp = half * (here + lanes_after(here, s))
        diagonal = zm + zp + ym + yp + xm + xp
        lanes = iota(here.shape, 1)
        cz[z] = zm
        cym[z] = ym
        cyp[z] = yp
        cxm[z] = jnp.where(lanes >= s, xm, 0.0)
        cxp[z] = jnp.where(lanes < 128 - s, xp, 0.0)
        dg[z] = diagonal
        scaled = jnp.where(inside(z // layers - 1), relax_weight / diagonal, 0.0)
        di[z] = scaled
        return scaled

    def residual_at(v, b, z, s, cz, cym, cyp, cxm, cxp, dg):
        here = v[z]
        beside = cz[z] * v[z - 1] + cz[z + 1] * v[z + 1]
        beside = beside + (cym[z] * turn(here, s, 0) + cyp[z] * turn(here, -s, 0))
        beside = beside + (cxm[z] * turn(here, s, 1) + cxp[z] * turn(here, -s, 1))
        return here, (b[z] - dg[z] * here) + beside

    def sweep(v, to, b, z, s, cz, cym, cyp, cxm, cxp, dg, di):
        here, residual = residual_at(v, b, z, s, cz, cym, cyp, cxm, cxp, dg)
        to[z] = here + di[z] * residual

    level0 = (z0, ym0, yp0, xm0, xp0, dg0)
    level1 = (z1, ym1, yp1, xm1, xp1, dg1)

    def first0(z):
        b = c0[z] - por0[z] * (1.0 / step_duration)
        b0[z] = b
        va0[z] = coefs(por0, z, 1, 0.5, 8, *level0, di0) * b

    zloop(2, 22, first0, 20)
    zloop(3, 21, lambda z: sweep(va0, vb0, b0, z, 1, *level0, di0), 18)

    def por1_of(i):
        por1[i] = coarser((por0[2 * i], por0[2 * i + 1]), 1)

    zloop(0, 12, por1_of, 12)

    def down0(i):
        _, low = residual_at(vb0, b0, 2 * i, 1, *level0)
        _, high = residual_at(vb0, b0, 2 * i + 1, 1, *level0)
        b1[i] = coarser((low, high), 1)

    zloop(2, 10, down0, 8)
    zloop(1, 11, lambda i: coefs(por1, i, 2, 0.125, 4, *level1, di1), 10)
    z1[11] = 0.125 * (por1[11] + por1[10])

    def first1(i):
        va1[i] = di1[i] * b1[i]

    zloop(2, 10, first1, 8)
    zloop(3, 9, lambda i: sweep(va1, vb1, b1, i, 2, *level1, di1), 6)
    left = [residual_at(vb1, b1, i, 2, *level1)[1][8:16] for i in range(4, 8)]
    c1b[n] = packed([coarser((left[0], left[1]), 2), coarser((left[2], left[3]), 2)])
    send_rows(c1b, 2)
    leave(copies_a + copies_c0)

    even_lane = (lane & 1) == 0
    row = iota((8, 128), 0)
    even_row = (row & 1) == 0
    for k in range(2):
        i = 4 + 2 * k
        right = jnp.where(even_lane, b1[i, 8:16], b1[i + 1, 8:16])
        iterate = jnp.where(even_lane, vb1[i, 8:16], vb1[i + 1, 8:16])
        l1out[k] = jnp.where(even_row, right, iterate)
    copies_l1 = [
        (
            remote(l1out, l1in.at[1 - a, 1 - b], sent.at[i], r_l1.at[i], (w + a, n + b)),
            there(a, b),
            there(-a, -b),
        )
        for i, (a, b) in enumerate(AROUND)
    ]
    start(copies_l1)

    for ok, wait in all_slabs(l2p, REACH, 1):
        pl.when(ok)(wait.wait_recv)

    def unpack4(slab):
        def split(v, s):
            low = (lane & s) == 0
            return jnp.where(low, v, turn(v, s, 1)), jnp.where(low, turn(v, -s, 1), v)

        first, second = split(slab, 1)
        (zero, two), (one, three) = split(first, 2), split(second, 2)
        return zero, one, two, three

    def unpack_por(k):
        cells = unpack4(l2p[k])
        for q in range(4):
            p2[2 * k + q // 2, q % 2] = cells[q]
        p3[k] = pair_sum((cells[0] + cells[1]) + (cells[2] + cells[3]), 4, 1) * 0.125

    zloop(0, 2 * REACH + 1, unpack_por, 5)
    real_row = jnp.where(row < nn, 1, 0)

    def inside_coarse(block):
        ok = jnp.logical_and(w + block >= 0, w + block < nw)
        return real_row * jnp.where(ok, 1, 0) > 0

    def coefs2(j):
        half = 0.5 * 0.25**2
        even, odd = p2[j, 0], p2[j, 1]
        inner = half * (even + odd)
        ci2[j] = inner
        outer = half * (even + rows_before(odd, 1))
        co2[j] = outer
        outer_odd = half * (odd + rows_after(even, 1))
        ok = inside_coarse(j // 2 - REACH)
        for y, here in enumerate((even, odd)):
            zm = half * (here + p2[j - 1, y])
            zp = half * (here + p2[j + 1, y])
            xm = half * (here + lanes_before(here, 4))
            xp = half * (here + lanes_after(here, 4))
            diagonal = zm + zp + inner + (outer_odd if y else outer) + xm + xp
            z2[j, y] = zm
            xm2[j, y] = jnp.where(lane >= 4, xm, 0.0)
            xp2[j, y] = jnp.where(lane < 124, xp, 0.0)
            dg2[j, y] = diagonal
            di2[j, y] = jnp.where(ok, relax_weight / diagonal, 0.0)

    zloop(1, 4 * REACH + 1, coefs2)

    def coefs3(k):
        half = 0.5 * 0.25**3
        here = p3[k]
        zm = half * (here + p3[k - 1])
        zp = half * (here + p3[k + 1])
        ym = half * (here + rows_before(here, 1))
        yp = half * (here + rows_after(here, 1))
        xm = half * (here + lanes_before(here, 8))
        xp = half * (here + lanes_after(here, 8))
        diagonal = zm + zp + ym + yp + xm + xp
        z3[k] = zm
        y3[k] = ym
        xm3[k] = jnp.where(lane >= 8, xm, 0.0)
        xp3[k] = jnp.where(lane < 120, xp, 0.0)
        dg3[k] = diagonal
        di3[k] = jnp.where(inside_coarse(k - REACH), relax_weight / diagonal, 0.0)

    zloop(1, 2 * REACH, coefs3)

    all_rows(c1b, 2).wait_recv()
    l2b[REACH] = rows_to_slab(c1b)
    send_slab(l2b, RHS_REACH, 3)
    leave(copies_b + copies_e)

    arrive(copies_l1)
    for a, b in AROUND:
        for k in range(2):
            both_layers = l1in[1 + a, 1 + b, k]
            for q in range(2):
                if q == 0:
                    layer = jnp.where(even_lane, both_layers, turn(both_layers, 1, 1))
                else:
                    layer = jnp.where(even_lane, turn(both_layers, -1, 1), both_layers)
                i = 4 * (1 + a) + 2 * k + q
                at = slice(8 * (1 + b), 8 * (2 + b))
                b1[i, at] = jnp.where(even_row, layer, turn(layer, 1, 0))
                vb1[i, at] = jnp.where(even_row, turn(layer, -1, 0), layer)

    def residual2(v, j):
        even, odd = v[j, 0], v[j, 1]
        outer = co2[j]
        made = []
        for y, here in enumerate((even, odd)):
            beside = z2[j, y] * v[j - 1, y] + z2[j + 1, y] * v[j + 1, y]
            if y == 0:
                beside = beside + (ci2[j] * odd + outer * rows_before(odd, 1))
            else:
                beside = beside + (ci2[j] * even + rows_after(outer, 1) * rows_after(even, 1))
            beside = beside + (xm2[j, y] * turn(here, 4, 1) + xp2[j, y] * turn(here, -4, 1))
            made.append((here, (b2[j, y] - dg2[j, y] * here) + beside))
        return made

    def sweep2(v, to):
        def at(j):
            for y, (here, residual) in enumerate(residual2(v, j)):
                to[j, y] = here + di2[j, y] * residual

        return at

    def residual3(v, k):
        here = v[k]
        beside = z3[k] * v[k - 1] + z3[k + 1] * v[k + 1]
        beside = beside + (y3[k] * rows_before(here, 1) + rows_after(y3[k], 1) * rows_after(here, 1))
        beside = beside + (xm3[k] * turn(here, 8, 1) + xp3[k] * turn(here, -8, 1))
        return here, (b3[k] - dg3[k] * here) + beside

    def sweep3(v, to):
        def at(k):
            here, residual = residual3(v, k)
            to[k] = here + di3[k] * residual

        return at

    for ok, wait in all_slabs(l2b, RHS_REACH, 3):
        pl.when(ok)(wait.wait_recv)

    def first2(k):
        cells = unpack4(l2b[k])
        for q in range(4):
            j, y = 2 * k + q // 2, q % 2
            b2[j, y] = cells[q]
            va2[j, y] = di2[j, y] * cells[q]

    zloop(1, 2 * REACH, first2, 13)
    zloop(3, 27, sweep2(va2, vb2), 24)

    def down2(k):
        low = residual2(vb2, 2 * k)
        high = residual2(vb2, 2 * k + 1)
        b = pair_sum((low[0][1] + low[1][1]) + (high[0][1] + high[1][1]), 4, 1) * 0.125
        b3[k] = b
        va3[k] = di3[k] * b

    zloop(2, 13, down2, 11)
    zloop(3, 12, sweep3(va3, vb3), 9)
    zloop(4, 11, sweep3(vb3, va3), 7)
    zloop(5, 10, sweep3(va3, vb3), 5)

    def up2(k):
        for q in range(4):
            j, y = 2 * k + q // 2, q % 2
            va2[j, y] = vb2[j, y] + vb3[k]

    zloop(5, 10, up2, 5)
    zloop(11, 19, sweep2(va2, vb2), 8)
    for j in range(12, 18):
        for y, (here, residual) in enumerate(residual2(vb2, j)):
            vfin[j - 12, y, 8:16] = here + di2[j, y] * residual

    low_row = row < 4
    for q in range(6):
        for b in range(3):
            cells = [
                jnp.broadcast_to(vfin[q, y, pl.ds(7 + n + b, 1)], (8, 128)) for y in range(2)
            ]
            step = jnp.where(low_row, cells[0], cells[1])
            at = slice(8 * b, 8 * b + 8)
            for i in (2 * q, 2 * q + 1):
                va1[i, at] = vb1[i, at] + step
    zloop(1, 11, lambda i: sweep(va1, vb1, b1, i, 2, *level1, di1), 10)
    zloop(2, 10, lambda i: sweep(vb1, va1, b1, i, 2, *level1, di1), 8)

    def up0(i):
        step = va1[i]
        va0[2 * i] = vb0[2 * i] + step
        va0[2 * i + 1] = vb0[2 * i + 1] + step

    zloop(2, 10, up0, 8)
    zloop(6, 18, lambda z: sweep(va0, vb0, b0, z, 1, *level0, di0), 12)
    zloop(7, 17, lambda z: sweep(vb0, va0, b0, z, 1, *level0, di0), 10)

    for z in range(8):
        whole = va0[8 + z]
        here = whole[8:16]
        slopes = [
            0.5 * (va0[9 + z, 8:16] - va0[7 + z, 8:16]),
            0.5 * (turn(whole, -1, 0)[8:16] - turn(whole, 1, 0)[8:16]),
            0.5 * (lanes_after(here, 1) - lanes_before(here, 1)),
        ]
        for c in range(3):
            g_out[c, z] = slopes[c]
            high, low = halves(slopes[c])
            glhs[64 * c + 8 * z : 64 * c + 8 * z + 8, 0:128] = high
            glhs[64 * c + 8 * z : 64 * c + 8 * z + 8, 128:256] = low
    gather(3)
    for o in range(GROUPS):
        for c in range(3):
            at = slice(c * CAP, (c + 1) * CAP)
            drg[o, at] = drg[o, at] - pin[o, 0:CAP] * gath[o, at]
    copies_d = []
    for o in range(GROUPS):
        d = o - SPREAD
        if d:
            i = len(copies_d)
            copies_d.append(
                (remote(drg.at[o], back.at[o], sent_b.at[i], r_b.at[i], (w - d, n)), w_ok(-d), w_ok(d))
            )
    start(copies_d)
    back[SPREAD] = drg[SPREAD]
    for z in range(8):
        p_out[z] = va0[8 + z, 8:16]
        for c in range(3):
            g_out[c, z] = grow[c, 8 * z : 8 * z + 8] - step_duration * g_out[c, z]
    leave(copies_l1)
    all_rows(c1p, 0).wait_send()
    all_rows(c1b, 2).wait_send()
    for ok, wait in all_slabs(l2p, REACH, 1) + all_slabs(l2b, RHS_REACH, 3):
        pl.when(ok)(wait.wait_send)
    fluid_scale = live * step_duration / (particle_density * volume)
    moved = [
        live * (vel[c] + (step_duration * gravity if c == 0 else 0.0)) + fluid_scale * con[c] * live
        for c in range(3)
    ]
    arrive(copies_d)
    for c in range(3):
        fluid = jnp.zeros((blocks, slots), F32)
        for b in range(blocks):
            one = back[off[b] + SPREAD, pl.ds(c * CAP + rank[b], 1)]
            fluid = jnp.where(row8 == b, jnp.broadcast_to(one, fluid.shape), fluid)
        u_out[c] = moved[c] + fluid_scale * fluid

    leave(copies_d)


def put_out(p, g, u, p_out, g_out, u_out):
    p_out[...] = p[...]
    g_out[...] = g[...]
    u_out[...] = u[...]


def local(nw, nn, position, velocity, radius, count, cell, offset, neighbours, gas, source, before):
    vmem = pl.BlockSpec(memory_space=pltpu.VMEM)
    hbm = pl.BlockSpec(memory_space=pltpu.HBM)

    def ram(*shape, dtype=F32):
        return pltpu.VMEM(shape, dtype)

    dma = pltpu.SemaphoreType.DMA
    block = ram(24, 24, 128)
    block1 = ram(12, 24, 128)
    tall = 2 * REACH + 1
    coarse2 = ram(2 * tall, 2, 8, 128)
    coarse2y = ram(2 * tall, 8, 128)
    coarse3 = ram(tall, 8, 128)
    particles = SLOTS * radius.shape[1]
    given = (count, offset, neighbours, position, velocity, radius, cell, gas, source, before)
    scratch = [
        *[pltpu.SMEM(a.shape, a.dtype) for a in given[:3]],
        *[pltpu.VMEM(a.shape, a.dtype) for a in given[3:]],
        *[ram(GROUPS, 16, 128)] * 5,
        ram(3, 64, 128),
        ram(3, 8, 128),
        ram(4, 8, 128, 128),
        ram(256, particles, dtype=BF16),
        ram(384, particles, dtype=BF16),
        ram(256, 256, dtype=BF16),
        *[block] * 12,
        *[block1] * 11,
        ram(4, 3, 8, 128),
        ram(4, 3, 8, 128),
        ram(2, 8, 128),
        ram(3, 3, 2, 8, 128),
        ram(8, 1, 128),
        ram(8, 1, 128),
        coarse3,
        coarse3,
        *[coarse2] * 5,
        coarse2y,
        coarse2y,
        *[coarse2] * 4,
        *[coarse3] * 10,
        ram(6, 2, 24, 128),
        dma((12,)),
        dma((8,)),
        dma((4,)),
        dma((4,)),
        *[dma((8,))] * 3,
        dma((4,)),
        pltpu.SemaphoreType.REGULAR((2,)),
    ]
    results = (
        jax.ShapeDtypeStruct(source.shape, F32),
        jax.ShapeDtypeStruct(gas.shape, F32),
        jax.ShapeDtypeStruct(velocity.shape, F32),
    )
    made = pl.pallas_call(
        functools.partial(kernel, nw, nn),
        out_shape=results,
        in_specs=[hbm] * len(given),
        out_specs=(vmem, vmem, vmem),
        scratch_shapes=scratch,
        compiler_params=pltpu.CompilerParams(
            collective_id=0, has_side_effects=True, vmem_limit_bytes=24 << 20
        ),
        name="bed_step",
    )(*[pltpu.with_memory_space_constraint(a, pltpu.HBM) for a in given])
    return pl.pallas_call(
        put_out,
        out_shape=results,
        in_specs=[vmem] * 3,
        out_specs=(vmem, vmem, vmem),
        compiler_params=pltpu.CompilerParams(vmem_limit_bytes=8 << 20),
        name="put_out",
    )(*made)


def solution(mesh):
    placed = (
        P(None, ("wide", "narrow"), None),
        P(None, ("wide", "narrow"), None),
        P(("wide", "narrow"), None),
        P(("wide", "narrow")),
        P(("wide", "narrow"), None),
        P(("wide", "narrow")),
        P(("wide", "narrow"), None),
        P(None, "wide", "narrow", None),
        P("wide", "narrow", None),
        P("wide", "narrow", None),
    )
    return jax.shard_map(
        functools.partial(local, mesh.shape["wide"], mesh.shape["narrow"]),
        mesh=mesh,
        in_specs=placed,
        out_specs=(
            P("wide", "narrow", None),
            P(None, "wide", "narrow", None),
            P(None, ("wide", "narrow"), None),
        ),
        check_vma=False,
    )
```
